8 devices in a mesh: dp: 1 (over z), tp: 2 (over y), cp: 4 (over x, core).
Axes of the slice: x: 2, y: 2, z: 1, core: 2. Of those that a mesh axis runs over, the one named last changes fastest.
Arguments:
- x_tokens: bfloat16 [512, 5120], P(('dp', 'cp', 'tp'))
- w_q: bfloat16 [5120, 40, 128], P(None, 'tp')
- w_k: bfloat16 [5120, 40, 128], P(None, 'tp')
- w_v: bfloat16 [5120, 40, 128], P(None, 'tp')
- w_o: bfloat16 [40, 128, 5120], P('tp')
Outputs:
- output: bfloat16 [512, 5120], P(('dp', 'cp', 'tp'))
All inputs are finite; a program needn't handle non-finite values.
Results may differ from the reference program's by a relative error of at most 0.00536832.
Values are sent between devices in bfloat16 or wider.
A program may use at most 1 GiB of HBM per device.

```python
import jax
import jax.numpy as jnp
from jax import lax

SEQ_LEN = 512
CP_SIZE = 4
D_MODEL = 5120
NUM_HEADS = 40
HEAD_DIM = 128


def setup_inputs(seed: int = 0, part: int = 0) -> dict:
    root_key = jax.random.key(seed)
    x_key = jax.random.fold_in(jax.random.fold_in(root_key, 1), part)
    q_key, k_key, v_key, o_key = jax.random.split(jax.random.fold_in(root_key, 2), 4)
    in_scale = D_MODEL ** -0.5
    out_scale = (NUM_HEADS * HEAD_DIM) ** -0.5
    head_shape = (D_MODEL, NUM_HEADS, HEAD_DIM)
    x_tokens = jax.random.normal(x_key, (SEQ_LEN, D_MODEL), jnp.float32)
    w_q = jax.random.normal(q_key, head_shape, jnp.float32) * (2.5 * in_scale)
    w_k = jax.random.normal(k_key, head_shape, jnp.float32) * in_scale
    w_v = jax.random.normal(v_key, head_shape, jnp.float32) * in_scale
    w_o = jax.random.normal(o_key, (NUM_HEADS, HEAD_DIM, D_MODEL), jnp.float32) * out_scale
    return {'x_tokens': x_tokens.astype(jnp.bfloat16), 'w_q': w_q.astype(jnp.bfloat16), 'w_k': w_k.astype(jnp.bfloat16), 'w_v': w_v.astype(jnp.bfloat16), 'w_o': w_o.astype(jnp.bfloat16)}


def token_positions():
    shard_len = SEQ_LEN // CP_SIZE
    block_len = shard_len // 2
    token_idx = jnp.arange(SEQ_LEN, dtype=jnp.int32)
    owner_shard = token_idx // shard_len
    within = token_idx % shard_len
    nat_block = jnp.where(within < block_len, owner_shard, 2 * CP_SIZE - 1 - owner_shard)
    return nat_block * block_len + within % block_len


def reference(x_tokens, w_q, w_k, w_v, w_o):
    def project(weight):
        flat = jnp.dot(x_tokens, weight.reshape(D_MODEL, NUM_HEADS * HEAD_DIM), preferred_element_type=jnp.float32)
        return flat.astype(jnp.bfloat16).reshape(SEQ_LEN, NUM_HEADS, HEAD_DIM).transpose(1, 0, 2)

    q_heads = project(w_q)
    k_heads = project(w_k)
    v_heads = project(w_v)
    positions = token_positions()
    n_blocks = 2 * CP_SIZE
    block_len = SEQ_LEN // n_blocks
    inv_sqrt = HEAD_DIM ** -0.5

    def one_head(head_args):
        q_head, k_head, v_head = head_args

        def one_block(block_args):
            q_blk, q_pos = block_args
            scores = jnp.dot(q_blk, k_head.T, preferred_element_type=jnp.float32) * inv_sqrt
            causal_mask = positions[None, :] <= q_pos[:, None]
            scores = jnp.where(causal_mask, scores, -1e30)
            weights = jnp.exp(scores - scores.max(axis=-1, keepdims=True))
            row_total = weights.sum(axis=-1, keepdims=True)
            block_out = jnp.dot(weights.astype(jnp.bfloat16), v_head, preferred_element_type=jnp.float32) / row_total
            return block_out.astype(jnp.bfloat16)

        head_blocks = lax.map(one_block, (q_head.reshape(n_blocks, block_len, HEAD_DIM), positions.reshape(n_blocks, block_len)))
        return head_blocks.reshape(SEQ_LEN, HEAD_DIM)

    attn_heads = lax.map(one_head, (q_heads, k_heads, v_heads))
    attn_flat = attn_heads.transpose(1, 0, 2).reshape(SEQ_LEN, NUM_HEADS * HEAD_DIM)
    y_full = jnp.dot(attn_flat, w_o.reshape(NUM_HEADS * HEAD_DIM, D_MODEL), preferred_element_type=jnp.float32)
    return y_full.astype(jnp.bfloat16)
```

```python
import functools

import jax
import jax.numpy as jnp
from jax import lax
from jax.experimental import pallas as pl
from jax.experimental.pallas import tpu as pltpu
from jax.sharding import PartitionSpec as P

BF16, F32 = jnp.bfloat16, jnp.float32
NEG_BIG = -1e30
D = 5120
E = 128
HEADS = 5
HE = HEADS * E
NQKV = 3 * HE
BLK = 64
NK = 4
KC = D // NK
NOUT = 10
NC = D // NOUT
MESH = pl.DeviceIdType.MESH


def remote(src, dst, send_sem, recv_sem, dev):
    return pltpu.make_async_remote_copy(src_ref=src, dst_ref=dst, send_sem=send_sem, recv_sem=recv_sem, device_id=dev, device_id_type=MESH)


def kernel(x_hbm, wq_hbm, wk_hbm, wv_hbm, wo_hbm, y_hbm, xs, w, wo, qkv, acc, osend, ofull, ysend, yrecv, ykeep, yout,
           xin_sem, w_sem, wo_sem, own_send, own_recv, fwd_send, fwd_recv, dg_send, dg_recv, dgf_send, dgf_recv, o_send_sem, o_recv_sem,
           y_send_sem, y_recv_sem, out_sem):
    cp, tp = lax.axis_index('cp'), lax.axis_index('tp')
    x, c = cp // 2, cp % 2
    sib = {'cp': 2 * x + 1 - c, 'tp': tp}
    xn = {'cp': 2 * (1 - x) + c, 'tp': tp}
    xo = {'cp': 2 * (1 - x) + 1 - c, 'tp': tp}
    yn = {'cp': cp, 'tp': 1 - tp}

    def rows(group, core, first=0, n=BLK):
        return pl.ds(pl.multiple_of(group * 128 + core * BLK + first, 32), n)

    def x_in(k):
        return pltpu.make_async_copy(x_hbm.at[:, pl.ds(k * KC, KC)], xs.at[k, rows(0, c), :], xin_sem.at[k])

    for k in range(NK):
        x_in(k).start()

    def w_in(j):
        src = (wq_hbm, wk_hbm, wv_hbm)[j // HEADS].at[cp * HEADS + j % HEADS]
        return pltpu.make_async_copy(src, w.at[:, pl.ds(j * E, E)], w_sem.at[j])

    for j in range(3 * HEADS):
        w_in(j).start()

    def wo_in(n):
        return pltpu.make_async_copy(wo_hbm.at[:, pl.ds(n * NC, NC)], wo.at[n], wo_sem.at[n])

    barrier = pltpu.get_barrier_semaphore()
    for dev in (sib, xn, xo, yn):
        pl.semaphore_signal(barrier, inc=1, device_id=dev, device_id_type=MESH)
    pl.semaphore_wait(barrier, 4)

    def own(k, which):
        dev, group = ((xn, 1), (yn, 2), (sib, 0))[which]
        return remote(xs.at[k, rows(0, c), :], xs.at[k, rows(group, c), :], own_send.at[which, k], own_recv.at[which, k], dev)

    def fwd(k, which):
        return remote(xs.at[k, rows(1 + which, c), :], xs.at[k, rows(1 + which, c), :], fwd_send.at[which, k], fwd_recv.at[which, k], sib)

    def diag(k, which):
        dev = (yn, xn)[which]
        return remote(xs.at[k, rows(1 + which, c, 32 * which, 32), :], xs.at[k, rows(3, c, 32 * which, 32), :],
                      dg_send.at[which, k], dg_recv.at[which, k], dev)

    def diag_fwd(k, which):
        sl = rows(3, c, 32 * which, 32)
        return remote(xs.at[k, sl, :], xs.at[k, sl, :], dgf_send.at[which, k], dgf_recv.at[which, k], sib)

    for k in range(NK):
        x_in(k).wait()
        for which in range(3):
            own(k, which).start()

    def nat(xx, core, t):
        b = 2 * xx + core
        return jnp.where(t == 0, b, 7 - b) * BLK

    nat_of = [nat(x, 0, tp), nat(x, 1, tp), nat(1 - x, 0, tp), nat(1 - x, 1, tp),
              nat(x, 0, 1 - tp), nat(x, 1, 1 - tp), nat(1 - x, 0, 1 - tp), nat(1 - x, 1, 1 - tp)]

    def put_qkv(slot, col, n, val):
        qkv[pl.ds(pl.multiple_of(nat_of[slot], BLK), BLK), pl.ds(col, n)] = val.astype(BF16)

    NSTEPS = ((0, 512), (512, 512), (1024, 512), (1536, 384))

    for k in range(NK):
        own(k, 2).wait_recv()
    for j in range(3 * HEADS):
        w_in(j).wait()
    for n in range(NOUT):
        wo_in(n).start()

    for col, n in NSTEPS:
        val = jnp.dot(xs[0, 0:128, :], w[0:KC, col:col + n], preferred_element_type=F32)
        for k in range(1, NK):
            val += jnp.dot(xs[k, 0:128, :], w[k * KC:(k + 1) * KC, col:col + n], preferred_element_type=F32)
        put_qkv(0, col, n, val[:BLK])
        put_qkv(1, col, n, val[BLK:])

    acc[...] = jnp.zeros_like(acc)

    def accumulate(k, row, m, arow):
        kk = pl.ds(pl.multiple_of(k * KC, KC), KC)
        for col, n in NSTEPS:
            acc[arow:arow + m, col:col + n] += jnp.dot(xs[k, row:row + m, :], w[kk, col:col + n], preferred_element_type=F32)

    @pl.loop(0, NK)
    def _(k):
        for which in range(2):
            own(k, which).wait_recv()
            diag(k, which).start()
            fwd(k, which).start()
        for which in range(2):
            fwd(k, which).wait_recv()
        accumulate(k, 128, 256, 0)

    for col, n in NSTEPS:
        for s in range(4):
            put_qkv(2 + s, col, n, acc[s * BLK:(s + 1) * BLK, col:col + n])

    @pl.loop(0, NK)
    def _(k):
        for which in range(2):
            diag(k, which).wait_recv()
            diag_fwd(k, which).start()
        for which in range(2):
            diag_fwd(k, which).wait_recv()
        accumulate(k, 384, 128, 256)

    for col, n in NSTEPS:
        for s in range(2):
            put_qkv(6 + s, col, n, acc[256 + s * BLK:256 + (s + 1) * BLK, col:col + n])

    inv_sqrt = E ** -0.5

    def o_copy(b, dev_cp):
        lohi = b // 4
        return remote(osend.at[b], ofull.at[lohi, :, pl.ds(pl.multiple_of(cp * HE, E), HE)],
                      o_send_sem.at[b], o_recv_sem.at[lohi, (cp - dev_cp + 4) % 4], {'cp': dev_cp, 'tp': tp})

    def attend(i):
        length = 128 * (i + 1)
        ri = lax.broadcasted_iota(jnp.int32, (128, 128), 0)
        ci = lax.broadcasted_iota(jnp.int32, (128, 128), 1)
        mask = ci <= ri
        for h in range(HEADS):
            q = qkv[i * 128:(i + 1) * 128, h * E:(h + 1) * E]
            kk = qkv[0:length, HE + h * E:HE + (h + 1) * E]
            v = qkv[0:length, 2 * HE + h * E:2 * HE + (h + 1) * E]
            s = lax.dot_general(q, kk, (((1,), (1,)), ((), ())), preferred_element_type=F32) * inv_sqrt
            last = jnp.where(mask, s[:, length - 128:], NEG_BIG)
            s = last if i == 0 else jnp.concatenate([s[:, :length - 128], last], axis=1)
            m = jnp.max(s, axis=-1, keepdims=True)
            p = jnp.exp(s - m)
            l = jnp.sum(p, axis=-1, keepdims=True)
            o = (jnp.dot(p.astype(BF16), v, preferred_element_type=F32) / l).astype(BF16)
            osend[2 * i, :, h * E:(h + 1) * E] = o[:BLK]
            osend[2 * i + 1, :, h * E:(h + 1) * E] = o[BLK:]
        for b in (2 * i, 2 * i + 1):
            r = b if b < 4 else 7 - b

            @pl.when(cp == r)
            def _():
                ofull[b // 4, :, pl.ds(pl.multiple_of(cp * HE, E), HE)] = osend[b]

            @pl.when(cp != r)
            def _():
                o_copy(b, r).start()

    def wait_o(lohi):
        for d in range(1, 4):
            remote(osend.at[0], ofull.at[0, :, pl.ds(0, HE)], o_send_sem.at[0], o_recv_sem.at[lohi, d], sib).wait_recv()

    @pl.when(tp == 0)
    def _():
        attend(3)
        attend(2)
        attend(1)
        attend(0)

    @pl.when(tp == 1)
    def _():
        attend(1)
        attend(0)
        attend(3)
        attend(2)

    away, home = 1 - tp, tp

    def y_copy(n):
        return remote(ysend.at[n], yrecv.at[n], y_send_sem.at[n], y_recv_sem.at[n], yn)

    wait_o(away)

    @pl.loop(0, NOUT)
    def _(n):
        wo_in(n).wait()
        ysend[n] = jnp.dot(ofull[away], wo[n], preferred_element_type=F32)
        y_copy(n).start()

    wait_o(home)

    @pl.loop(0, NOUT)
    def _(n):
        ykeep[n] = jnp.dot(ofull[home], wo[n], preferred_element_type=F32)

    def out_copy(n):
        return pltpu.make_async_copy(yout.at[n], y_hbm.at[:, pl.ds(pl.multiple_of(n * NC, NC), NC)], out_sem.at[n])

    @pl.loop(0, NOUT)
    def _(n):
        y_copy(n).wait_recv()
        yout[n] = (ykeep[n] + yrecv[n]).astype(BF16)
        out_copy(n).start()

    @pl.loop(0, NK)
    def _(k):
        for which in range(3):
            own(k, which).wait_send()
        for which in range(2):
            fwd(k, which).wait_send()
            diag(k, which).wait_send()
            diag_fwd(k, which).wait_send()

    for b in range(8):
        r = b if b < 4 else 7 - b

        @pl.when(cp != r)
        def _():
            o_copy(b, r).wait_send()

    @pl.loop(0, NOUT)
    def _(n):
        y_copy(n).wait_send()
        out_copy(n).wait()


def solution(mesh):
    def device_fn(x_loc, w_q, w_k, w_v, w_o):
        dma = pltpu.SemaphoreType.DMA
        heads_major = [jnp.transpose(t, (1, 0, 2)) for t in (w_q, w_k, w_v)]
        return pl.pallas_call(
            kernel,
            name='attention_layer',
            out_shape=jax.ShapeDtypeStruct((BLK, D), BF16),
            in_specs=[pl.BlockSpec(memory_space=pl.ANY)] * 5,
            out_specs=pl.BlockSpec(memory_space=pl.ANY),
            scratch_shapes=[
                pltpu.VMEM((NK, 512, KC), BF16),
                pltpu.VMEM((D, NQKV), BF16),
                pltpu.VMEM((NOUT, 20 * E, NC), BF16),
                pltpu.VMEM((512, NQKV), BF16),
                pltpu.VMEM((384, NQKV), F32),
                pltpu.VMEM((8, BLK, HE), BF16),
                pltpu.VMEM((2, BLK, 20 * E), BF16),
                pltpu.VMEM((NOUT, BLK, NC), F32),
                pltpu.VMEM((NOUT, BLK, NC), F32),
                pltpu.VMEM((NOUT, BLK, NC), F32),
                pltpu.VMEM((NOUT, BLK, NC), BF16),
                dma((NK,)), dma((3 * HEADS,)), dma((NOUT,)),
                dma((3, NK)), dma((3, NK)),
                dma((2, NK)), dma((2, NK)),
                dma((2, NK)), dma((2, NK)),
                dma((2, NK)), dma((2, NK)),
                dma((8,)), dma((2, 4)),
                dma((NOUT,)), dma((NOUT,)), dma((NOUT,)),
            ],
            compiler_params=pltpu.CompilerParams(collective_id=0, has_side_effects=True, vmem_limit_bytes=67043328),
        )(x_loc, *heads_major, w_o.reshape(20 * E, D))

    seq_spec = P(('dp', 'cp', 'tp'), None)
    head_spec = P(None, 'tp', None)
    return jax.shard_map(device_fn, mesh=mesh, in_specs=(seq_spec, head_spec, head_spec, head_spec, P('tp', None, None)), out_specs=seq_spec, check_vma=False)
```

```python
import functools

import jax
import jax.numpy as jnp
from jax import lax
from jax.experimental import pallas as pl
from jax.experimental.pallas import tpu as pltpu
from jax.sharding import PartitionSpec as P


BF16, F32 = jnp.bfloat16, jnp.float32
NEG_BIG = -1e30
D = 5120
E = 128
HEADS = 5
HE = HEADS * E
NQKV = 3 * HE
BLK = 64
NK = 4
KC = D // NK
NOUT = 10
NC = D // NOUT
MESH = pl.DeviceIdType.MESH


def remote(src, dst, send_sem, recv_sem, dev):
    return pltpu.make_async_remote_copy(src_ref=src, dst_ref=dst, send_sem=send_sem, recv_sem=recv_sem, device_id=dev, device_id_type=MESH)


def kernel(x_hbm, wq_hbm, wk_hbm, wv_hbm, wo_hbm, y_hbm, xs, w, wo, qkv, acc, osend, ofull, ysend, yrecv, yout,
           xin_sem, w_sem, wo_sem, own_send, own_recv, fwd_send, fwd_recv, dg_send, dg_recv, dgf_send, dgf_recv, o_send_sem, o_recv_sem,
           y_send_sem, y_recv_sem, out_sem):
    cp, tp = lax.axis_index('cp'), lax.axis_index('tp')
    x, c = cp // 2, cp % 2
    sib = {'cp': 2 * x + 1 - c, 'tp': tp}
    xn = {'cp': 2 * (1 - x) + c, 'tp': tp}
    xo = {'cp': 2 * (1 - x) + 1 - c, 'tp': tp}
    yn = {'cp': cp, 'tp': 1 - tp}

    def rows(group, core, first=0, n=BLK):
        return pl.ds(pl.multiple_of(group * 128 + core * BLK + first, 32), n)

    def x_in(k):
        return pltpu.make_async_copy(x_hbm.at[:, pl.ds(k * KC, KC)], xs.at[k, rows(0, c), :], xin_sem.at[k])

    for k in range(NK):
        x_in(k).start()

    def w_in(j):
        src = (wq_hbm, wk_hbm, wv_hbm)[j // HEADS].at[cp * HEADS + j % HEADS]
        return pltpu.make_async_copy(src, w.at[:, pl.ds(j * E, E)], w_sem.at[j])

    def wo_in(n):
        return pltpu.make_async_copy(wo_hbm.at[:, pl.ds(n * NC, NC)], wo.at[n], wo_sem.at[n])

    barrier = pltpu.get_barrier_semaphore()
    for dev in (sib, xn, xo, yn):
        pl.semaphore_signal(barrier, inc=1, device_id=dev, device_id_type=MESH)
    for k in range(NK):
        x_in(k).wait()
    for j in range(3 * HEADS):
        w_in(j).start()
    with jax.named_scope('barrier'):
        pl.semaphore_wait(barrier, 4)

    def own(k, which):
        dev, group = ((xn, 1), (yn, 2), (sib, 0))[which]
        return remote(xs.at[k, rows(0, c), :], xs.at[k, rows(group, c), :], own_send.at[which, k], own_recv.at[which, k], dev)

    def fwd(k, which):
        return remote(xs.at[k, rows(1 + which, c), :], xs.at[k, rows(1 + which, c), :], fwd_send.at[which, k], fwd_recv.at[which, k], sib)

    def diag(k, which):
        dev = (yn, xn)[which]
        return remote(xs.at[k, rows(1 + which, c, 32 * which, 32), :], xs.at[k, rows(3, c, 32 * which, 32), :],
                      dg_send.at[which, k], dg_recv.at[which, k], dev)

    def diag_fwd(k, which):
        sl = rows(3, c, 32 * which, 32)
        return remote(xs.at[k, sl, :], xs.at[k, sl, :], dgf_send.at[which, k], dgf_recv.at[which, k], sib)

    for k in range(NK):
        for which in range(3):
            own(k, which).start()

    def nat(xx, core, t):
        b = 2 * xx + core
        return jnp.where(t == 0, b, 7 - b) * BLK

    nat_of = [nat(x, 0, tp), nat(x, 1, tp), nat(1 - x, 0, tp), nat(1 - x, 1, tp),
              nat(x, 0, 1 - tp), nat(x, 1, 1 - tp), nat(1 - x, 0, 1 - tp), nat(1 - x, 1, 1 - tp)]

    def put_qkv(slot, col, n, val):
        qkv[pl.ds(pl.multiple_of(nat_of[slot], BLK), BLK), pl.ds(col, n)] = val.astype(BF16)

    NSTEPS = ((0, 512), (512, 512), (1024, 512), (1536, 384))

    with jax.named_scope('wait_sib'):
        for k in range(NK):
            own(k, 2).wait_recv()
    with jax.named_scope('wait_w'):
        for j in range(3 * HEADS):
            w_in(j).wait()
    for n in range(NOUT):
        wo_in(n).start()

    for col, n in NSTEPS:
        val = jnp.dot(xs[0, 0:128, :], w[0:KC, col:col + n], preferred_element_type=F32)
        for k in range(1, NK):
            val += jnp.dot(xs[k, 0:128, :], w[k * KC:(k + 1) * KC, col:col + n], preferred_element_type=F32)
        put_qkv(0, col, n, val[:BLK])
        put_qkv(1, col, n, val[BLK:])

    acc[...] = jnp.zeros_like(acc)

    def accumulate(k, row, m, arow):
        kk = pl.ds(pl.multiple_of(k * KC, KC), KC)
        for col, n in NSTEPS:
            acc[arow:arow + m, col:col + n] += jnp.dot(xs[k, row:row + m, :], w[kk, col:col + n], preferred_element_type=F32)

    @pl.loop(0, NK)
    def _(k):
        for which in range(2):
            with jax.named_scope(f'wait_own{which}'):
                own(k, which).wait_recv()
            diag(k, which).start()
            fwd(k, which).start()
        for which in range(2):
            with jax.named_scope(f'wait_fwd{which}'):
                fwd(k, which).wait_recv()
        with jax.named_scope('acc_nbr'):
            accumulate(k, 128, 256, 0)

    for col, n in NSTEPS:
        for s in range(4):
            put_qkv(2 + s, col, n, acc[s * BLK:(s + 1) * BLK, col:col + n])

    @pl.loop(0, NK)
    def _(k):
        for which in range(2):
            with jax.named_scope(f'wait_diag{which}'):
                diag(k, which).wait_recv()
            diag_fwd(k, which).start()
        for which in range(2):
            with jax.named_scope(f'wait_dgf{which}'):
                diag_fwd(k, which).wait_recv()
        with jax.named_scope('acc_diag'):
            accumulate(k, 384, 128, 256)

    for col, n in NSTEPS:
        for s in range(2):
            put_qkv(6 + s, col, n, acc[256 + s * BLK:256 + (s + 1) * BLK, col:col + n])

    inv_sqrt = E ** -0.5

    def o_copy(b, dev_cp):
        lohi = b // 4
        return remote(osend.at[b], ofull.at[lohi, :, pl.ds(pl.multiple_of(cp * HE, E), HE)],
                      o_send_sem.at[b], o_recv_sem.at[lohi, (cp - dev_cp + 4) % 4], {'cp': dev_cp, 'tp': tp})

    def attend(i):
        length = 128 * (i + 1)
        ri = lax.broadcasted_iota(jnp.int32, (128, 128), 0)
        ci = lax.broadcasted_iota(jnp.int32, (128, 128), 1)
        mask = ci <= ri
        for h in range(HEADS):
            q = qkv[i * 128:(i + 1) * 128, h * E:(h + 1) * E]
            kk = qkv[0:length, HE + h * E:HE + (h + 1) * E]
            v = qkv[0:length, 2 * HE + h * E:2 * HE + (h + 1) * E]
            s = lax.dot_general(q, kk, (((1,), (1,)), ((), ())), preferred_element_type=F32) * inv_sqrt
            last = jnp.where(mask, s[:, length - 128:], NEG_BIG)
            s = last if i == 0 else jnp.concatenate([s[:, :length - 128], last], axis=1)
            m = jnp.max(s, axis=-1, keepdims=True)
            p = jnp.exp(s - m)
            l = jnp.sum(p, axis=-1, keepdims=True)
            o = (jnp.dot(p.astype(BF16), v, preferred_element_type=F32) / l).astype(BF16)
            osend[2 * i, :, h * E:(h + 1) * E] = o[:BLK]
            osend[2 * i + 1, :, h * E:(h + 1) * E] = o[BLK:]
        for b in (2 * i, 2 * i + 1):
            r = b if b < 4 else 7 - b

            @pl.when(cp == r)
            def _():
                ofull[b // 4, :, pl.ds(pl.multiple_of(cp * HE, E), HE)] = osend[b]

            @pl.when(cp != r)
            def _():
                o_copy(b, r).start()

    def wait_o(lohi):
        for d in range(1, 4):
            remote(osend.at[0], ofull.at[0, :, pl.ds(0, HE)], o_send_sem.at[0], o_recv_sem.at[lohi, d], sib).wait_recv()

    @pl.loop(0, 4)
    def _(step):
        hi = (tp + step // 2) % 2 == 0
        other = step % 2 == 0
        pair = jnp.where(hi, jnp.where(other, 2 + x, 3 - x), jnp.where(other, 1 - x, x))
        for i in range(4):
            @pl.when(pair == i)
            def _():
                with jax.named_scope(f'attend{i}'):
                    attend(i)

    away, home = 1 - tp, tp

    def y_copy(n):
        return remote(ysend.at[n], yrecv.at[n], y_send_sem.at[n], y_recv_sem.at[n], yn)

    with jax.named_scope('wait_o_away'):
        wait_o(away)

    @pl.loop(0, NOUT)
    def _(n):
        with jax.named_scope('wait_wo'):
            wo_in(n).wait()
        ysend[n] = jnp.dot(ofull[away], wo[n], preferred_element_type=F32)
        y_copy(n).start()

    with jax.named_scope('wait_o_home'):
        wait_o(home)

    def out_copy(n):
        return pltpu.make_async_copy(yout.at[n], y_hbm.at[:, pl.ds(pl.multiple_of(n * NC, NC), NC)], out_sem.at[n])

    @pl.loop(0, NOUT)
    def _(n):
        part = jnp.dot(ofull[home], wo[n], preferred_element_type=F32)
        with jax.named_scope('wait_y'):
            y_copy(n).wait_recv()
        yout[n] = (part + yrecv[n]).astype(BF16)
        out_copy(n).start()

    @pl.loop(0, NK)
    def _(k):
        for which in range(3):
            own(k, which).wait_send()
        for which in range(2):
            fwd(k, which).wait_send()
            diag(k, which).wait_send()
            diag_fwd(k, which).wait_send()

    for b in range(8):
        r = b if b < 4 else 7 - b

        @pl.when(cp != r)
        def _():
            o_copy(b, r).wait_send()

    @pl.loop(0, NOUT)
    def _(n):
        with jax.named_scope('tail'):
            y_copy(n).wait_send()
            out_copy(n).wait()


def solution(mesh):
    def device_fn(x_loc, w_q, w_k, w_v, w_o):
        dma = pltpu.SemaphoreType.DMA
        heads_major = [jnp.transpose(t, (1, 0, 2)) for t in (w_q, w_k, w_v)]
        return pl.pallas_call(
            kernel,
            name='attention_layer',
            out_shape=jax.ShapeDtypeStruct((BLK, D), BF16),
            in_specs=[pl.BlockSpec(memory_space=pl.ANY)] * 5,
            out_specs=pl.BlockSpec(memory_space=pl.ANY),
            scratch_shapes=[
                pltpu.VMEM((NK, 512, KC), BF16),
                pltpu.VMEM((D, NQKV), BF16),
                pltpu.VMEM((NOUT, 20 * E, NC), BF16),
                pltpu.VMEM((512, NQKV), BF16),
                pltpu.VMEM((384, NQKV), F32),
                pltpu.VMEM((8, BLK, HE), BF16),
                pltpu.VMEM((2, BLK, 20 * E), BF16),
                pltpu.VMEM((NOUT, BLK, NC), F32),
                pltpu.VMEM((NOUT, BLK, NC), F32),
                pltpu.VMEM((NOUT, BLK, NC), BF16),
                dma((NK,)), dma((3 * HEADS,)), dma((NOUT,)),
                dma((3, NK)), dma((3, NK)),
                dma((2, NK)), dma((2, NK)),
                dma((2, NK)), dma((2, NK)),
                dma((2, NK)), dma((2, NK)),
                dma((8,)), dma((2, 4)),
                dma((NOUT,)), dma((NOUT,)), dma((NOUT,)),
            ],
            compiler_params=pltpu.CompilerParams(collective_id=0, has_side_effects=True, vmem_limit_bytes=67043328),
        )(x_loc, *heads_major, w_o.reshape(20 * E, D))

    seq_spec = P(('dp', 'cp', 'tp'), None)
    head_spec = P(None, 'tp', None)
    return jax.shard_map(device_fn, mesh=mesh, in_specs=(seq_spec, head_spec, head_spec, head_spec, P('tp', None, None)), out_specs=seq_spec, check_vma=False)
```

```python
import functools

import jax
import jax.numpy as jnp
from jax import lax
from jax.experimental import pallas as pl
from jax.experimental.pallas import tpu as pltpu
from jax.sharding import PartitionSpec as P


BF16, F32 = jnp.bfloat16, jnp.float32
NEG_BIG = -1e30
D = 5120
E = 128
HEADS = 5
HE = HEADS * E
NQKV = 3 * HE
BLK = 64
NK = 10
KC = D // NK
LATE = NK // 2
DIAG_X = 7
NOUT = 10
NC = D // NOUT
MESH = pl.DeviceIdType.MESH


def remote(src, dst, send_sem, recv_sem, dev):
    return pltpu.make_async_remote_copy(src_ref=src, dst_ref=dst, send_sem=send_sem, recv_sem=recv_sem, device_id=dev, device_id_type=MESH)


def kernel(x_hbm, wq_hbm, wk_hbm, wv_hbm, wo_hbm, y_hbm, xs, w, wo, qkv, acc, osend, ofull, ysend, yrecv, yout,
           xin_sem, w_sem, wo_sem, own_send, direct_recv, fwd_send, fwd_recv, dg_send, o_send_sem, o_recv_sem,
           y_send_sem, y_recv_sem, out_sem):
    cp, tp = lax.axis_index('cp'), lax.axis_index('tp')
    x, c = cp // 2, cp % 2
    sib = {'cp': 2 * x + 1 - c, 'tp': tp}
    xn = {'cp': 2 * (1 - x) + c, 'tp': tp}
    xo = {'cp': 2 * (1 - x) + 1 - c, 'tp': tp}
    yn = {'cp': cp, 'tp': 1 - tp}

    def rows(group, core):
        return pl.ds(pl.multiple_of(group * 128 + core * BLK, BLK), BLK)

    def x_in(k):
        return pltpu.make_async_copy(x_hbm.at[:, pl.ds(k * KC, KC)], xs.at[k, rows(0, c), :], xin_sem.at[k])

    def w_in(j):
        src = (wq_hbm, wk_hbm, wv_hbm)[j // HEADS].at[cp * HEADS + j % HEADS]
        return pltpu.make_async_copy(src, w.at[:, pl.ds(j * E, E)], w_sem.at[j])

    def wo_in(n):
        return pltpu.make_async_copy(wo_hbm.at[:, pl.ds(n * NC, NC)], wo.at[n], wo_sem.at[n])

    for k in range(NK):
        x_in(k).start()
    barrier = pltpu.get_barrier_semaphore()
    for dev in (sib, xn, xo, yn):
        pl.semaphore_signal(barrier, inc=1, device_id=dev, device_id_type=MESH)
    for k in range(NK):
        x_in(k).wait()
    for j in range(3 * HEADS):
        w_in(j).start()
    with jax.named_scope('barrier'):
        pl.semaphore_wait(barrier, 4)

    def group_of(kind, t):
        return (1, 2 + t, 3 - t, 0)[kind]

    def own(k, kind):
        dev, t = ((yn, 1 - tp), (xn, tp), None, (sib, tp))[kind]
        return remote(xs.at[k, rows(0, c), :], xs.at[k, rows(group_of(kind, t), c), :], own_send.at[kind, k], direct_recv.at[kind, k], dev)

    def diag(k, over_y):
        dev, src, t = (yn, group_of(1, tp), 1 - tp) if over_y else (xn, group_of(0, tp), tp)
        return remote(xs.at[k, rows(src, c), :], xs.at[k, rows(group_of(2, t), c), :], dg_send.at[int(over_y), k], direct_recv.at[2, k], dev)

    def fwd(k, kind):
        sl = rows(group_of(kind, tp), c)
        return remote(xs.at[k, sl, :], xs.at[k, sl, :], fwd_send.at[kind, k], fwd_recv.at[kind, k], sib)

    def direct_wait(k, kind):
        sl = rows(group_of(kind, tp), c)
        remote(xs.at[k, sl, :], xs.at[k, sl, :], own_send.at[kind, k], direct_recv.at[kind, k], sib).wait_recv()

    def sends_diag_x(k):
        return jnp.where(tp == 0, k >= LATE, k < DIAG_X)

    def sends_diag_y(k):
        return jnp.where(tp == 0, k >= DIAG_X, k < LATE)

    def handle(k, kind):
        direct_wait(k, kind)
        fwd(k, kind).start()
        if kind == 0:
            @pl.when(sends_diag_x(k))
            def _():
                diag(k, False).start()
        if kind == 1:
            @pl.when(sends_diag_y(k))
            def _():
                diag(k, True).start()

    for k in range(NK):
        if k < LATE:
            own(k, 1).start()
        else:
            @pl.when(tp == 0)
            def _():
                own(k, 1).start()
        own(k, 0).start()
        own(k, 3).start()

    acc[...] = jnp.zeros_like(acc)

    def nat(xx, core, t):
        b = 2 * xx + core
        return jnp.where(t == 0, b, 7 - b) * BLK

    nat_of = [nat(x, 0, tp), nat(x, 1, tp), nat(x, 0, 1 - tp), nat(x, 1, 1 - tp),
              nat(1 - x, 0, 0), nat(1 - x, 1, 0), nat(1 - x, 0, 1), nat(1 - x, 1, 1)]

    def put_qkv(slot, col, n, val):
        qkv[pl.ds(pl.multiple_of(nat_of[slot], BLK), BLK), pl.ds(col, n)] = val.astype(BF16)

    NSTEPS = ((0, 512), (512, 512), (1024, 512), (1536, 384))

    def own_chip():
        with jax.named_scope('wait_sib'):
            for k in range(NK):
                direct_wait(k, 3)
        with jax.named_scope('wait_w'):
            for j in range(3 * HEADS):
                w_in(j).wait()
        for n in range(NOUT):
            wo_in(n).start()
        for col, n in NSTEPS:
            val = jnp.dot(xs[0, 0:128, :], w[0:KC, col:col + n], preferred_element_type=F32)
            for k in range(1, NK):
                val += jnp.dot(xs[k, 0:128, :], w[k * KC:(k + 1) * KC, col:col + n], preferred_element_type=F32)
            put_qkv(0, col, n, val[:BLK])
            put_qkv(1, col, n, val[BLK:])

    def accumulate(k, row, m, arow):
        kk = pl.ds(pl.multiple_of(k * KC, KC), KC)
        for col, n in NSTEPS:
            acc[arow:arow + m, col:col + n] += jnp.dot(xs[k, row:row + m, :], w[kk, col:col + n], preferred_element_type=F32)

    lag = jnp.where(tp == 0, 3, 6)

    @pl.loop(0, NK + 6)
    def _(i):
        @pl.when(i < NK)
        def _():
            with jax.named_scope('h_y'):
                handle(i, 0)

        @pl.when(i < jnp.where(tp == 0, NK, LATE))
        def _():
            with jax.named_scope('h_x'):
                handle(i, 1)

        @pl.when((tp == 1) & (i == DIAG_X - 1))
        def _():
            for k in range(LATE, NK):
                own(k, 1).start()

        @pl.when((tp == 1) & (i >= 5) & (i < NK + 5))
        def _():
            with jax.named_scope('h_d'):
                handle(i - 5, 2)

        @pl.when(i == 2)
        def _():
            own_chip()

        @pl.when((i >= lag) & (i < NK + lag))
        def _():
            k = i - lag
            with jax.named_scope('w_fwd'):
                fwd(k, 0).wait_recv()

                @pl.when(tp == 0)
                def _():
                    fwd(k, 1).wait_recv()

                @pl.when(tp == 1)
                def _():
                    fwd(k, 2).wait_recv()
            with jax.named_scope('acc_a'):
                accumulate(k, 128, 256, 0)

    for col, n in NSTEPS:
        for s in range(4):
            put_qkv(2 + s, col, n, acc[s * BLK:(s + 1) * BLK, col:col + n])

    def rest_of_rows():
        @pl.loop(0, LATE + 1)
        def _(j):
            @pl.when((tp == 0) & (j < LATE))
            def _():
                with jax.named_scope('h_d2'):
                    handle(j, 2)
                    handle(j + LATE, 2)

            @pl.when((tp == 1) & (j < LATE))
            def _():
                with jax.named_scope('h_x2'):
                    handle(j + LATE, 1)

            @pl.when(j > 0)
            def _():
                with jax.named_scope('w_fwd2'):
                    for k in (j - 1, j - 1 + LATE):
                        @pl.when(tp == 0)
                        def _():
                            fwd(k, 2).wait_recv()

                        @pl.when(tp == 1)
                        def _():
                            fwd(k, 1).wait_recv()
                with jax.named_scope('acc_b'):
                    @pl.loop(0, 2)
                    def _(h):
                        accumulate(j - 1 + h * LATE, 384, 128, 256)

        for col, n in NSTEPS:
            for s in range(2):
                put_qkv(6 + s, col, n, acc[256 + s * BLK:256 + (s + 1) * BLK, col:col + n])

    inv_sqrt = E ** -0.5

    def o_copy(b, dev_cp):
        lohi = b // 4
        return remote(osend.at[b], ofull.at[lohi, :, pl.ds(pl.multiple_of(cp * HE, E), HE)],
                      o_send_sem.at[b], o_recv_sem.at[lohi, (cp - dev_cp + 4) % 4], {'cp': dev_cp, 'tp': tp})

    def attend(i):
        length = 128 * (i + 1)
        ri = lax.broadcasted_iota(jnp.int32, (128, 128), 0)
        ci = lax.broadcasted_iota(jnp.int32, (128, 128), 1)
        mask = ci <= ri
        for h in range(HEADS):
            q = qkv[i * 128:(i + 1) * 128, h * E:(h + 1) * E]
            kk = qkv[0:length, HE + h * E:HE + (h + 1) * E]
            v = qkv[0:length, 2 * HE + h * E:2 * HE + (h + 1) * E]
            s = lax.dot_general(q, kk, (((1,), (1,)), ((), ())), preferred_element_type=F32) * inv_sqrt
            last = jnp.where(mask, s[:, length - 128:], NEG_BIG)
            s = last if i == 0 else jnp.concatenate([s[:, :length - 128], last], axis=1)
            m = jnp.max(s, axis=-1, keepdims=True)
            p = jnp.exp(s - m)
            l = jnp.sum(p, axis=-1, keepdims=True)
            o = (jnp.dot(p.astype(BF16), v, preferred_element_type=F32) / l).astype(BF16)
            osend[2 * i, :, h * E:(h + 1) * E] = o[:BLK]
            osend[2 * i + 1, :, h * E:(h + 1) * E] = o[BLK:]
        for b in (2 * i, 2 * i + 1):
            r = b if b < 4 else 7 - b

            @pl.when(cp == r)
            def _():
                ofull[b // 4, :, pl.ds(pl.multiple_of(cp * HE, E), HE)] = osend[b]

            @pl.when(cp != r)
            def _():
                o_copy(b, r).start()

    def wait_o(lohi):
        for d in range(1, 4):
            remote(osend.at[0], ofull.at[0, :, pl.ds(0, HE)], o_send_sem.at[0], o_recv_sem.at[lohi, d], sib).wait_recv()

    def attend_pairs(hi):
        @pl.loop(0, 2)
        def _(step):
            pair = jnp.where(hi, jnp.where(step == 0, 2 + x, 3 - x), jnp.where(step == 0, 1 - x, x))
            for i in range(4):
                @pl.when(pair == i)
                def _():
                    with jax.named_scope(f'attend{i}'):
                        attend(i)

    away, home = 1 - tp, tp

    def y_copy(n):
        return remote(ysend.at[n], yrecv.at[n], y_send_sem.at[n], y_recv_sem.at[n], yn)

    def project_away():
        with jax.named_scope('wait_o_away'):
            wait_o(away)

        @pl.loop(0, NOUT)
        def _(n):
            wo_in(n).wait()
            with jax.named_scope('proj'):
                ysend[n] = jnp.dot(ofull[away], wo[n], preferred_element_type=F32)
            y_copy(n).start()

    @pl.loop(0, 4)
    def _(stage):
        @pl.when(stage == 2 * tp)
        def _():
            rest_of_rows()

        @pl.when((stage == 1 - tp) | (stage == 2 + tp))
        def _():
            attend_pairs((stage < 2) == (tp == 0))

        @pl.when(stage == 3 - 2 * tp)
        def _():
            project_away()

    with jax.named_scope('wait_o_home'):
        wait_o(home)

    def out_copy(n):
        return pltpu.make_async_copy(yout.at[n], y_hbm.at[:, pl.ds(pl.multiple_of(n * NC, NC), NC)], out_sem.at[n])

    @pl.loop(0, NOUT)
    def _(n):
        part = jnp.dot(ofull[home], wo[n], preferred_element_type=F32)
        with jax.named_scope('wait_y'):
            y_copy(n).wait_recv()
        yout[n] = (part + yrecv[n]).astype(BF16)
        out_copy(n).start()

    @pl.loop(0, NK)
    def _(k):
        for kind in (0, 1, 3):
            own(k, kind).wait_send()
        for kind in (0, 1, 2):
            fwd(k, kind).wait_send()

        @pl.when(sends_diag_x(k))
        def _():
            diag(k, False).wait_send()

        @pl.when(sends_diag_y(k))
        def _():
            diag(k, True).wait_send()

    for b in range(8):
        r = b if b < 4 else 7 - b

        @pl.when(cp != r)
        def _():
            o_copy(b, r).wait_send()

    @pl.loop(0, NOUT)
    def _(n):
        with jax.named_scope('tail'):
            y_copy(n).wait_send()
            out_copy(n).wait()


def solution(mesh):
    def device_fn(x_loc, w_q, w_k, w_v, w_o):
        dma = pltpu.SemaphoreType.DMA
        heads_major = [jnp.transpose(t, (1, 0, 2)) for t in (w_q, w_k, w_v)]
        return pl.pallas_call(
            kernel,
            name='attention_layer',
            out_shape=jax.ShapeDtypeStruct((BLK, D), BF16),
            in_specs=[pl.BlockSpec(memory_space=pl.ANY)] * 5,
            out_specs=pl.BlockSpec(memory_space=pl.ANY),
            scratch_shapes=[
                pltpu.VMEM((NK, 512, KC), BF16),
                pltpu.VMEM((D, NQKV), BF16),
                pltpu.VMEM((NOUT, 20 * E, NC), BF16),
                pltpu.VMEM((512, NQKV), BF16),
                pltpu.VMEM((384, NQKV), F32),
                pltpu.VMEM((8, BLK, HE), BF16),
                pltpu.VMEM((2, BLK, 20 * E), BF16),
                pltpu.VMEM((NOUT, BLK, NC), F32),
                pltpu.VMEM((NOUT, BLK, NC), F32),
                pltpu.VMEM((NOUT, BLK, NC), BF16),
                dma((NK,)), dma((3 * HEADS,)), dma((NOUT,)),
                dma((4, NK)), dma((4, NK)),
                dma((3, NK)), dma((3, NK)),
                dma((2, NK)),
                dma((8,)), dma((2, 4)),
                dma((NOUT,)), dma((NOUT,)), dma((NOUT,)),
            ],
            compiler_params=pltpu.CompilerParams(collective_id=0, has_side_effects=True, vmem_limit_bytes=67043328),
        )(x_loc, *heads_major, w_o.reshape(20 * E, D))

    seq_spec = P(('dp', 'cp', 'tp'), None)
    head_spec = P(None, 'tp', None)
    return jax.shard_map(device_fn, mesh=mesh, in_specs=(seq_spec, head_spec, head_spec, head_spec, P('tp', None, None)), out_specs=seq_spec, check_vma=False)
```

```python
import functools

import jax
import jax.numpy as jnp
from jax import lax
from jax.experimental import pallas as pl
from jax.experimental.pallas import tpu as pltpu
from jax.sharding import PartitionSpec as P


BF16, F32 = jnp.bfloat16, jnp.float32
NEG_BIG = -1e30
D = 5120
E = 128
HEADS = 5
HE = HEADS * E
NQKV = 3 * HE
BLK = 64
NK = 10
KC = D // NK
LATE = NK // 2
DIAG_X = 7
NOUT = 10
NC = D // NOUT
MESH = pl.DeviceIdType.MESH


def remote(src, dst, send_sem, recv_sem, dev):
    return pltpu.make_async_remote_copy(src_ref=src, dst_ref=dst, send_sem=send_sem, recv_sem=recv_sem, device_id=dev, device_id_type=MESH)


def kernel(x_hbm, wq_hbm, wk_hbm, wv_hbm, wo_hbm, y_ref, xs, w, wo, qkv, acc, osend, ofull, ysend, yrecv,
           xin_sem, w_sem, wo_sem, own_send, direct_recv, fwd_send, fwd_recv, dg_send, o_send_sem, o_recv_sem,
           y_send_sem, y_recv_sem):
    cp, tp = lax.axis_index('cp'), lax.axis_index('tp')
    x, c = cp // 2, cp % 2
    sib = {'cp': 2 * x + 1 - c, 'tp': tp}
    xn = {'cp': 2 * (1 - x) + c, 'tp': tp}
    xo = {'cp': 2 * (1 - x) + 1 - c, 'tp': tp}
    yn = {'cp': cp, 'tp': 1 - tp}

    def rows(group, core):
        return pl.ds(pl.multiple_of(group * 128 + core * BLK, BLK), BLK)

    def x_in(k):
        return pltpu.make_async_copy(x_hbm.at[:, pl.ds(k * KC, KC)], xs.at[k, rows(0, c), :], xin_sem.at[k])

    def w_in(j):
        src = (wq_hbm, wk_hbm, wv_hbm)[j // HEADS].at[cp * HEADS + j % HEADS]
        return pltpu.make_async_copy(src, w.at[:, pl.ds(j * E, E)], w_sem.at[j])

    def wo_in(n):
        return pltpu.make_async_copy(wo_hbm.at[:, pl.ds(n * NC, NC)], wo.at[n], wo_sem.at[n])

    for k in range(NK):
        x_in(k).start()
    barrier = pltpu.get_barrier_semaphore()
    for dev in (sib, xn, xo, yn):
        pl.semaphore_signal(barrier, inc=1, device_id=dev, device_id_type=MESH)
    for k in range(NK):
        x_in(k).wait()
    for j in range(3 * HEADS):
        w_in(j).start()
    with jax.named_scope('barrier'):
        pl.semaphore_wait(barrier, 4)

    def group_of(kind, t):
        return (1, 2 + t, 3 - t, 0)[kind]

    def own(k, kind):
        dev, t = ((yn, 1 - tp), (xn, tp), None, (sib, tp))[kind]
        return remote(xs.at[k, rows(0, c), :], xs.at[k, rows(group_of(kind, t), c), :], own_send.at[kind, k], direct_recv.at[kind, k], dev)

    def diag(k, over_y):
        dev, src, t = (yn, group_of(1, tp), 1 - tp) if over_y else (xn, group_of(0, tp), tp)
        return remote(xs.at[k, rows(src, c), :], xs.at[k, rows(group_of(2, t), c), :], dg_send.at[int(over_y), k], direct_recv.at[2, k], dev)

    def fwd(k, kind):
        sl = rows(group_of(kind, tp), c)
        return remote(xs.at[k, sl, :], xs.at[k, sl, :], fwd_send.at[kind, k], fwd_recv.at[kind, k], sib)

    def direct_wait(k, kind):
        sl = rows(group_of(kind, tp), c)
        remote(xs.at[k, sl, :], xs.at[k, sl, :], own_send.at[kind, k], direct_recv.at[kind, k], sib).wait_recv()

    def sends_diag_x(k):
        return jnp.where(tp == 0, k >= LATE, k < DIAG_X)

    def sends_diag_y(k):
        return jnp.where(tp == 0, k >= DIAG_X, k < LATE)

    def handle(k, kind):
        direct_wait(k, kind)
        fwd(k, kind).start()
        if kind == 0:
            @pl.when(sends_diag_x(k))
            def _():
                diag(k, False).start()
        if kind == 1:
            @pl.when(sends_diag_y(k))
            def _():
                diag(k, True).start()

    for k in range(NK):
        if k < LATE:
            own(k, 1).start()
        else:
            @pl.when(tp == 0)
            def _():
                own(k, 1).start()
        own(k, 0).start()
        own(k, 3).start()

    acc[...] = jnp.zeros_like(acc)

    def nat(xx, core, t):
        b = 2 * xx + core
        return jnp.where(t == 0, b, 7 - b) * BLK

    nat_of = [nat(x, 0, tp), nat(x, 1, tp), nat(x, 0, 1 - tp), nat(x, 1, 1 - tp),
              nat(1 - x, 0, 0), nat(1 - x, 1, 0), nat(1 - x, 0, 1), nat(1 - x, 1, 1)]

    def put_qkv(slot, col, n, val):
        qkv[pl.ds(pl.multiple_of(nat_of[slot], BLK), BLK), pl.ds(col, n)] = val.astype(BF16)

    NSTEPS = ((0, 512), (512, 512), (1024, 512), (1536, 384))

    def own_chip():
        with jax.named_scope('wait_sib'):
            for k in range(NK):
                direct_wait(k, 3)
        with jax.named_scope('wait_w'):
            for j in range(3 * HEADS):
                w_in(j).wait()
        for n in range(NOUT):
            wo_in(n).start()
        for col, n in NSTEPS:
            val = jnp.dot(xs[0, 0:128, :], w[0:KC, col:col + n], preferred_element_type=F32)
            for k in range(1, NK):
                val += jnp.dot(xs[k, 0:128, :], w[k * KC:(k + 1) * KC, col:col + n], preferred_element_type=F32)
            put_qkv(0, col, n, val[:BLK])
            put_qkv(1, col, n, val[BLK:])

    def accumulate(chunks, row, m, arow):
        for col, n in NSTEPS:
            val = acc[arow:arow + m, col:col + n]
            for k in chunks:
                val += jnp.dot(xs[k, row:row + m, :], w[pl.ds(pl.multiple_of(k * KC, KC), KC), col:col + n], preferred_element_type=F32)
            acc[arow:arow + m, col:col + n] = val

    lag = jnp.where(tp == 0, 3, 6)

    @pl.loop(0, NK + 6)
    def _(i):
        @pl.when(i < NK)
        def _():
            with jax.named_scope('h_y'):
                handle(i, 0)

        @pl.when(i < jnp.where(tp == 0, NK, LATE))
        def _():
            with jax.named_scope('h_x'):
                handle(i, 1)

        @pl.when((tp == 1) & (i == DIAG_X - 1))
        def _():
            for k in range(LATE, NK):
                own(k, 1).start()

        @pl.when((tp == 1) & (i >= 5) & (i < NK + 5))
        def _():
            with jax.named_scope('h_d'):
                handle(i - 5, 2)

        @pl.when(i == 2)
        def _():
            own_chip()

        @pl.when((i >= lag) & (i < NK + lag))
        def _():
            k = i - lag
            with jax.named_scope('w_fwd'):
                fwd(k, 0).wait_recv()

                @pl.when(tp == 0)
                def _():
                    fwd(k, 1).wait_recv()

                @pl.when(tp == 1)
                def _():
                    fwd(k, 2).wait_recv()
            with jax.named_scope('acc_a'):
                accumulate((k,), 128, 256, 0)

    for col, n in NSTEPS:
        for s in range(4):
            put_qkv(2 + s, col, n, acc[s * BLK:(s + 1) * BLK, col:col + n])

    def rest_of_rows():
        @pl.loop(0, LATE + 1)
        def _(j):
            @pl.when((tp == 0) & (j < LATE))
            def _():
                with jax.named_scope('h_d2'):
                    handle(j, 2)
                    handle(j + LATE, 2)

            @pl.when((tp == 1) & (j < LATE))
            def _():
                with jax.named_scope('h_x2'):
                    handle(j + LATE, 1)

            @pl.when(j > 0)
            def _():
                with jax.named_scope('w_fwd2'):
                    for k in (j - 1, j - 1 + LATE):
                        @pl.when(tp == 0)
                        def _():
                            fwd(k, 2).wait_recv()

                        @pl.when(tp == 1)
                        def _():
                            fwd(k, 1).wait_recv()
                with jax.named_scope('acc_b'):
                    accumulate((j - 1, j - 1 + LATE), 384, 128, 256)

        for col, n in NSTEPS:
            for s in range(2):
                put_qkv(6 + s, col, n, acc[256 + s * BLK:256 + (s + 1) * BLK, col:col + n])

    inv_sqrt = E ** -0.5

    def o_copy(b, dev_cp):
        lohi = b // 4
        return remote(osend.at[b], ofull.at[lohi, :, pl.ds(pl.multiple_of(cp * HE, E), HE)],
                      o_send_sem.at[b], o_recv_sem.at[lohi, (cp - dev_cp + 4) % 4], {'cp': dev_cp, 'tp': tp})

    def attend(b):
        length = 128 * (b // 2 + 1)
        ri = lax.broadcasted_iota(jnp.int32, (BLK, 128), 0) + BLK * (b % 2)
        ci = lax.broadcasted_iota(jnp.int32, (BLK, 128), 1)
        mask = ci <= ri
        heads = range(HEADS)
        q = [qkv[b * BLK:(b + 1) * BLK, h * E:(h + 1) * E] for h in heads]
        kk = [qkv[0:length, HE + h * E:HE + (h + 1) * E] for h in heads]
        v = [qkv[0:length, 2 * HE + h * E:2 * HE + (h + 1) * E] for h in heads]
        s = [lax.dot_general(q[h], kk[h], (((1,), (1,)), ((), ())), preferred_element_type=F32) * inv_sqrt for h in heads]
        last = [jnp.where(mask, s[h][:, length - 128:], NEG_BIG) for h in heads]
        s = [last[h] if length == 128 else jnp.concatenate([s[h][:, :length - 128], last[h]], axis=1) for h in heads]
        m = [jnp.max(s[h], axis=-1, keepdims=True) for h in heads]
        p = [jnp.exp(s[h] - m[h]) for h in heads]
        l = [jnp.sum(p[h], axis=-1, keepdims=True) for h in heads]
        o = [jnp.dot(p[h].astype(BF16), v[h], preferred_element_type=F32) for h in heads]
        for h in heads:
            osend[b, :, h * E:(h + 1) * E] = (o[h] / l[h]).astype(BF16)
        r = b if b < 4 else 7 - b

        @pl.when(cp == r)
        def _():
            ofull[b // 4, :, pl.ds(pl.multiple_of(cp * HE, E), HE)] = osend[b]

        @pl.when(cp != r)
        def _():
            o_copy(b, r).start()

    def wait_o(lohi):
        for d in range(1, 4):
            remote(osend.at[0], ofull.at[0, :, pl.ds(0, HE)], o_send_sem.at[0], o_recv_sem.at[lohi, d], sib).wait_recv()

    def attend_blocks(hi):
        @pl.loop(0, 4)
        def _(step):
            first = step < 2
            pair = jnp.where(hi, jnp.where(first, 2 + x, 3 - x), jnp.where(first, 1 - x, x))
            block = 2 * pair + step % 2
            for b in range(8):
                @pl.when(block == b)
                def _():
                    with jax.named_scope(f'attend{b}'):
                        attend(b)

    away, home = 1 - tp, tp

    def y_copy(n):
        return remote(ysend.at[n], yrecv.at[n], y_send_sem.at[n], y_recv_sem.at[n], yn)

    def project_away():
        with jax.named_scope('wait_o_away'):
            wait_o(away)

        @pl.loop(0, NOUT)
        def _(n):
            wo_in(n).wait()
            with jax.named_scope('proj'):
                ysend[n] = jnp.dot(ofull[away], wo[n], preferred_element_type=F32)
            y_copy(n).start()

    @pl.loop(0, 4)
    def _(stage):
        @pl.when(stage == 2 * tp)
        def _():
            rest_of_rows()

        @pl.when((stage == 1 - tp) | (stage == 2 + tp))
        def _():
            attend_blocks((stage < 2) == (tp == 0))

        @pl.when(stage == 3 - 2 * tp)
        def _():
            project_away()

    with jax.named_scope('wait_o_home'):
        wait_o(home)

    @pl.loop(0, NOUT)
    def _(n):
        part = jnp.dot(ofull[home], wo[n], preferred_element_type=F32)
        with jax.named_scope('wait_y'):
            y_copy(n).wait_recv()
        y_ref[:, pl.ds(pl.multiple_of(n * NC, NC), NC)] = (part + yrecv[n]).astype(BF16)

    @pl.loop(0, NK)
    def _(k):
        for kind in (0, 1, 3):
            own(k, kind).wait_send()
        for kind in (0, 1, 2):
            fwd(k, kind).wait_send()

        @pl.when(sends_diag_x(k))
        def _():
            diag(k, False).wait_send()

        @pl.when(sends_diag_y(k))
        def _():
            diag(k, True).wait_send()

    for b in range(8):
        r = b if b < 4 else 7 - b

        @pl.when(cp != r)
        def _():
            o_copy(b, r).wait_send()

    @pl.loop(0, NOUT)
    def _(n):
        with jax.named_scope('tail'):
            y_copy(n).wait_send()


def solution(mesh):
    def device_fn(x_loc, w_q, w_k, w_v, w_o):
        dma = pltpu.SemaphoreType.DMA
        heads_major = [jnp.transpose(t, (1, 0, 2)) for t in (w_q, w_k, w_v)]
        return pl.pallas_call(
            kernel,
            name='attention_layer',
            out_shape=pltpu.VMEM((BLK, D), BF16),
            in_specs=[pl.BlockSpec(memory_space=pl.ANY)] * 5,
            out_specs=pl.BlockSpec(memory_space=pltpu.VMEM),
            scratch_shapes=[
                pltpu.VMEM((NK, 512, KC), BF16),
                pltpu.VMEM((D, NQKV), BF16),
                pltpu.VMEM((NOUT, 20 * E, NC), BF16),
                pltpu.VMEM((512, NQKV), BF16),
                pltpu.VMEM((384, NQKV), F32),
                pltpu.VMEM((8, BLK, HE), BF16),
                pltpu.VMEM((2, BLK, 20 * E), BF16),
                pltpu.VMEM((NOUT, BLK, NC), F32),
                pltpu.VMEM((NOUT, BLK, NC), F32),
                dma((NK,)), dma((3 * HEADS,)), dma((NOUT,)),
                dma((4, NK)), dma((4, NK)),
                dma((3, NK)), dma((3, NK)),
                dma((2, NK)),
                dma((8,)), dma((2, 4)),
                dma((NOUT,)), dma((NOUT,)),
            ],
            compiler_params=pltpu.CompilerParams(collective_id=0, has_side_effects=True, vmem_limit_bytes=64 * 1000 * 1000),
        )(x_loc, *heads_major, w_o.reshape(20 * E, D))

    seq_spec = P(('dp', 'cp', 'tp'), None)
    head_spec = P(None, 'tp', None)
    return jax.shard_map(device_fn, mesh=mesh, in_specs=(seq_spec, head_spec, head_spec, head_spec, P('tp', None, None)), out_specs=seq_spec, check_vma=False)
```

```python
import functools

import jax
import jax.numpy as jnp
from jax import lax
from jax.experimental import pallas as pl
from jax.experimental.pallas import tpu as pltpu
from jax.sharding import PartitionSpec as P


BF16, F32 = jnp.bfloat16, jnp.float32
NEG_BIG = -1e30
D = 5120
E = 128
HEADS = 5
HE = HEADS * E
NQKV = 3 * HE
BLK = 64
NK = 10
KC = D // NK
LATE = NK // 2
DIAG_X = 7
NOUT = 10
NC = D // NOUT
MESH = pl.DeviceIdType.MESH


def remote(src, dst, send_sem, recv_sem, dev):
    return pltpu.make_async_remote_copy(src_ref=src, dst_ref=dst, send_sem=send_sem, recv_sem=recv_sem, device_id=dev, device_id_type=MESH)


def drain(ref, sem):
    pltpu.make_async_copy(ref, ref, sem).wait()


def kernel(x_hbm, wq_hbm, wk_hbm, wv_hbm, wo_hbm, y_ref, xs, w, wo, qkv, acc, osend, ofull, ysend, yrecv,
           xin_sem, w_sem, wo_sem, own_send, sib_recv, direct_recv, fwd_send, fwd_recv, dg_send, o_send_sem, o_recv_sem,
           y_send_sem, y_recv_sem):
    cp, tp = lax.axis_index('cp'), lax.axis_index('tp')
    x, c = cp // 2, cp % 2
    sib = {'cp': 2 * x + 1 - c, 'tp': tp}
    xn = {'cp': 2 * (1 - x) + c, 'tp': tp}
    xo = {'cp': 2 * (1 - x) + 1 - c, 'tp': tp}
    yn = {'cp': cp, 'tp': 1 - tp}

    def rows(group, core):
        return pl.ds(pl.multiple_of(group * 128 + core * BLK, BLK), BLK)

    def x_in(k):
        return pltpu.make_async_copy(x_hbm.at[:, pl.ds(k * KC, KC)], xs.at[k, rows(0, c), :], xin_sem)

    def w_in(j):
        src = (wq_hbm, wk_hbm, wv_hbm)[j // HEADS].at[cp * HEADS + j % HEADS]
        return pltpu.make_async_copy(src, w.at[:, pl.ds(j * E, E)], w_sem)

    def wo_in(n):
        return pltpu.make_async_copy(wo_hbm.at[:, pl.ds(n * NC, NC)], wo.at[n], wo_sem)

    for k in range(NK):
        x_in(k).start()
    barrier = pltpu.get_barrier_semaphore()
    for dev in (sib, xn, xo, yn):
        pl.semaphore_signal(barrier, inc=1, device_id=dev, device_id_type=MESH)
    drain(xs.at[:, rows(0, c), :], xin_sem)
    for j in range(3 * HEADS):
        w_in(j).start()
    with jax.named_scope('barrier'):
        pl.semaphore_wait(barrier, 4)

    def group_of(kind, t):
        return (1, 2 + t, 3 - t, 0)[kind]

    def own(k, kind):
        dev, t = ((yn, 1 - tp), (xn, tp), None, (sib, tp))[kind]
        return remote(xs.at[k, rows(0, c), :], xs.at[k, rows(group_of(kind, t), c), :], own_send.at[kind], sib_recv if kind == 3 else direct_recv.at[kind, k], dev)

    def diag(k, over_y):
        dev, src, t = (yn, group_of(1, tp), 1 - tp) if over_y else (xn, group_of(0, tp), tp)
        return remote(xs.at[k, rows(src, c), :], xs.at[k, rows(group_of(2, t), c), :], dg_send.at[int(over_y)], direct_recv.at[2, k], dev)

    def fwd(k, kind):
        sl = rows(group_of(kind, tp), c)
        early = (True, tp == 0, tp == 1)[kind]
        return remote(xs.at[k, sl, :], xs.at[k, sl, :], fwd_send.at[kind], fwd_recv.at[jnp.where(early, k, NK + k % LATE)], sib)

    def direct_wait(k, kind):
        drain(xs.at[k, rows(group_of(kind, tp), c), :], direct_recv.at[kind, k])

    def sends_diag_x(k):
        return jnp.where(tp == 0, k >= LATE, k < DIAG_X)

    def sends_diag_y(k):
        return jnp.where(tp == 0, k >= DIAG_X, k < LATE)

    def handle(k, kind):
        direct_wait(k, kind)
        fwd(k, kind).start()
        if kind == 0:
            @pl.when(sends_diag_x(k))
            def _():
                diag(k, False).start()
        if kind == 1:
            @pl.when(sends_diag_y(k))
            def _():
                diag(k, True).start()

    for k in range(NK):
        if k < LATE:
            own(k, 1).start()
        else:
            @pl.when(tp == 0)
            def _():
                own(k, 1).start()
        own(k, 0).start()
        own(k, 3).start()

    acc[...] = jnp.zeros_like(acc)

    def nat(xx, core, t):
        b = 2 * xx + core
        return jnp.where(t == 0, b, 7 - b) * BLK

    nat_of = [nat(x, 0, tp), nat(x, 1, tp), nat(x, 0, 1 - tp), nat(x, 1, 1 - tp),
              nat(1 - x, 0, 0), nat(1 - x, 1, 0), nat(1 - x, 0, 1), nat(1 - x, 1, 1)]

    def put_qkv(slot, col, n, val):
        qkv[pl.ds(pl.multiple_of(nat_of[slot], BLK), BLK), pl.ds(col, n)] = val.astype(BF16)

    NSTEPS = ((0, 512), (512, 512), (1024, 512), (1536, 384))

    def own_chip():
        with jax.named_scope('wait_sib'):
            drain(xs.at[:, rows(0, c), :], sib_recv)
        with jax.named_scope('wait_w'):
            drain(w, w_sem)
        for n in range(NOUT):
            wo_in(n).start()
        for col, n in NSTEPS:
            val = jnp.dot(xs[0, 0:128, :], w[0:KC, col:col + n], preferred_element_type=F32)
            for k in range(1, NK):
                val += jnp.dot(xs[k, 0:128, :], w[k * KC:(k + 1) * KC, col:col + n], preferred_element_type=F32)
            put_qkv(0, col, n, val[:BLK])
            put_qkv(1, col, n, val[BLK:])

    def accumulate(chunks, row, m, arow):
        for col, n in NSTEPS:
            val = acc[arow:arow + m, col:col + n]
            for k in chunks:
                val += jnp.dot(xs[k, row:row + m, :], w[pl.ds(pl.multiple_of(k * KC, KC), KC), col:col + n], preferred_element_type=F32)
            acc[arow:arow + m, col:col + n] = val

    lag = jnp.where(tp == 0, 3, 6)

    @pl.loop(0, NK + 6)
    def _(i):
        @pl.when(i < NK)
        def _():
            with jax.named_scope('h_y'):
                handle(i, 0)

        @pl.when(i < jnp.where(tp == 0, NK, LATE))
        def _():
            with jax.named_scope('h_x'):
                handle(i, 1)

        @pl.when((tp == 1) & (i == DIAG_X - 1))
        def _():
            for k in range(LATE, NK):
                own(k, 1).start()

        @pl.when((tp == 1) & (i >= 5) & (i < NK + 5))
        def _():
            with jax.named_scope('h_d'):
                handle(i - 5, 2)

        @pl.when(i == 2)
        def _():
            own_chip()

        @pl.when((i >= lag) & (i < NK + lag))
        def _():
            k = i - lag
            with jax.named_scope('w_fwd'):
                drain(xs.at[k, pl.ds(128, 128), :], fwd_recv.at[k])
            with jax.named_scope('acc_a'):
                accumulate((k,), 128, 256, 0)

    for col, n in NSTEPS:
        for s in range(4):
            put_qkv(2 + s, col, n, acc[s * BLK:(s + 1) * BLK, col:col + n])

    def rest_of_rows():
        @pl.loop(0, LATE + 1)
        def _(j):
            @pl.when((tp == 0) & (j < LATE))
            def _():
                with jax.named_scope('h_d2'):
                    handle(j, 2)
                    handle(j + LATE, 2)

            @pl.when((tp == 1) & (j < LATE))
            def _():
                with jax.named_scope('h_x2'):
                    handle(j + LATE, 1)

            @pl.when(j > 0)
            def _():
                with jax.named_scope('w_fwd2'):
                    drain(xs.at[0, pl.ds(384, 128), :], fwd_recv.at[NK + j - 1])
                with jax.named_scope('acc_b'):
                    accumulate((j - 1, j - 1 + LATE), 384, 128, 256)

        for col, n in NSTEPS:
            for s in range(2):
                put_qkv(6 + s, col, n, acc[256 + s * BLK:256 + (s + 1) * BLK, col:col + n])

    inv_sqrt = E ** -0.5

    def o_copy(b, dev_cp):
        lohi = b // 4
        return remote(osend.at[b], ofull.at[lohi, :, pl.ds(pl.multiple_of(cp * HE, E), HE)],
                      o_send_sem, o_recv_sem.at[lohi], {'cp': dev_cp, 'tp': tp})

    def attend(b):
        length = 128 * (b // 2 + 1)
        ri = lax.broadcasted_iota(jnp.int32, (BLK, 128), 0) + BLK * (b % 2)
        ci = lax.broadcasted_iota(jnp.int32, (BLK, 128), 1)
        mask = ci <= ri
        heads = range(HEADS)
        q = [qkv[b * BLK:(b + 1) * BLK, h * E:(h + 1) * E] for h in heads]
        kk = [qkv[0:length, HE + h * E:HE + (h + 1) * E] for h in heads]
        v = [qkv[0:length, 2 * HE + h * E:2 * HE + (h + 1) * E] for h in heads]
        s = [lax.dot_general(q[h], kk[h], (((1,), (1,)), ((), ())), preferred_element_type=F32) * inv_sqrt for h in heads]
        last = [jnp.where(mask, s[h][:, length - 128:], NEG_BIG) for h in heads]
        s = [last[h] if length == 128 else jnp.concatenate([s[h][:, :length - 128], last[h]], axis=1) for h in heads]
        m = [jnp.max(s[h], axis=-1, keepdims=True) for h in heads]
        p = [jnp.exp(s[h] - m[h]) for h in heads]
        l = [jnp.sum(p[h], axis=-1, keepdims=True) for h in heads]
        o = [jnp.dot(p[h].astype(BF16), v[h], preferred_element_type=F32) for h in heads]
        for h in heads:
            osend[b, :, h * E:(h + 1) * E] = (o[h] / l[h]).astype(BF16)
        r = b if b < 4 else 7 - b

        @pl.when(cp == r)
        def _():
            ofull[b // 4, :, pl.ds(pl.multiple_of(cp * HE, E), HE)] = osend[b]

        @pl.when(cp != r)
        def _():
            o_copy(b, r).start()

    def wait_o(lohi):
        drain(osend.at[pl.ds(0, 3)], o_recv_sem.at[lohi])

    def attend_blocks(hi):
        @pl.loop(0, 4)
        def _(step):
            first = step < 2
            pair = jnp.where(hi, jnp.where(first, 2 + x, 3 - x), jnp.where(first, 1 - x, x))
            block = 2 * pair + step % 2
            for b in range(8):
                @pl.when(block == b)
                def _():
                    with jax.named_scope(f'attend{b}'):
                        attend(b)

    away, home = 1 - tp, tp

    def y_copy(n, half):
        sl = pl.ds(half * (NC // 2), NC // 2)
        return remote(ysend.at[n, :, sl], yrecv.at[n, :, sl], y_send_sem, y_recv_sem.at[n], yn)

    def project_away():
        with jax.named_scope('wait_o_away'):
            wait_o(away)
            drain(wo, wo_sem)

        @pl.loop(0, NOUT)
        def _(n):
            for half in range(2):
                cols = slice(half * (NC // 2), (half + 1) * (NC // 2))
                with jax.named_scope('proj'):
                    ysend[n, :, cols] = jnp.dot(ofull[away], wo[n, :, cols], preferred_element_type=F32)
                y_copy(n, half).start()

    @pl.loop(0, 4)
    def _(stage):
        @pl.when(stage == 2 * tp)
        def _():
            rest_of_rows()

        @pl.when((stage == 1 - tp) | (stage == 2 + tp))
        def _():
            attend_blocks((stage < 2) == (tp == 0))

        @pl.when(stage == 3 - 2 * tp)
        def _():
            project_away()

    with jax.named_scope('wait_o_home'):
        wait_o(home)

    @pl.loop(0, NOUT)
    def _(n):
        part = jnp.dot(ofull[home], wo[n], preferred_element_type=F32)
        with jax.named_scope('wait_y'):
            drain(yrecv.at[n], y_recv_sem.at[n])
        y_ref[:, pl.ds(pl.multiple_of(n * NC, NC), NC)] = (part + yrecv[n]).astype(BF16)

    for kind in (0, 1, 3):
        drain(xs.at[:, rows(0, c), :], own_send.at[kind])
    for kind in (0, 1, 2):
        drain(xs.at[:, rows(0, c), :], fwd_send.at[kind])
    for t, over_x, over_y in ((0, NK - LATE, NK - DIAG_X), (1, DIAG_X, LATE)):
        @pl.when(tp == t)
        def _():
            drain(xs.at[pl.ds(0, over_x), rows(0, c), :], dg_send.at[0])
            drain(xs.at[pl.ds(0, over_y), rows(0, c), :], dg_send.at[1])
    drain(osend.at[pl.ds(0, 6)], o_send_sem)
    drain(ysend, y_send_sem)


def solution(mesh):
    def device_fn(x_loc, w_q, w_k, w_v, w_o):
        dma = pltpu.SemaphoreType.DMA
        heads_major = [jnp.transpose(t, (1, 0, 2)) for t in (w_q, w_k, w_v)]
        return pl.pallas_call(
            kernel,
            name='attention_layer',
            out_shape=pltpu.VMEM((BLK, D), BF16),
            in_specs=[pl.BlockSpec(memory_space=pl.ANY)] * 5,
            out_specs=pl.BlockSpec(memory_space=pltpu.VMEM),
            scratch_shapes=[
                pltpu.VMEM((NK, 512, KC), BF16),
                pltpu.VMEM((D, NQKV), BF16),
                pltpu.VMEM((NOUT, 20 * E, NC), BF16),
                pltpu.VMEM((512, NQKV), BF16),
                pltpu.VMEM((384, NQKV), F32),
                pltpu.VMEM((8, BLK, HE), BF16),
                pltpu.VMEM((2, BLK, 20 * E), BF16),
                pltpu.VMEM((NOUT, BLK, NC), F32),
                pltpu.VMEM((NOUT, BLK, NC), F32),
                dma, dma, dma,
                dma((4,)), dma, dma((3, NK)),
                dma((3,)), dma((NK + LATE,)), dma((2,)),
                dma, dma((2,)),
                dma, dma((NOUT,)),
            ],
            compiler_params=pltpu.CompilerParams(collective_id=0, has_side_effects=True, vmem_limit_bytes=64 * 1000 * 1000),
        )(x_loc, *heads_major, w_o.reshape(20 * E, D))

    seq_spec = P(('dp', 'cp', 'tp'), None)
    head_spec = P(None, 'tp', None)
    return jax.shard_map(device_fn, mesh=mesh, in_specs=(seq_spec, head_spec, head_spec, head_spec, P('tp', None, None)), out_specs=seq_spec, check_vma=False)
```

```python
import functools

import jax
import jax.numpy as jnp
from jax import lax
from jax.experimental import pallas as pl
from jax.experimental.pallas import tpu as pltpu
from jax.sharding import PartitionSpec as P


BF16, F32 = jnp.bfloat16, jnp.float32
NEG_BIG = -1e30
D = 5120
E = 128
HEADS = 5
HE = HEADS * E
NQKV = 3 * HE
BLK = 64
HALF = BLK // 2
NK = 10
KC = D // NK
LATE = NK // 2
DIAG_X = 7
NOUT = 10
NC = D // NOUT
MESH = pl.DeviceIdType.MESH


def remote(src, dst, send_sem, recv_sem, dev):
    return pltpu.make_async_remote_copy(src_ref=src, dst_ref=dst, send_sem=send_sem, recv_sem=recv_sem, device_id=dev, device_id_type=MESH)


def drain(ref, sem):
    pltpu.make_async_copy(ref, ref, sem).wait()


def kernel(x_hbm, wq_hbm, wk_hbm, wv_hbm, wo_hbm, y_ref, xs, w, wo, qkv, acc, osend, ofull, ysend, yrecv,
           xin_sem, w_sem, wo_sem, own_send, sib_recv, direct_recv, fwd_send, fwd_recv, dg_send, o_send_sem, o_recv_sem,
           y_send_sem, y_recv_sem):
    cp, tp = lax.axis_index('cp'), lax.axis_index('tp')
    x, c = cp // 2, cp % 2
    sib = {'cp': 2 * x + 1 - c, 'tp': tp}
    xn = {'cp': 2 * (1 - x) + c, 'tp': tp}
    xo = {'cp': 2 * (1 - x) + 1 - c, 'tp': tp}
    yn = {'cp': cp, 'tp': 1 - tp}

    def rows(group, core):
        return pl.ds(pl.multiple_of(group * 128 + core * BLK, BLK), BLK)

    def x_in(k):
        return pltpu.make_async_copy(x_hbm.at[:, pl.ds(k * KC, KC)], xs.at[k, rows(0, c), :], xin_sem)

    def w_in(j):
        src = (wq_hbm, wk_hbm, wv_hbm)[j // HEADS].at[cp * HEADS + j % HEADS]
        return pltpu.make_async_copy(src, w.at[:, pl.ds(j * E, E)], w_sem)

    def wo_in(n):
        return pltpu.make_async_copy(wo_hbm.at[:, pl.ds(n * NC, NC)], wo.at[n], wo_sem)

    for k in range(NK):
        x_in(k).start()
    barrier = pltpu.get_barrier_semaphore()
    for dev in (sib, xn, xo, yn):
        pl.semaphore_signal(barrier, inc=1, device_id=dev, device_id_type=MESH)
    drain(xs.at[:, rows(0, c), :], xin_sem)
    for j in range(3 * HEADS):
        w_in(j).start()
    with jax.named_scope('barrier'):
        pl.semaphore_wait(barrier, 4)

    def group_of(kind, t):
        return (1, 2 + t, 3 - t, 0)[kind]

    def own(k, kind):
        dev, t = ((yn, 1 - tp), (xn, tp), None, (sib, tp))[kind]
        return remote(xs.at[k, rows(0, c), :], xs.at[k, rows(group_of(kind, t), c), :], own_send.at[kind], sib_recv if kind == 3 else direct_recv.at[kind, k], dev)

    def diag(k, over_y):
        dev, src, t = (yn, group_of(1, tp), 1 - tp) if over_y else (xn, group_of(0, tp), tp)
        return remote(xs.at[k, rows(src, c), :], xs.at[k, rows(group_of(2, t), c), :], dg_send.at[int(over_y)], direct_recv.at[2, k], dev)

    def fwd(k, kind):
        sl = rows(group_of(kind, tp), c)
        early = (True, tp == 0, tp == 1)[kind]
        return remote(xs.at[k, sl, :], xs.at[k, sl, :], fwd_send.at[kind], fwd_recv.at[jnp.where(early, k, NK + k % LATE)], sib)

    def direct_wait(k, kind):
        drain(xs.at[k, rows(group_of(kind, tp), c), :], direct_recv.at[kind, k])

    def sends_diag_x(k):
        return jnp.where(tp == 0, k >= LATE, k < DIAG_X)

    def sends_diag_y(k):
        return jnp.where(tp == 0, k >= DIAG_X, k < LATE)

    def handle(k, kind):
        direct_wait(k, kind)
        fwd(k, kind).start()
        if kind == 0:
            @pl.when(sends_diag_x(k))
            def _():
                diag(k, False).start()
        if kind == 1:
            @pl.when(sends_diag_y(k))
            def _():
                diag(k, True).start()

    for k in range(NK):
        if k < LATE:
            own(k, 1).start()
        else:
            @pl.when(tp == 0)
            def _():
                own(k, 1).start()
        own(k, 0).start()
        own(k, 3).start()

    acc[...] = jnp.zeros_like(acc)

    def nat(xx, core, t):
        b = 2 * xx + core
        return jnp.where(t == 0, b, 7 - b) * BLK

    nat_of = [nat(x, 0, tp), nat(x, 1, tp), nat(x, 0, 1 - tp), nat(x, 1, 1 - tp),
              nat(1 - x, 0, 0), nat(1 - x, 1, 0), nat(1 - x, 0, 1), nat(1 - x, 1, 1)]

    def put_qkv(slot, col, n, val):
        qkv[pl.ds(pl.multiple_of(nat_of[slot], BLK), BLK), pl.ds(col, n)] = val.astype(BF16)

    NSTEPS = ((0, 512), (512, 512), (1024, 512), (1536, 384))

    def own_chip():
        with jax.named_scope('wait_sib'):
            drain(xs.at[:, rows(0, c), :], sib_recv)
        with jax.named_scope('wait_w'):
            drain(w, w_sem)
        for n in range(NOUT):
            wo_in(n).start()
        for col, n in NSTEPS:
            val = jnp.dot(xs[0, 0:128, :], w[0:KC, col:col + n], preferred_element_type=F32)
            for k in range(1, NK):
                val += jnp.dot(xs[k, 0:128, :], w[k * KC:(k + 1) * KC, col:col + n], preferred_element_type=F32)
            put_qkv(0, col, n, val[:BLK])
            put_qkv(1, col, n, val[BLK:])

    def accumulate(chunks, row, m, arow):
        for col, n in NSTEPS:
            val = acc[arow:arow + m, col:col + n]
            for k in chunks:
                val += jnp.dot(xs[k, row:row + m, :], w[pl.ds(pl.multiple_of(k * KC, KC), KC), col:col + n], preferred_element_type=F32)
            acc[arow:arow + m, col:col + n] = val

    lag = jnp.where(tp == 0, 3, 6)

    @pl.loop(0, NK + 6)
    def _(i):
        @pl.when(i < NK)
        def _():
            with jax.named_scope('h_y'):
                handle(i, 0)

        @pl.when(i < jnp.where(tp == 0, NK, LATE))
        def _():
            with jax.named_scope('h_x'):
                handle(i, 1)

        @pl.when((tp == 1) & (i == DIAG_X - 1))
        def _():
            for k in range(LATE, NK):
                own(k, 1).start()

        @pl.when((tp == 1) & (i >= 5) & (i < NK + 5))
        def _():
            with jax.named_scope('h_d'):
                handle(i - 5, 2)

        @pl.when(i == 2)
        def _():
            own_chip()

        @pl.when((i >= lag) & (i < NK + lag))
        def _():
            k = i - lag
            with jax.named_scope('w_fwd'):
                drain(xs.at[k, pl.ds(128, 128), :], fwd_recv.at[k])
            with jax.named_scope('acc_a'):
                accumulate((k,), 128, 256, 0)

    for col, n in NSTEPS:
        for s in range(4):
            put_qkv(2 + s, col, n, acc[s * BLK:(s + 1) * BLK, col:col + n])

    def rest_of_rows():
        @pl.loop(0, LATE + 1)
        def _(j):
            @pl.when((tp == 0) & (j < LATE))
            def _():
                with jax.named_scope('h_d2'):
                    handle(j, 2)
                    handle(j + LATE, 2)

            @pl.when((tp == 1) & (j < LATE))
            def _():
                with jax.named_scope('h_x2'):
                    handle(j + LATE, 1)

            @pl.when(j > 0)
            def _():
                with jax.named_scope('w_fwd2'):
                    drain(xs.at[0, pl.ds(384, 128), :], fwd_recv.at[NK + j - 1])
                with jax.named_scope('acc_b'):
                    accumulate((j - 1, j - 1 + LATE), 384, 128, 256)

        for col, n in NSTEPS:
            for s in range(2):
                put_qkv(6 + s, col, n, acc[256 + s * BLK:256 + (s + 1) * BLK, col:col + n])

    inv_sqrt = E ** -0.5

    def o_copy(b, half, dev_cp):
        lohi, part = b // 4, pl.ds(half * HALF, HALF)
        return remote(osend.at[b, part], ofull.at[lohi, part, pl.ds(pl.multiple_of(cp * HE, E), HE)],
                      o_send_sem, o_recv_sem.at[lohi, half], {'cp': dev_cp, 'tp': tp})

    def attend(b):
        length = 128 * (b // 2 + 1)
        ri = lax.broadcasted_iota(jnp.int32, (BLK, 128), 0) + BLK * (b % 2)
        ci = lax.broadcasted_iota(jnp.int32, (BLK, 128), 1)
        mask = ci <= ri
        heads = range(HEADS)
        q = [qkv[b * BLK:(b + 1) * BLK, h * E:(h + 1) * E] for h in heads]
        kk = [qkv[0:length, HE + h * E:HE + (h + 1) * E] for h in heads]
        v = [qkv[0:length, 2 * HE + h * E:2 * HE + (h + 1) * E] for h in heads]
        s = [lax.dot_general(q[h], kk[h], (((1,), (1,)), ((), ())), preferred_element_type=F32) * inv_sqrt for h in heads]
        last = [jnp.where(mask, s[h][:, length - 128:], NEG_BIG) for h in heads]
        s = [last[h] if length == 128 else jnp.concatenate([s[h][:, :length - 128], last[h]], axis=1) for h in heads]
        m = [jnp.max(s[h], axis=-1, keepdims=True) for h in heads]
        p = [jnp.exp(s[h] - m[h]) for h in heads]
        l = [jnp.sum(p[h], axis=-1, keepdims=True) for h in heads]
        o = [jnp.dot(p[h].astype(BF16), v[h], preferred_element_type=F32) for h in heads]
        for h in heads:
            osend[b, :, h * E:(h + 1) * E] = (o[h] / l[h]).astype(BF16)
        r = b if b < 4 else 7 - b

        @pl.when(cp == r)
        def _():
            ofull[b // 4, :, pl.ds(pl.multiple_of(cp * HE, E), HE)] = osend[b]

        @pl.when(cp != r)
        def _():
            for half in range(2):
                o_copy(b, half, r).start()

    def wait_o(lohi, half):
        drain(osend.at[pl.ds(0, 3), pl.ds(0, HALF)], o_recv_sem.at[lohi, half])

    def attend_blocks(hi):
        @pl.loop(0, 4)
        def _(step):
            first = step < 2
            pair = jnp.where(hi, jnp.where(first, 2 + x, 3 - x), jnp.where(first, 1 - x, x))
            block = 2 * pair + jnp.where(hi, step % 2, 1 - step % 2)
            for b in range(8):
                @pl.when(block == b)
                def _():
                    with jax.named_scope(f'attend{b}'):
                        attend(b)

    away, home = 1 - tp, tp

    def y_copy(n, half):
        part = pl.ds(pl.multiple_of(half * HALF, HALF), HALF)
        return remote(ysend.at[n, part], yrecv.at[n, part], y_send_sem, y_recv_sem.at[n], yn)

    def project_away():
        @pl.loop(0, 2)
        def _(half):
            with jax.named_scope('wait_o_away'):
                wait_o(away, half)

            @pl.when(half == 0)
            def _():
                drain(wo, wo_sem)

            part = pl.ds(pl.multiple_of(half * HALF, HALF), HALF)

            @pl.loop(0, NOUT)
            def _(n):
                with jax.named_scope('proj'):
                    ysend[n, part] = jnp.dot(ofull[away, part], wo[n], preferred_element_type=F32)
                y_copy(n, half).start()

    @pl.loop(0, 4)
    def _(stage):
        @pl.when(stage == 2 * tp)
        def _():
            rest_of_rows()

        @pl.when((stage == 1 - tp) | (stage == 2 + tp))
        def _():
            attend_blocks((stage < 2) == (tp == 0))

        @pl.when(stage == 3 - 2 * tp)
        def _():
            project_away()

    with jax.named_scope('wait_o_home'):
        for half in range(2):
            wait_o(home, half)

    @pl.loop(0, NOUT)
    def _(n):
        part = jnp.dot(ofull[home], wo[n], preferred_element_type=F32)
        with jax.named_scope('wait_y'):
            drain(yrecv.at[n], y_recv_sem.at[n])
        y_ref[:, pl.ds(pl.multiple_of(n * NC, NC), NC)] = (part + yrecv[n]).astype(BF16)

    for kind in (0, 1, 3):
        drain(xs.at[:, rows(0, c), :], own_send.at[kind])
    for kind in (0, 1, 2):
        drain(xs.at[:, rows(0, c), :], fwd_send.at[kind])
    for t, over_x, over_y in ((0, NK - LATE, NK - DIAG_X), (1, DIAG_X, LATE)):
        @pl.when(tp == t)
        def _():
            drain(xs.at[pl.ds(0, over_x), rows(0, c), :], dg_send.at[0])
            drain(xs.at[pl.ds(0, over_y), rows(0, c), :], dg_send.at[1])
    drain(osend.at[pl.ds(0, 6)], o_send_sem)
    drain(ysend, y_send_sem)


def solution(mesh):
    def device_fn(x_loc, w_q, w_k, w_v, w_o):
        dma = pltpu.SemaphoreType.DMA
        heads_major = [jnp.transpose(t, (1, 0, 2)) for t in (w_q, w_k, w_v)]
        return pl.pallas_call(
            kernel,
            name='attention_layer',
            out_shape=pltpu.VMEM((BLK, D), BF16),
            in_specs=[pl.BlockSpec(memory_space=pl.ANY)] * 5,
            out_specs=pl.BlockSpec(memory_space=pltpu.VMEM),
            scratch_shapes=[
                pltpu.VMEM((NK, 512, KC), BF16),
                pltpu.VMEM((D, NQKV), BF16),
                pltpu.VMEM((NOUT, 20 * E, NC), BF16),
                pltpu.VMEM((512, NQKV), BF16),
                pltpu.VMEM((384, NQKV), F32),
                pltpu.VMEM((8, BLK, HE), BF16),
                pltpu.VMEM((2, BLK, 20 * E), BF16),
                pltpu.VMEM((NOUT, BLK, NC), F32),
                pltpu.VMEM((NOUT, BLK, NC), F32),
                dma, dma, dma,
                dma((4,)), dma, dma((3, NK)),
                dma((3,)), dma((NK + LATE,)), dma((2,)),
                dma, dma((2, 2)),
                dma, dma((NOUT,)),
            ],
            compiler_params=pltpu.CompilerParams(collective_id=0, has_side_effects=True, vmem_limit_bytes=64 * 1000 * 1000),
        )(x_loc, *heads_major, w_o.reshape(20 * E, D))

    seq_spec = P(('dp', 'cp', 'tp'), None)
    head_spec = P(None, 'tp', None)
    return jax.shard_map(device_fn, mesh=mesh, in_specs=(seq_spec, head_spec, head_spec, head_spec, P('tp', None, None)), out_specs=seq_spec, check_vma=False)
```

```python
import functools

import jax
import jax.numpy as jnp
from jax import lax
from jax.experimental import pallas as pl
from jax.experimental.pallas import tpu as pltpu
from jax.sharding import PartitionSpec as P


BF16, F32 = jnp.bfloat16, jnp.float32
NEG_BIG = -1e30
D = 5120
E = 128
HEADS = 5
HE = HEADS * E
NQKV = 3 * HE
BLK = 64
HALF = BLK // 2
NK = 10
KC = D // NK
LATE = NK // 2
DIAG_X = 7
NOUT = 10
NC = D // NOUT
MESH = pl.DeviceIdType.MESH


def remote(src, dst, send_sem, recv_sem, dev):
    return pltpu.make_async_remote_copy(src_ref=src, dst_ref=dst, send_sem=send_sem, recv_sem=recv_sem, device_id=dev, device_id_type=MESH)


def drain(ref, sem):
    pltpu.make_async_copy(ref, ref, sem).wait()


def kernel(x_hbm, wq_hbm, wk_hbm, wv_hbm, wo_hbm, y_ref, xs, w, wo, qkv, acc, osend, ofull, ysend, yrecv,
           xin_sem, w_sem, wo_sem, own_send, sib_recv, direct_recv, fwd_send, fwd_recv, dg_send, o_send_sem, o_recv_sem,
           y_send_sem, y_recv_sem):
    cp, tp = lax.axis_index('cp'), lax.axis_index('tp')
    x, c = cp // 2, cp % 2
    sib = {'cp': 2 * x + 1 - c, 'tp': tp}
    xn = {'cp': 2 * (1 - x) + c, 'tp': tp}
    xo = {'cp': 2 * (1 - x) + 1 - c, 'tp': tp}
    yn = {'cp': cp, 'tp': 1 - tp}

    def rows(group, core):
        return pl.ds(pl.multiple_of(group * 128 + core * BLK, BLK), BLK)

    def x_in(k):
        return pltpu.make_async_copy(x_hbm.at[:, pl.ds(k * KC, KC)], xs.at[k, rows(0, c), :], xin_sem)

    def w_in(j):
        src = (wq_hbm, wk_hbm, wv_hbm)[j // HEADS].at[cp * HEADS + j % HEADS]
        return pltpu.make_async_copy(src, w.at[:, pl.ds(j * E, E)], w_sem)

    def wo_in(n):
        return pltpu.make_async_copy(wo_hbm.at[:, pl.ds(n * NC, NC)], wo.at[n], wo_sem)

    for k in range(NK):
        x_in(k).start()
    barrier = pltpu.get_barrier_semaphore()
    for dev in (sib, xn, xo, yn):
        pl.semaphore_signal(barrier, inc=1, device_id=dev, device_id_type=MESH)
    drain(xs.at[:, rows(0, c), :], xin_sem)
    for j in range(3 * HEADS):
        w_in(j).start()
    with jax.named_scope('barrier'):
        pl.semaphore_wait(barrier, 4)

    def group_of(kind, t):
        return (1, 2 + t, 3 - t, 0)[kind]

    def own(k, kind):
        dev, t = ((yn, 1 - tp), (xn, tp), None, (sib, tp))[kind]
        return remote(xs.at[k, rows(0, c), :], xs.at[k, rows(group_of(kind, t), c), :], own_send.at[kind], sib_recv if kind == 3 else direct_recv.at[kind, k], dev)

    def diag(k, over_y):
        dev, src, t = (yn, group_of(1, tp), 1 - tp) if over_y else (xn, group_of(0, tp), tp)
        return remote(xs.at[k, rows(src, c), :], xs.at[k, rows(group_of(2, t), c), :], dg_send.at[int(over_y)], direct_recv.at[2, k], dev)

    def fwd(k, kind):
        sl = rows(group_of(kind, tp), c)
        early = (True, tp == 0, tp == 1)[kind]
        return remote(xs.at[k, sl, :], xs.at[k, sl, :], fwd_send.at[kind], fwd_recv.at[jnp.where(early, k, NK + k % LATE)], sib)

    def direct_wait(k, kind):
        drain(xs.at[k, rows(group_of(kind, tp), c), :], direct_recv.at[kind, k])

    def sends_diag_x(k):
        return jnp.where(tp == 0, k >= LATE, k < DIAG_X)

    def sends_diag_y(k):
        return jnp.where(tp == 0, k >= DIAG_X, k < LATE)

    def handle(k, kind):
        direct_wait(k, kind)
        fwd(k, kind).start()
        if kind == 0:
            @pl.when(sends_diag_x(k))
            def _():
                diag(k, False).start()
        if kind == 1:
            @pl.when(sends_diag_y(k))
            def _():
                diag(k, True).start()

    for k in range(NK):
        if k < LATE:
            own(k, 1).start()
        else:
            @pl.when(tp == 0)
            def _():
                own(k, 1).start()
        own(k, 0).start()
        own(k, 3).start()

    acc[...] = jnp.zeros_like(acc)

    def nat(xx, core, t):
        b = 2 * xx + core
        return jnp.where(t == 0, b, 7 - b) * BLK

    nat_of = [nat(x, 0, tp), nat(x, 1, tp), nat(x, 0, 1 - tp), nat(x, 1, 1 - tp),
              nat(1 - x, 0, 0), nat(1 - x, 1, 0), nat(1 - x, 0, 1), nat(1 - x, 1, 1)]

    def put_qkv(slot, col, n, val):
        qkv[pl.ds(pl.multiple_of(nat_of[slot], BLK), BLK), pl.ds(col, n)] = val.astype(BF16)

    NSTEPS = ((0, 512), (512, 512), (1024, 512), (1536, 384))

    def own_chip():
        with jax.named_scope('wait_sib'):
            drain(xs.at[:, rows(0, c), :], sib_recv)
        with jax.named_scope('wait_w'):
            drain(w, w_sem)
        for n in range(NOUT):
            wo_in(n).start()
        for col, n in NSTEPS:
            val = jnp.dot(xs[0, 0:128, :], w[0:KC, col:col + n], preferred_element_type=F32)
            for k in range(1, NK):
                val += jnp.dot(xs[k, 0:128, :], w[k * KC:(k + 1) * KC, col:col + n], preferred_element_type=F32)
            put_qkv(0, col, n, val[:BLK])
            put_qkv(1, col, n, val[BLK:])

    def accumulate(chunks, row, m, arow):
        for col, n in NSTEPS:
            val = acc[arow:arow + m, col:col + n]
            for k in chunks:
                val += jnp.dot(xs[k, row:row + m, :], w[pl.ds(pl.multiple_of(k * KC, KC), KC), col:col + n], preferred_element_type=F32)
            acc[arow:arow + m, col:col + n] = val

    lag = jnp.where(tp == 0, 3, 6)

    @pl.loop(0, NK + 6)
    def _(i):
        @pl.when(i < NK)
        def _():
            with jax.named_scope('h_y'):
                handle(i, 0)

        @pl.when(i < jnp.where(tp == 0, NK, LATE))
        def _():
            with jax.named_scope('h_x'):
                handle(i, 1)

        @pl.when((tp == 1) & (i == DIAG_X - 1))
        def _():
            for k in range(LATE, NK):
                own(k, 1).start()

        @pl.when((tp == 1) & (i >= 5) & (i < NK + 5))
        def _():
            with jax.named_scope('h_d'):
                handle(i - 5, 2)

        @pl.when(i == 2)
        def _():
            own_chip()

        @pl.when((i >= lag) & (i < NK + lag))
        def _():
            k = i - lag
            with jax.named_scope('w_fwd'):
                drain(xs.at[k, pl.ds(128, 128), :], fwd_recv.at[k])
            with jax.named_scope('acc_a'):
                accumulate((k,), 128, 256, 0)

    for col, n in NSTEPS:
        for s in range(4):
            put_qkv(2 + s, col, n, acc[s * BLK:(s + 1) * BLK, col:col + n])

    def rest_of_rows():
        @pl.loop(0, LATE + 1)
        def _(j):
            @pl.when((tp == 0) & (j < LATE))
            def _():
                with jax.named_scope('h_d2'):
                    handle(j, 2)
                    handle(j + LATE, 2)

            @pl.when((tp == 1) & (j < LATE))
            def _():
                with jax.named_scope('h_x2'):
                    handle(j + LATE, 1)

            @pl.when(j > 0)
            def _():
                with jax.named_scope('w_fwd2'):
                    drain(xs.at[0, pl.ds(384, 128), :], fwd_recv.at[NK + j - 1])
                with jax.named_scope('acc_b'):
                    accumulate((j - 1, j - 1 + LATE), 384, 128, 256)

        for col, n in NSTEPS:
            for s in range(2):
                put_qkv(6 + s, col, n, acc[256 + s * BLK:256 + (s + 1) * BLK, col:col + n])

    inv_sqrt = E ** -0.5

    def o_copy(b, half, dev_cp):
        lohi, part = b // 4, pl.ds(half * HALF, HALF)
        return remote(osend.at[b, part], ofull.at[lohi, part, pl.ds(pl.multiple_of(cp * HE, E), HE)],
                      o_send_sem, o_recv_sem.at[lohi, half, jnp.where(x == dev_cp // 2, 0, 1)], {'cp': dev_cp, 'tp': tp})

    def attend(b):
        length = 128 * (b // 2 + 1)
        ri = lax.broadcasted_iota(jnp.int32, (BLK, 128), 0) + BLK * (b % 2)
        ci = lax.broadcasted_iota(jnp.int32, (BLK, 128), 1)
        mask = ci <= ri
        heads = range(HEADS)
        q = [qkv[b * BLK:(b + 1) * BLK, h * E:(h + 1) * E] for h in heads]
        kk = [qkv[0:length, HE + h * E:HE + (h + 1) * E] for h in heads]
        v = [qkv[0:length, 2 * HE + h * E:2 * HE + (h + 1) * E] for h in heads]
        s = [lax.dot_general(q[h], kk[h], (((1,), (1,)), ((), ())), preferred_element_type=F32) * inv_sqrt for h in heads]
        last = [jnp.where(mask, s[h][:, length - 128:], NEG_BIG) for h in heads]
        s = [last[h] if length == 128 else jnp.concatenate([s[h][:, :length - 128], last[h]], axis=1) for h in heads]
        m = [jnp.max(s[h], axis=-1, keepdims=True) for h in heads]
        p = [jnp.exp(s[h] - m[h]) for h in heads]
        l = [jnp.sum(p[h], axis=-1, keepdims=True) for h in heads]
        o = [jnp.dot(p[h].astype(BF16), v[h], preferred_element_type=F32) for h in heads]
        for h in heads:
            osend[b, :, h * E:(h + 1) * E] = (o[h] / l[h]).astype(BF16)
        r = b if b < 4 else 7 - b

        @pl.when(cp == r)
        def _():
            ofull[b // 4, :, pl.ds(pl.multiple_of(cp * HE, E), HE)] = osend[b]

        @pl.when(cp != r)
        def _():
            for half in range(2):
                o_copy(b, half, r).start()

    def wait_o(lohi, half, far):
        drain(osend.at[pl.ds(0, 1 + far), pl.ds(0, HALF)], o_recv_sem.at[lohi, half, far])

    def attend_blocks(hi):
        @pl.loop(0, 4)
        def _(step):
            first = step < 2
            pair = jnp.where(hi, jnp.where(first, 2 + x, 3 - x), jnp.where(first, 1 - x, x))
            block = 2 * pair + jnp.where(hi, step % 2, 1 - step % 2)
            for b in range(8):
                @pl.when(block == b)
                def _():
                    with jax.named_scope(f'attend{b}'):
                        attend(b)

    away, home = 1 - tp, tp

    def y_copy(n, half):
        part = pl.ds(half * HALF, HALF)
        return remote(ysend.at[n, part], yrecv.at[n, part], y_send_sem, y_recv_sem.at[n], yn)

    def project_away():
        near = pl.ds(pl.multiple_of(2 * x * HE, E), 2 * HE)
        far = pl.ds(pl.multiple_of(2 * (1 - x) * HE, E), 2 * HE)
        top, bottom = slice(0, HALF), slice(HALF, BLK)
        drain(wo, wo_sem)
        with jax.named_scope('wait_o_away'):
            wait_o(away, 0, 0)
        with jax.named_scope('proj'):
            ysend[0, top] = jnp.dot(ofull[away, top, near], wo[0, near, :], preferred_element_type=F32)
        with jax.named_scope('wait_o_away'):
            wait_o(away, 0, 1)
        with jax.named_scope('proj'):
            ysend[0, top] += jnp.dot(ofull[away, top, far], wo[0, far, :], preferred_element_type=F32)
        y_copy(0, 0).start()

        @pl.loop(1, NOUT)
        def _(n):
            with jax.named_scope('proj'):
                ysend[n, top] = jnp.dot(ofull[away, top], wo[n], preferred_element_type=F32)
            y_copy(n, 0).start()

        with jax.named_scope('wait_o_away'):
            wait_o(away, 1, 0)
            wait_o(away, 1, 1)

        @pl.loop(0, NOUT)
        def _(n):
            with jax.named_scope('proj'):
                ysend[n, bottom] = jnp.dot(ofull[away, bottom], wo[n], preferred_element_type=F32)
            y_copy(n, 1).start()

    @pl.loop(0, 4)
    def _(stage):
        @pl.when(stage == 2 * tp)
        def _():
            rest_of_rows()

        @pl.when((stage == 1 - tp) | (stage == 3))
        def _():
            attend_blocks((stage < 2) == (tp == 0))

        @pl.when(stage == 2 - tp)
        def _():
            project_away()

    with jax.named_scope('wait_o_home'):
        for half in range(2):
            for far in range(2):
                wait_o(home, half, far)

    def kept(n):
        return acc.at[pl.ds(pl.multiple_of(n % 6 * BLK, BLK), BLK), pl.ds(pl.multiple_of(n // 6 * NC, NC), NC)]

    @pl.loop(0, NOUT)
    def _(n):
        kept(n)[...] = jnp.dot(ofull[home], wo[n], preferred_element_type=F32)

    @pl.loop(0, NOUT)
    def _(n):
        with jax.named_scope('wait_y'):
            drain(yrecv.at[n], y_recv_sem.at[n])
        y_ref[:, pl.ds(pl.multiple_of(n * NC, NC), NC)] = (kept(n)[...] + yrecv[n]).astype(BF16)

    for kind in (0, 1, 3):
        drain(xs.at[:, rows(0, c), :], own_send.at[kind])
    for kind in (0, 1, 2):
        drain(xs.at[:, rows(0, c), :], fwd_send.at[kind])
    for t, over_x, over_y in ((0, NK - LATE, NK - DIAG_X), (1, DIAG_X, LATE)):
        @pl.when(tp == t)
        def _():
            drain(xs.at[pl.ds(0, over_x), rows(0, c), :], dg_send.at[0])
            drain(xs.at[pl.ds(0, over_y), rows(0, c), :], dg_send.at[1])
    drain(osend.at[pl.ds(0, 6)], o_send_sem)
    drain(ysend, y_send_sem)


def solution(mesh):
    def device_fn(x_loc, w_q, w_k, w_v, w_o):
        dma = pltpu.SemaphoreType.DMA
        heads_major = [jnp.transpose(t, (1, 0, 2)) for t in (w_q, w_k, w_v)]
        return pl.pallas_call(
            kernel,
            name='attention_layer',
            out_shape=pltpu.VMEM((BLK, D), BF16),
            in_specs=[pl.BlockSpec(memory_space=pl.ANY)] * 5,
            out_specs=pl.BlockSpec(memory_space=pltpu.VMEM),
            scratch_shapes=[
                pltpu.VMEM((NK, 512, KC), BF16),
                pltpu.VMEM((D, NQKV), BF16),
                pltpu.VMEM((NOUT, 20 * E, NC), BF16),
                pltpu.VMEM((512, NQKV), BF16),
                pltpu.VMEM((384, NQKV), F32),
                pltpu.VMEM((8, BLK, HE), BF16),
                pltpu.VMEM((2, BLK, 20 * E), BF16),
                pltpu.VMEM((NOUT, BLK, NC), F32),
                pltpu.VMEM((NOUT, BLK, NC), F32),
                dma, dma, dma,
                dma((4,)), dma, dma((3, NK)),
                dma((3,)), dma((NK + LATE,)), dma((2,)),
                dma, dma((2, 2, 2)),
                dma, dma((NOUT,)),
            ],
            compiler_params=pltpu.CompilerParams(collective_id=0, has_side_effects=True, vmem_limit_bytes=64 * 1000 * 1000),
        )(x_loc, *heads_major, w_o.reshape(20 * E, D))

    seq_spec = P(('dp', 'cp', 'tp'), None)
    head_spec = P(None, 'tp', None)
    return jax.shard_map(device_fn, mesh=mesh, in_specs=(seq_spec, head_spec, head_spec, head_spec, P('tp', None, None)), out_specs=seq_spec, check_vma=False)
```

```python
import functools

import jax
import jax.numpy as jnp
from jax import lax
from jax.experimental import pallas as pl
from jax.experimental.pallas import tpu as pltpu
from jax.sharding import PartitionSpec as P


BF16, F32 = jnp.bfloat16, jnp.float32
NEG_BIG = -1e30
D = 5120
E = 128
HEADS = 5
HE = HEADS * E
NQKV = 3 * HE
BLK = 64
HALF = BLK // 2
NK = 10
KC = D // NK
LATE = NK // 2
DIAG_X = 7
NOUT = 10
NC = D // NOUT
MESH = pl.DeviceIdType.MESH


def remote(src, dst, send_sem, recv_sem, dev):
    return pltpu.make_async_remote_copy(src_ref=src, dst_ref=dst, send_sem=send_sem, recv_sem=recv_sem, device_id=dev, device_id_type=MESH)


def drain(ref, sem):
    pltpu.make_async_copy(ref, ref, sem).wait()


def kernel(x_hbm, wq_hbm, wk_hbm, wv_hbm, wo_hbm, y_ref, xs, w, wo, qkv, acc, osend, ofull, ysend, yrecv,
           xin_sem, w_sem, wo_sem, own_send, sib_recv, direct_recv, fwd_send, fwd_recv, dg_send, o_send_sem, o_recv_sem,
           y_send_sem, y_recv_sem):
    cp, tp = lax.axis_index('cp'), lax.axis_index('tp')
    x, c = cp // 2, cp % 2
    sib = {'cp': 2 * x + 1 - c, 'tp': tp}
    xn = {'cp': 2 * (1 - x) + c, 'tp': tp}
    xo = {'cp': 2 * (1 - x) + 1 - c, 'tp': tp}
    yn = {'cp': cp, 'tp': 1 - tp}

    def rows(group, core):
        return pl.ds(pl.multiple_of(group * 128 + core * BLK, BLK), BLK)

    def x_in(k):
        return pltpu.make_async_copy(x_hbm.at[:, pl.ds(k * KC, KC)], xs.at[k, rows(0, c), :], xin_sem)

    def w_in(j):
        src = (wq_hbm, wk_hbm, wv_hbm)[j // HEADS].at[cp * HEADS + j % HEADS]
        return pltpu.make_async_copy(src, w.at[:, pl.ds(j * E, E)], w_sem)

    def wo_in(n):
        return pltpu.make_async_copy(wo_hbm.at[:, pl.ds(n * NC, NC)], wo.at[n], wo_sem)

    for k in range(NK):
        x_in(k).start()
    barrier = pltpu.get_barrier_semaphore()
    for dev in (sib, xn, xo, yn):
        pl.semaphore_signal(barrier, inc=1, device_id=dev, device_id_type=MESH)
    drain(xs.at[:, rows(0, c), :], xin_sem)
    for j in range(3 * HEADS):
        w_in(j).start()
    with jax.named_scope('barrier'):
        pl.semaphore_wait(barrier, 4)

    def group_of(kind, t):
        return (1, 2 + t, 3 - t, 0)[kind]

    def own(k, kind):
        dev, t = ((yn, 1 - tp), (xn, tp), None, (sib, tp))[kind]
        return remote(xs.at[k, rows(0, c), :], xs.at[k, rows(group_of(kind, t), c), :], own_send, sib_recv if kind == 3 else direct_recv.at[kind, k], dev)

    def diag(k, over_y):
        dev, src, t = (yn, group_of(1, tp), 1 - tp) if over_y else (xn, group_of(0, tp), tp)
        return remote(xs.at[k, rows(src, c), :], xs.at[k, rows(group_of(2, t), c), :], dg_send.at[int(over_y)], direct_recv.at[2, k], dev)

    def half_diag(over_y):
        dev, src, t = (yn, group_of(1, tp), 1 - tp) if over_y else (xn, group_of(0, tp), tp)
        k, first = LATE - 1, 0 if over_y else HALF
        return remote(xs.at[k, pl.ds(pl.multiple_of(src * 128 + c * BLK + first, HALF), HALF), :],
                      xs.at[k, pl.ds(pl.multiple_of(group_of(2, t) * 128 + c * BLK + first, HALF), HALF), :],
                      dg_send.at[int(over_y)], direct_recv.at[2, k], dev)

    def fwd(k, kind):
        sl = rows(group_of(kind, tp), c)
        second = NK + k % LATE
        sem = (k, jnp.where(tp == 0, k, second), jnp.where(tp == 0, second, NK + LATE + k))[kind]
        return remote(xs.at[k, sl, :], xs.at[k, sl, :], fwd_send, fwd_recv.at[sem], sib)

    def direct_wait(k, kind):
        drain(xs.at[k, rows(group_of(kind, tp), c), :], direct_recv.at[kind, k])

    def sends_diag_x(k):
        return jnp.where(tp == 0, k >= LATE, k < DIAG_X)

    def sends_half_x(k):
        return (tp == 0) & (x == 0) & (k == LATE - 1)

    def sends_diag_y(k):
        return jnp.where(tp == 0, k >= DIAG_X, k < LATE - x)

    def sends_half_y(k):
        return (tp == 1) & (x == 1) & (k == LATE - 1)

    def handle(k, kind):
        direct_wait(k, kind)
        fwd(k, kind).start()
        if kind == 0:
            @pl.when(sends_diag_x(k))
            def _():
                diag(k, False).start()

            @pl.when(sends_half_x(k))
            def _():
                half_diag(False).start()
        if kind == 1:
            @pl.when(sends_diag_y(k))
            def _():
                diag(k, True).start()

            @pl.when(sends_half_y(k))
            def _():
                half_diag(True).start()

    for k in range(NK):
        if k < LATE:
            own(k, 1).start()
        else:
            @pl.when(tp == 0)
            def _():
                own(k, 1).start()
        own(k, 0).start()
        own(k, 3).start()

    acc[...] = jnp.zeros_like(acc)

    def nat(xx, core, t):
        b = 2 * xx + core
        return jnp.where(t == 0, b, 7 - b) * BLK

    nat_of = [nat(x, 0, tp), nat(x, 1, tp), nat(x, 0, 1 - tp), nat(x, 1, 1 - tp),
              nat(1 - x, 0, 0), nat(1 - x, 1, 0), nat(1 - x, 0, 1), nat(1 - x, 1, 1)]

    def put_qkv(slot, col, n, val):
        qkv[pl.ds(pl.multiple_of(nat_of[slot], BLK), BLK), pl.ds(col, n)] = val.astype(BF16)

    NSTEPS = ((0, 512), (512, 512), (1024, 512), (1536, 384))

    def own_chip():
        with jax.named_scope('wait_sib'):
            drain(xs.at[:, rows(0, c), :], sib_recv)
        with jax.named_scope('wait_w'):
            drain(w, w_sem)
        for n in range(NOUT):
            wo_in(n).start()
        for col, n in NSTEPS:
            val = jnp.dot(xs[0, 0:128, :], w[0:KC, col:col + n], preferred_element_type=F32)
            for k in range(1, NK):
                val += jnp.dot(xs[k, 0:128, :], w[k * KC:(k + 1) * KC, col:col + n], preferred_element_type=F32)
            put_qkv(0, col, n, val[:BLK])
            put_qkv(1, col, n, val[BLK:])

    def accumulate(chunks, row, m, arow):
        for col, n in NSTEPS:
            val = acc[arow:arow + m, col:col + n]
            for k in chunks:
                val += jnp.dot(xs[k, row:row + m, :], w[pl.ds(pl.multiple_of(k * KC, KC), KC), col:col + n], preferred_element_type=F32)
            acc[arow:arow + m, col:col + n] = val

    def diag_order(m):
        return jnp.where(m < 5, m, jnp.where(m % 2 == 1, 7 + (m - 5) // 2, 5 + (m - 6) // 2))

    @pl.loop(0, NK + 6)
    def _(i):
        @pl.when(i < NK)
        def _():
            with jax.named_scope('h_y'):
                handle(i, 0)

        @pl.when(i < jnp.where(tp == 0, NK, LATE))
        def _():
            with jax.named_scope('h_x'):
                handle(i, 1)

        @pl.when((tp == 1) & (i == DIAG_X - 1))
        def _():
            for k in range(LATE, NK):
                own(k, 1).start()

        @pl.when((tp == 1) & (i >= 5) & (i < NK + 5))
        def _():
            with jax.named_scope('h_d'):
                handle(diag_order(i - 5), 2)

        @pl.when(i == 2)
        def _():
            own_chip()

        @pl.when((i >= 3) & (i < NK + 3))
        def _():
            k = i - 3

            @pl.when(tp == 0)
            def _():
                with jax.named_scope('w_fwd'):
                    drain(xs.at[k, pl.ds(128, 128), :], fwd_recv.at[k])
                with jax.named_scope('acc_a'):
                    accumulate((k,), 128, 256, 0)

            @pl.when(tp == 1)
            def _():
                with jax.named_scope('w_fwd'):
                    drain(xs.at[k, pl.ds(128, BLK), :], fwd_recv.at[k])
                with jax.named_scope('acc_y'):
                    accumulate((k,), 128, 128, 0)

        @pl.when((tp == 1) & (i >= 6))
        def _():
            k = diag_order(i - 6)
            with jax.named_scope('w_fwd'):
                drain(xs.at[k, pl.ds(256, BLK), :], fwd_recv.at[NK + LATE + k])
            with jax.named_scope('acc_d'):
                accumulate((k,), 256, 128, 128)

    for col, n in NSTEPS:
        for s in range(4):
            put_qkv(2 + s, col, n, acc[s * BLK:(s + 1) * BLK, col:col + n])

    def rest_of_rows():
        def wait_fwd2(j):
            with jax.named_scope('w_fwd2'):
                drain(xs.at[0, pl.ds(384, 128), :], fwd_recv.at[NK + j])

        @pl.loop(0, LATE)
        def _(j):
            @pl.when(tp == 0)
            def _():
                with jax.named_scope('h_d2'):
                    handle(j, 2)
                    handle(j + LATE, 2)

            @pl.when(tp == 1)
            def _():
                with jax.named_scope('h_x2'):
                    handle(j + LATE, 1)

            @pl.when(j > 0)
            def _():
                wait_fwd2(j - 1)
                with jax.named_scope('acc_b'):
                    accumulate((j - 1, j - 1 + LATE), 384, 128, 256)

        wait_fwd2(LATE - 1)
        with jax.named_scope('acc_b'):
            for col, n in NSTEPS:
                val = acc[256:384, col:col + n]
                for k in (LATE - 1, NK - 1):
                    val += jnp.dot(xs[k, 384:512, :], w[k * KC:(k + 1) * KC, col:col + n], preferred_element_type=F32)
                for s in range(2):
                    put_qkv(6 + s, col, n, val[s * BLK:(s + 1) * BLK])

    inv_sqrt = E ** -0.5

    def o_copy(b, half, dev_cp):
        lohi, part = b // 4, pl.ds(half * HALF, HALF)
        return remote(osend.at[b, part], ofull.at[lohi, part, pl.ds(pl.multiple_of(cp * HE, E), HE)],
                      o_send_sem, o_recv_sem.at[jnp.where(lohi == tp, 4, 2 * half + jnp.where(x == dev_cp // 2, 0, 1))], {'cp': dev_cp, 'tp': tp})

    def attend(b):
        length = 128 * (b // 2 + 1)
        ri = lax.broadcasted_iota(jnp.int32, (BLK, 128), 0) + BLK * (b % 2)
        ci = lax.broadcasted_iota(jnp.int32, (BLK, 128), 1)
        mask = ci <= ri
        heads = range(HEADS)
        q = [qkv[b * BLK:(b + 1) * BLK, h * E:(h + 1) * E] for h in heads]
        kk = [qkv[0:length, HE + h * E:HE + (h + 1) * E] for h in heads]
        v = [qkv[0:length, 2 * HE + h * E:2 * HE + (h + 1) * E] for h in heads]
        s = [lax.dot_general(q[h], kk[h], (((1,), (1,)), ((), ())), preferred_element_type=F32) * inv_sqrt for h in heads]
        last = [jnp.where(mask, s[h][:, length - 128:], NEG_BIG) for h in heads]
        s = [last[h] if length == 128 else jnp.concatenate([s[h][:, :length - 128], last[h]], axis=1) for h in heads]
        m = [jnp.max(s[h], axis=-1, keepdims=True) for h in heads]
        p = [jnp.exp(s[h] - m[h]) for h in heads]
        l = [jnp.sum(p[h], axis=-1, keepdims=True) for h in heads]
        o = [jnp.dot(p[h].astype(BF16), v[h], preferred_element_type=F32) for h in heads]
        for h in heads:
            osend[b, :, h * E:(h + 1) * E] = (o[h] / l[h]).astype(BF16)
        r = b if b < 4 else 7 - b

        @pl.when(cp == r)
        def _():
            ofull[b // 4, :, pl.ds(pl.multiple_of(cp * HE, E), HE)] = osend[b]

        @pl.when(cp != r)
        def _():
            for half in range(2):
                o_copy(b, half, r).start()

    def wait_o(half, far):
        drain(osend.at[pl.ds(0, 1 + far), pl.ds(0, HALF)], o_recv_sem.at[2 * half + far])

    def attend_blocks(hi):
        @pl.loop(0, 4)
        def _(step):
            first = step < 2
            pair = jnp.where(hi, jnp.where(first, 2 + x, 3 - x), jnp.where(first, 1 - x, x))
            block = 2 * pair + jnp.where(hi, step % 2, 1 - step % 2)
            for b in range(8):
                @pl.when(block == b)
                def _():
                    with jax.named_scope(f'attend{b}'):
                        attend(b)

    away, home = 1 - tp, tp

    def y_copy(n, half):
        part = pl.ds(half * HALF, HALF)
        return remote(ysend.at[n, part], yrecv.at[n, part], y_send_sem, y_recv_sem.at[n], yn)

    def project_away():
        near = pl.ds(pl.multiple_of(2 * x * HE, E), 2 * HE)
        far = pl.ds(pl.multiple_of(2 * (1 - x) * HE, E), 2 * HE)
        top, bottom = slice(0, HALF), slice(HALF, BLK)
        drain(wo, wo_sem)
        with jax.named_scope('wait_o_away'):
            wait_o(0, 0)
        with jax.named_scope('proj'):
            ysend[0, top] = jnp.dot(ofull[away, top, near], wo[0, near, :], preferred_element_type=F32)
        with jax.named_scope('wait_o_away'):
            wait_o(0, 1)
        with jax.named_scope('proj'):
            ysend[0, top] += jnp.dot(ofull[away, top, far], wo[0, far, :], preferred_element_type=F32)
        y_copy(0, 0).start()

        @pl.loop(1, NOUT)
        def _(n):
            with jax.named_scope('proj'):
                ysend[n, top] = jnp.dot(ofull[away, top], wo[n], preferred_element_type=F32)
            y_copy(n, 0).start()

        with jax.named_scope('wait_o_away'):
            wait_o(1, 0)
            wait_o(1, 1)

        @pl.loop(0, NOUT)
        def _(n):
            with jax.named_scope('proj'):
                ysend[n, bottom] = jnp.dot(ofull[away, bottom], wo[n], preferred_element_type=F32)
            y_copy(n, 1).start()

    @pl.loop(0, 4)
    def _(stage):
        @pl.when(stage == 2 * tp)
        def _():
            rest_of_rows()

        @pl.when((stage == 1 - tp) | (stage == 3))
        def _():
            attend_blocks((stage < 2) == (tp == 0))

        @pl.when(stage == 2 - tp)
        def _():
            project_away()

    with jax.named_scope('wait_o_home'):
        drain(osend.at[pl.ds(0, 3)], o_recv_sem.at[4])

    def kept(n):
        return acc.at[pl.ds(pl.multiple_of(n % 6 * BLK, BLK), BLK), pl.ds(pl.multiple_of(n // 6 * NC, NC), NC)]

    @pl.loop(0, NOUT)
    def _(n):
        kept(n)[...] = jnp.dot(ofull[home], wo[n], preferred_element_type=F32)

    @pl.loop(0, NOUT)
    def _(n):
        with jax.named_scope('wait_y'):
            drain(yrecv.at[n], y_recv_sem.at[n])
        y_ref[:, pl.ds(pl.multiple_of(n * NC, NC), NC)] = (kept(n)[...] + yrecv[n]).astype(BF16)

    drain(xs.at[:, pl.ds(0, 3 * BLK), :], own_send)
    drain(xs.at[:, pl.ds(0, 3 * BLK), :], fwd_send)
    for t in range(2):
        for xx in range(2):
            over_x = DIAG_X * BLK if t else (NK - LATE) * BLK + (1 - xx) * HALF
            over_y = LATE * BLK - xx * HALF if t else (NK - DIAG_X) * BLK

            @pl.when((tp == t) & (x == xx))
            def _():
                drain(xs.at[0, pl.ds(0, over_x), :], dg_send.at[0])
                drain(xs.at[0, pl.ds(0, over_y), :], dg_send.at[1])
    drain(osend.at[pl.ds(0, 6)], o_send_sem)
    drain(ysend, y_send_sem)


def solution(mesh):
    def device_fn(x_loc, w_q, w_k, w_v, w_o):
        dma = pltpu.SemaphoreType.DMA
        heads_major = [jnp.transpose(t, (1, 0, 2)) for t in (w_q, w_k, w_v)]
        return pl.pallas_call(
            kernel,
            name='attention_layer',
            out_shape=pltpu.VMEM((BLK, D), BF16),
            in_specs=[pl.BlockSpec(memory_space=pl.ANY)] * 5,
            out_specs=pl.BlockSpec(memory_space=pltpu.VMEM),
            scratch_shapes=[
                pltpu.VMEM((NK, 512, KC), BF16),
                pltpu.VMEM((D, NQKV), BF16),
                pltpu.VMEM((NOUT, 20 * E, NC), BF16),
                pltpu.VMEM((512, NQKV), BF16),
                pltpu.VMEM((384, NQKV), F32),
                pltpu.VMEM((8, BLK, HE), BF16),
                pltpu.VMEM((2, BLK, 20 * E), BF16),
                pltpu.VMEM((NOUT, BLK, NC), F32),
                pltpu.VMEM((NOUT, BLK, NC), F32),
                dma, dma, dma,
                dma, dma, dma((3, NK)),
                dma, dma((2 * NK + LATE,)), dma((2,)),
                dma, dma((5,)),
                dma, dma((NOUT,)),
            ],
            compiler_params=pltpu.CompilerParams(collective_id=0, has_side_effects=True, vmem_limit_bytes=64 * 1000 * 1000),
        )(x_loc, *heads_major, w_o.reshape(20 * E, D))

    seq_spec = P(('dp', 'cp', 'tp'), None)
    head_spec = P(None, 'tp', None)
    return jax.shard_map(device_fn, mesh=mesh, in_specs=(seq_spec, head_spec, head_spec, head_spec, P('tp', None, None)), out_specs=seq_spec, check_vma=False)
```

```python
import functools

import jax
import jax.numpy as jnp
from jax import lax
from jax.experimental import pallas as pl
from jax.experimental.pallas import tpu as pltpu
from jax.sharding import PartitionSpec as P


BF16, F32 = jnp.bfloat16, jnp.float32
NEG_BIG = -1e30
D = 5120
E = 128
HEADS = 5
HE = HEADS * E
NQKV = 3 * HE
BLK = 64
HALF = BLK // 2
NK = 10
KC = D // NK
LATE = NK // 2
DIAG_X = 7
NOUT = 10
NC = D // NOUT
MESH = pl.DeviceIdType.MESH


def remote(src, dst, send_sem, recv_sem, dev):
    return pltpu.make_async_remote_copy(src_ref=src, dst_ref=dst, send_sem=send_sem, recv_sem=recv_sem, device_id=dev, device_id_type=MESH)


def drain(ref, sem):
    pltpu.make_async_copy(ref, ref, sem).wait()


def kernel(x_hbm, wq_hbm, wk_hbm, wv_hbm, wo_hbm, y_ref, xs, w, wo, qkv, acc, osend, ofull, ysend, yrecv,
           xin_sem, w_sem, wo_sem, own_send, sib_recv, direct_recv, fwd_send, fwd_recv, dg_send, o_send_sem, o_recv_sem,
           y_send_sem, y_recv_sem):
    cp, tp = lax.axis_index('cp'), lax.axis_index('tp')
    x, c = cp // 2, cp % 2
    sib = {'cp': 2 * x + 1 - c, 'tp': tp}
    xn = {'cp': 2 * (1 - x) + c, 'tp': tp}
    xo = {'cp': 2 * (1 - x) + 1 - c, 'tp': tp}
    yn = {'cp': cp, 'tp': 1 - tp}

    def rows(group, core):
        return pl.ds(pl.multiple_of(group * 128 + core * BLK, BLK), BLK)

    def x_in(k):
        return pltpu.make_async_copy(x_hbm.at[:, pl.ds(k * KC, KC)], xs.at[k, rows(0, c), :], xin_sem)

    def w_in(j):
        src = (wq_hbm, wk_hbm, wv_hbm)[j // HEADS].at[cp * HEADS + j % HEADS]
        return pltpu.make_async_copy(src, w.at[:, pl.ds(j * E, E)], w_sem)

    def wo_in(n):
        return pltpu.make_async_copy(wo_hbm.at[:, pl.ds(n * NC, NC)], wo.at[n], wo_sem)

    for k in range(NK):
        x_in(k).start()
    barrier = pltpu.get_barrier_semaphore()
    for dev in (sib, xn, xo, yn):
        pl.semaphore_signal(barrier, inc=1, device_id=dev, device_id_type=MESH)
    drain(xs.at[:, rows(0, c), :], xin_sem)
    for j in range(3 * HEADS):
        w_in(j).start()
    with jax.named_scope('barrier'):
        pl.semaphore_wait(barrier, 4)

    def group_of(kind, t):
        return (1, 2 + t, 3 - t, 0)[kind]

    def own(k, kind):
        dev, t = ((yn, 1 - tp), (xn, tp), None, (sib, tp))[kind]
        return remote(xs.at[k, rows(0, c), :], xs.at[k, rows(group_of(kind, t), c), :], own_send, sib_recv if kind == 3 else direct_recv.at[kind, k], dev)

    def diag(k, over_y):
        dev, src, t = (yn, group_of(1, tp), 1 - tp) if over_y else (xn, group_of(0, tp), tp)
        return remote(xs.at[k, rows(src, c), :], xs.at[k, rows(group_of(2, t), c), :], dg_send.at[int(over_y)], direct_recv.at[2, k], dev)

    def half_diag(over_y):
        dev, src, t = (yn, group_of(1, tp), 1 - tp) if over_y else (xn, group_of(0, tp), tp)
        k, first = LATE - 1, 0 if over_y else HALF
        return remote(xs.at[k, pl.ds(pl.multiple_of(src * 128 + c * BLK + first, HALF), HALF), :],
                      xs.at[k, pl.ds(pl.multiple_of(group_of(2, t) * 128 + c * BLK + first, HALF), HALF), :],
                      dg_send.at[int(over_y)], direct_recv.at[2, k], dev)

    def fwd(k, kind):
        sl = rows(group_of(kind, tp), c)
        second = NK + k % LATE
        sem = (k, jnp.where(tp == 0, k, second), jnp.where(tp == 0, second, NK + LATE + k))[kind]
        return remote(xs.at[k, sl, :], xs.at[k, sl, :], fwd_send, fwd_recv.at[sem], sib)

    def direct_wait(k, kind):
        drain(xs.at[k, rows(group_of(kind, tp), c), :], direct_recv.at[kind, k])

    def sends_diag_x(k):
        return jnp.where(tp == 0, k >= LATE, k < DIAG_X)

    def sends_half_x(k):
        return (tp == 0) & (x == 0) & (k == LATE - 1)

    def sends_diag_y(k):
        return jnp.where(tp == 0, k >= DIAG_X, k < LATE - x)

    def sends_half_y(k):
        return (tp == 1) & (x == 1) & (k == LATE - 1)

    def handle(k, kind):
        direct_wait(k, kind)
        fwd(k, kind).start()
        if kind == 0:
            @pl.when(sends_diag_x(k))
            def _():
                diag(k, False).start()

            @pl.when(sends_half_x(k))
            def _():
                half_diag(False).start()
        if kind == 1:
            @pl.when(sends_diag_y(k))
            def _():
                diag(k, True).start()

            @pl.when(sends_half_y(k))
            def _():
                half_diag(True).start()

    for k in range(NK):
        if k < LATE:
            own(k, 1).start()
        else:
            @pl.when(tp == 0)
            def _():
                own(k, 1).start()
        own(k, 0).start()
        own(k, 3).start()

    acc[...] = jnp.zeros_like(acc)

    def nat(xx, core, t):
        b = 2 * xx + core
        return jnp.where(t == 0, b, 7 - b) * BLK

    nat_of = [nat(x, 0, tp), nat(x, 1, tp), nat(x, 0, 1 - tp), nat(x, 1, 1 - tp),
              nat(1 - x, 0, 0), nat(1 - x, 1, 0), nat(1 - x, 0, 1), nat(1 - x, 1, 1)]

    def put_qkv(slot, col, n, val):
        qkv[pl.ds(pl.multiple_of(nat_of[slot], BLK), BLK), pl.ds(col, n)] = val.astype(BF16)

    NSTEPS = ((0, 512), (512, 512), (1024, 512), (1536, 384))

    def own_chip():
        with jax.named_scope('wait_sib'):
            drain(xs.at[:, rows(0, c), :], sib_recv)
        with jax.named_scope('wait_w'):
            drain(w, w_sem)
        for n in range(NOUT):
            wo_in(n).start()
        for col, n in NSTEPS:
            val = jnp.dot(xs[0, 0:128, :], w[0:KC, col:col + n], preferred_element_type=F32)
            for k in range(1, NK):
                val += jnp.dot(xs[k, 0:128, :], w[k * KC:(k + 1) * KC, col:col + n], preferred_element_type=F32)
            put_qkv(0, col, n, val[:BLK])
            put_qkv(1, col, n, val[BLK:])

    def accumulate(chunks, row, m, arow):
        for col, n in NSTEPS:
            val = acc[arow:arow + m, col:col + n]
            for k in chunks:
                val += jnp.dot(xs[k, row:row + m, :], w[pl.ds(pl.multiple_of(k * KC, KC), KC), col:col + n], preferred_element_type=F32)
            acc[arow:arow + m, col:col + n] = val

    def diag_order(m):
        return jnp.where(m < 5, m, jnp.where(m % 2 == 1, 7 + (m - 5) // 2, 5 + (m - 6) // 2))

    def wait_fwd2(j):
        with jax.named_scope('w_fwd2'):
            drain(xs.at[0, pl.ds(384, 128), :], fwd_recv.at[NK + j])

    def pair(j):
        wait_fwd2(j)
        with jax.named_scope('acc_b'):
            accumulate((j, j + LATE), 384, 128, 256)

    @pl.loop(0, NK + 6)
    def _(i):
        @pl.when(i < NK)
        def _():
            with jax.named_scope('h_y'):
                handle(i, 0)

        @pl.when(i < jnp.where(tp == 0, NK, LATE))
        def _():
            with jax.named_scope('h_x'):
                handle(i, 1)

        @pl.when((tp == 1) & (i == DIAG_X - 1))
        def _():
            for k in range(LATE, NK):
                own(k, 1).start()

        @pl.when((tp == 0) & (i >= NK) & (i < NK + LATE))
        def _():
            with jax.named_scope('h_d2'):
                handle(i - NK, 2)
                handle(i - NK + LATE, 2)

        @pl.when((tp == 1) & (i >= 5) & (i < NK + 5))
        def _():
            with jax.named_scope('h_d'):
                handle(diag_order(i - 5), 2)

        @pl.when(i == 2)
        def _():
            own_chip()

        @pl.when((i >= 2) & (i < NK + 2))
        def _():
            k = i - 2

            @pl.when(tp == 0)
            def _():
                with jax.named_scope('w_fwd'):
                    drain(xs.at[k, pl.ds(128, 128), :], fwd_recv.at[k])
                with jax.named_scope('acc_a'):
                    accumulate((k,), 128, 256, 0)

            @pl.when(tp == 1)
            def _():
                with jax.named_scope('w_fwd'):
                    drain(xs.at[k, pl.ds(128, BLK), :], fwd_recv.at[k])
                with jax.named_scope('acc_y'):
                    accumulate((k,), 128, 128, 0)

        @pl.when((tp == 1) & (i >= 6))
        def _():
            k = diag_order(i - 6)
            with jax.named_scope('w_fwd'):
                drain(xs.at[k, pl.ds(256, BLK), :], fwd_recv.at[NK + LATE + k])
            with jax.named_scope('acc_d'):
                accumulate((k,), 256, 128, 128)

        @pl.when((tp == 0) & (i > NK) & (i < NK + LATE))
        def _():
            pair(i - NK - 1)

    for col, n in NSTEPS:
        for s in range(4):
            put_qkv(2 + s, col, n, acc[s * BLK:(s + 1) * BLK, col:col + n])

    def rest_of_rows():
        @pl.when(tp == 1)
        def _():
            @pl.loop(0, LATE)
            def _(j):
                with jax.named_scope('h_x2'):
                    handle(j + LATE, 1)

                @pl.when(j > 0)
                def _():
                    pair(j - 1)

        wait_fwd2(LATE - 1)
        with jax.named_scope('acc_b'):
            for col, n in NSTEPS:
                val = acc[256:384, col:col + n]
                for k in (LATE - 1, NK - 1):
                    val += jnp.dot(xs[k, 384:512, :], w[k * KC:(k + 1) * KC, col:col + n], preferred_element_type=F32)
                for s in range(2):
                    put_qkv(6 + s, col, n, val[s * BLK:(s + 1) * BLK])

    inv_sqrt = E ** -0.5

    def o_copy(b, half, dev_cp):
        lohi, part = b // 4, pl.ds(half * HALF, HALF)
        return remote(osend.at[b, part], ofull.at[lohi, part, pl.ds(pl.multiple_of(cp * HE, E), HE)],
                      o_send_sem, o_recv_sem.at[jnp.where(lohi == tp, 4, 2 * half + jnp.where(x == dev_cp // 2, 0, 1))], {'cp': dev_cp, 'tp': tp})

    def attend(b):
        length = 128 * (b // 2 + 1)
        ri = lax.broadcasted_iota(jnp.int32, (BLK, 128), 0) + BLK * (b % 2)
        ci = lax.broadcasted_iota(jnp.int32, (BLK, 128), 1)
        mask = ci <= ri
        heads = range(HEADS)
        q = [qkv[b * BLK:(b + 1) * BLK, h * E:(h + 1) * E] for h in heads]
        kk = [qkv[0:length, HE + h * E:HE + (h + 1) * E] for h in heads]
        v = [qkv[0:length, 2 * HE + h * E:2 * HE + (h + 1) * E] for h in heads]
        s = [lax.dot_general(q[h], kk[h], (((1,), (1,)), ((), ())), preferred_element_type=F32) * inv_sqrt for h in heads]
        last = [jnp.where(mask, s[h][:, length - 128:], NEG_BIG) for h in heads]
        s = [last[h] if length == 128 else jnp.concatenate([s[h][:, :length - 128], last[h]], axis=1) for h in heads]
        m = [jnp.max(s[h], axis=-1, keepdims=True) for h in heads]
        p = [jnp.exp(s[h] - m[h]) for h in heads]
        l = [jnp.sum(p[h], axis=-1, keepdims=True) for h in heads]
        o = [jnp.dot(p[h].astype(BF16), v[h], preferred_element_type=F32) for h in heads]
        for h in heads:
            osend[b, :, h * E:(h + 1) * E] = (o[h] / l[h]).astype(BF16)
        r = b if b < 4 else 7 - b

        @pl.when(cp == r)
        def _():
            ofull[b // 4, :, pl.ds(pl.multiple_of(cp * HE, E), HE)] = osend[b]

        @pl.when(cp != r)
        def _():
            for half in range(2):
                o_copy(b, half, r).start()

    def wait_o(half, far):
        drain(osend.at[pl.ds(0, 1 + far), pl.ds(0, HALF)], o_recv_sem.at[2 * half + far])

    def attend_blocks(hi):
        @pl.loop(0, 4)
        def _(step):
            first = step < 2
            pair = jnp.where(hi, jnp.where(first, 2 + x, 3 - x), jnp.where(first, 1 - x, x))
            block = 2 * pair + jnp.where(hi, step % 2, 1 - step % 2)
            for b in range(8):
                @pl.when(block == b)
                def _():
                    with jax.named_scope(f'attend{b}'):
                        attend(b)

    away, home = 1 - tp, tp

    def y_copy(n, half):
        part = pl.ds(half * HALF, HALF)
        return remote(ysend.at[n, part], yrecv.at[n, part], y_send_sem, y_recv_sem.at[n], yn)

    def project_away():
        near = pl.ds(pl.multiple_of(2 * x * HE, E), 2 * HE)
        far = pl.ds(pl.multiple_of(2 * (1 - x) * HE, E), 2 * HE)
        top, bottom = slice(0, HALF), slice(HALF, BLK)
        drain(wo, wo_sem)
        with jax.named_scope('wait_o_away'):
            wait_o(0, 0)
        with jax.named_scope('proj'):
            ysend[0, top] = jnp.dot(ofull[away, top, near], wo[0, near, :], preferred_element_type=F32)
        with jax.named_scope('wait_o_away'):
            wait_o(0, 1)
        with jax.named_scope('proj'):
            ysend[0, top] += jnp.dot(ofull[away, top, far], wo[0, far, :], preferred_element_type=F32)
        y_copy(0, 0).start()

        @pl.loop(1, NOUT)
        def _(n):
            with jax.named_scope('proj'):
                ysend[n, top] = jnp.dot(ofull[away, top], wo[n], preferred_element_type=F32)
            y_copy(n, 0).start()

        with jax.named_scope('wait_o_away'):
            wait_o(1, 0)
            wait_o(1, 1)

        @pl.loop(0, NOUT)
        def _(n):
            with jax.named_scope('proj'):
                ysend[n, bottom] = jnp.dot(ofull[away, bottom], wo[n], preferred_element_type=F32)
            y_copy(n, 1).start()

    @pl.loop(0, 4)
    def _(stage):
        @pl.when(stage == 2 * tp)
        def _():
            rest_of_rows()

        @pl.when((stage == 1 - tp) | (stage == 3))
        def _():
            attend_blocks((stage < 2) == (tp == 0))

        @pl.when(stage == 2 - tp)
        def _():
            project_away()

    with jax.named_scope('wait_o_home'):
        drain(osend.at[pl.ds(0, 3)], o_recv_sem.at[4])

    def kept(n):
        return acc.at[pl.ds(pl.multiple_of(n % 6 * BLK, BLK), BLK), pl.ds(pl.multiple_of(n // 6 * NC, NC), NC)]

    @pl.loop(0, NOUT)
    def _(n):
        kept(n)[...] = jnp.dot(ofull[home], wo[n], preferred_element_type=F32)

    @pl.loop(0, NOUT)
    def _(n):
        with jax.named_scope('wait_y'):
            drain(yrecv.at[n], y_recv_sem.at[n])
        y_ref[:, pl.ds(pl.multiple_of(n * NC, NC), NC)] = (kept(n)[...] + yrecv[n]).astype(BF16)

    drain(xs.at[:, pl.ds(0, 3 * BLK), :], own_send)
    drain(xs.at[:, pl.ds(0, 3 * BLK), :], fwd_send)
    for t in range(2):
        for xx in range(2):
            over_x = DIAG_X * BLK if t else (NK - LATE) * BLK + (1 - xx) * HALF
            over_y = LATE * BLK - xx * HALF if t else (NK - DIAG_X) * BLK

            @pl.when((tp == t) & (x == xx))
            def _():
                drain(xs.at[0, pl.ds(0, over_x), :], dg_send.at[0])
                drain(xs.at[0, pl.ds(0, over_y), :], dg_send.at[1])
    drain(osend.at[pl.ds(0, 6)], o_send_sem)
    drain(ysend, y_send_sem)


def solution(mesh):
    def device_fn(x_loc, w_q, w_k, w_v, w_o):
        dma = pltpu.SemaphoreType.DMA
        heads_major = [jnp.transpose(t, (1, 0, 2)) for t in (w_q, w_k, w_v)]
        return pl.pallas_call(
            kernel,
            name='attention_layer',
            out_shape=pltpu.VMEM((BLK, D), BF16),
            in_specs=[pl.BlockSpec(memory_space=pl.ANY)] * 5,
            out_specs=pl.BlockSpec(memory_space=pltpu.VMEM),
            scratch_shapes=[
                pltpu.VMEM((NK, 512, KC), BF16),
                pltpu.VMEM((D, NQKV), BF16),
                pltpu.VMEM((NOUT, 20 * E, NC), BF16),
                pltpu.VMEM((512, NQKV), BF16),
                pltpu.VMEM((384, NQKV), F32),
                pltpu.VMEM((8, BLK, HE), BF16),
                pltpu.VMEM((2, BLK, 20 * E), BF16),
                pltpu.VMEM((NOUT, BLK, NC), F32),
                pltpu.VMEM((NOUT, BLK, NC), F32),
                dma, dma, dma,
                dma, dma, dma((3, NK)),
                dma, dma((2 * NK + LATE,)), dma((2,)),
                dma, dma((5,)),
                dma, dma((NOUT,)),
            ],
            compiler_params=pltpu.CompilerParams(collective_id=0, has_side_effects=True, vmem_limit_bytes=64 * 1000 * 1000),
        )(x_loc, *heads_major, w_o.reshape(20 * E, D))

    seq_spec = P(('dp', 'cp', 'tp'), None)
    head_spec = P(None, 'tp', None)
    return jax.shard_map(device_fn, mesh=mesh, in_specs=(seq_spec, head_spec, head_spec, head_spec, P('tp', None, None)), out_specs=seq_spec, check_vma=False)
```

```python
import functools

import jax
import jax.numpy as jnp
from jax import lax
from jax.experimental import pallas as pl
from jax.experimental.pallas import tpu as pltpu
from jax.sharding import PartitionSpec as P


BF16, F32 = jnp.bfloat16, jnp.float32
NEG_BIG = -1e30
D = 5120
E = 128
HEADS = 5
HE = HEADS * E
NQKV = 3 * HE
BLK = 64
HALF = BLK // 2
NK = 10
KC = D // NK
LATE = NK // 2
DIAG_X = 7
NOUT = 10
NC = D // NOUT
MESH = pl.DeviceIdType.MESH


def remote(src, dst, send_sem, recv_sem, dev):
    return pltpu.make_async_remote_copy(src_ref=src, dst_ref=dst, send_sem=send_sem, recv_sem=recv_sem, device_id=dev, device_id_type=MESH)


def drain(ref, sem):
    pltpu.make_async_copy(ref, ref, sem).wait()


def kernel(x_hbm, wq_hbm, wk_hbm, wv_hbm, wo_hbm, y_ref, xs, w, wo, qkv, acc, osend, ofull, ysend, yrecv,
           xin_sem, w_sem, wo_sem, own_send, sib_recv, direct_recv, fwd_send, fwd_recv, dg_send, o_send_sem, o_recv_sem,
           y_send_sem, y_recv_sem):
    cp, tp = lax.axis_index('cp'), lax.axis_index('tp')
    x, c = cp // 2, cp % 2
    sib = {'cp': 2 * x + 1 - c, 'tp': tp}
    xn = {'cp': 2 * (1 - x) + c, 'tp': tp}
    xo = {'cp': 2 * (1 - x) + 1 - c, 'tp': tp}
    yn = {'cp': cp, 'tp': 1 - tp}

    def rows(group, core):
        return pl.ds(pl.multiple_of(group * 128 + core * BLK, BLK), BLK)

    def x_in(k):
        return pltpu.make_async_copy(x_hbm.at[:, pl.ds(k * KC, KC)], xs.at[k, rows(0, c), :], xin_sem)

    def w_in(j):
        src = (wq_hbm, wk_hbm, wv_hbm)[j // HEADS].at[cp * HEADS + j % HEADS]
        return pltpu.make_async_copy(src, w.at[:, pl.ds(j * E, E)], w_sem)

    def wo_in(n):
        return pltpu.make_async_copy(wo_hbm.at[:, pl.ds(n * NC, NC)], wo.at[n], wo_sem)

    for k in range(NK):
        x_in(k).start()
    barrier = pltpu.get_barrier_semaphore()
    for dev in (sib, xn, xo, yn):
        pl.semaphore_signal(barrier, inc=1, device_id=dev, device_id_type=MESH)
    drain(xs.at[:, rows(0, c), :], xin_sem)
    for j in range(3 * HEADS):
        w_in(j).start()
    with jax.named_scope('barrier'):
        pl.semaphore_wait(barrier, 4)

    def group_of(kind, t):
        return (1, 2 + t, 3 - t, 0)[kind]

    def own(k, kind):
        dev, t = ((yn, 1 - tp), (xn, tp), None, (sib, tp))[kind]
        return remote(xs.at[k, rows(0, c), :], xs.at[k, rows(group_of(kind, t), c), :], own_send, sib_recv if kind == 3 else direct_recv.at[kind, k], dev)

    def diag(k, over_y):
        dev, src, t = (yn, group_of(1, tp), 1 - tp) if over_y else (xn, group_of(0, tp), tp)
        return remote(xs.at[k, rows(src, c), :], xs.at[k, rows(group_of(2, t), c), :], dg_send.at[int(over_y)], direct_recv.at[2, k], dev)

    def half_diag(over_y):
        dev, src, t = (yn, group_of(1, tp), 1 - tp) if over_y else (xn, group_of(0, tp), tp)
        k, first = LATE - 1, 0 if over_y else HALF
        return remote(xs.at[k, pl.ds(pl.multiple_of(src * 128 + c * BLK + first, HALF), HALF), :],
                      xs.at[k, pl.ds(pl.multiple_of(group_of(2, t) * 128 + c * BLK + first, HALF), HALF), :],
                      dg_send.at[int(over_y)], direct_recv.at[2, k], dev)

    def fwd(k, kind):
        sl = rows(group_of(kind, tp), c)
        second = NK + k % LATE
        sem = (k, jnp.where(tp == 0, k, second), jnp.where(tp == 0, second, NK + LATE + k))[kind]
        return remote(xs.at[k, sl, :], xs.at[k, sl, :], fwd_send, fwd_recv.at[sem], sib)

    def direct_wait(k, kind):
        drain(xs.at[k, rows(group_of(kind, tp), c), :], direct_recv.at[kind, k])

    def sends_diag_x(k):
        return jnp.where(tp == 0, k >= LATE, k < DIAG_X)

    def sends_half_x(k):
        return (tp == 0) & (x == 0) & (k == LATE - 1)

    def sends_diag_y(k):
        return jnp.where(tp == 0, k >= DIAG_X, k < LATE - x)

    def sends_half_y(k):
        return (tp == 1) & (x == 1) & (k == LATE - 1)

    def handle(k, kind):
        direct_wait(k, kind)
        fwd(k, kind).start()
        if kind == 0:
            @pl.when(sends_diag_x(k))
            def _():
                diag(k, False).start()

            @pl.when(sends_half_x(k))
            def _():
                half_diag(False).start()
        if kind == 1:
            @pl.when(sends_diag_y(k))
            def _():
                diag(k, True).start()

            @pl.when(sends_half_y(k))
            def _():
                half_diag(True).start()

    for k in range(NK):
        if k < LATE:
            own(k, 1).start()
        else:
            @pl.when(tp == 0)
            def _():
                own(k, 1).start()
        own(k, 0).start()
        own(k, 3).start()

    acc[...] = jnp.zeros_like(acc)

    def nat(xx, core, t):
        b = 2 * xx + core
        return jnp.where(t == 0, b, 7 - b) * BLK

    nat_of = [nat(x, 0, tp), nat(x, 1, tp), nat(x, 0, 1 - tp), nat(x, 1, 1 - tp),
              nat(1 - x, 0, 0), nat(1 - x, 1, 0), nat(1 - x, 0, 1), nat(1 - x, 1, 1)]

    def put_qkv(slot, col, n, val):
        qkv[pl.ds(pl.multiple_of(nat_of[slot], BLK), BLK), pl.ds(col, n)] = val.astype(BF16)

    NSTEPS = ((0, 512), (512, 512), (1024, 512), (1536, 384))

    def own_chip():
        with jax.named_scope('wait_sib'):
            drain(xs.at[:, rows(0, c), :], sib_recv)
        with jax.named_scope('wait_w'):
            drain(w, w_sem)
        for n in range(NOUT):
            wo_in(n).start()
        for col, n in NSTEPS:
            val = jnp.dot(xs[0, 0:128, :], w[0:KC, col:col + n], preferred_element_type=F32)
            for k in range(1, NK):
                val += jnp.dot(xs[k, 0:128, :], w[k * KC:(k + 1) * KC, col:col + n], preferred_element_type=F32)
            put_qkv(0, col, n, val[:BLK])
            put_qkv(1, col, n, val[BLK:])

    def accumulate(chunks, row, m, arow):
        for col, n in NSTEPS:
            val = acc[arow:arow + m, col:col + n]
            for k in chunks:
                val += jnp.dot(xs[k, row:row + m, :], w[pl.ds(pl.multiple_of(k * KC, KC), KC), col:col + n], preferred_element_type=F32)
            acc[arow:arow + m, col:col + n] = val

    def diag_order(m):
        return jnp.where(m < 5, m, jnp.where(m % 2 == 1, 7 + (m - 5) // 2, 5 + (m - 6) // 2))

    def wait_fwd2(j):
        with jax.named_scope('w_fwd2'):
            drain(xs.at[0, pl.ds(384, 128), :], fwd_recv.at[NK + j])

    def pair(j):
        wait_fwd2(j)
        with jax.named_scope('acc_b'):
            accumulate((j, j + LATE), 384, 128, 256)

    @pl.loop(0, NK + 6)
    def _(i):
        @pl.when(i < NK)
        def _():
            with jax.named_scope('h_y'):
                handle(i, 0)

        @pl.when(i < jnp.where(tp == 0, NK, LATE))
        def _():
            with jax.named_scope('h_x'):
                handle(i, 1)

        @pl.when((tp == 1) & (i == DIAG_X - 1))
        def _():
            for k in range(LATE, NK):
                own(k, 1).start()

        @pl.when((tp == 0) & (i >= NK) & (i < NK + LATE))
        def _():
            with jax.named_scope('h_d2'):
                handle(i - NK, 2)
                handle(i - NK + LATE, 2)

        @pl.when((tp == 1) & (i >= 5) & (i < NK + 5))
        def _():
            with jax.named_scope('h_d'):
                handle(diag_order(i - 5), 2)

        @pl.when(i == 2)
        def _():
            own_chip()

        @pl.when((i >= 2) & (i < NK + 2))
        def _():
            k = i - 2

            @pl.when(tp == 0)
            def _():
                with jax.named_scope('w_fwd'):
                    drain(xs.at[k, pl.ds(128, 128), :], fwd_recv.at[k])
                with jax.named_scope('acc_a'):
                    accumulate((k,), 128, 256, 0)

            @pl.when(tp == 1)
            def _():
                with jax.named_scope('w_fwd'):
                    drain(xs.at[k, pl.ds(128, BLK), :], fwd_recv.at[k])
                with jax.named_scope('acc_y'):
                    accumulate((k,), 128, 128, 0)

        @pl.when((tp == 1) & (i >= 6))
        def _():
            k = diag_order(i - 6)
            with jax.named_scope('w_fwd'):
                drain(xs.at[k, pl.ds(256, BLK), :], fwd_recv.at[NK + LATE + k])
            with jax.named_scope('acc_d'):
                accumulate((k,), 256, 128, 128)

        @pl.when((tp == 0) & (i > NK) & (i < NK + LATE))
        def _():
            pair(i - NK - 1)

    for col, n in NSTEPS:
        for s in range(4):
            put_qkv(2 + s, col, n, acc[s * BLK:(s + 1) * BLK, col:col + n])

    def rest_of_rows():
        @pl.when(tp == 1)
        def _():
            @pl.loop(0, LATE)
            def _(j):
                with jax.named_scope('h_x2'):
                    handle(j + LATE, 1)

                @pl.when(j > 0)
                def _():
                    pair(j - 1)

        wait_fwd2(LATE - 1)
        with jax.named_scope('acc_b'):
            for col, n in NSTEPS:
                val = acc[256:384, col:col + n]
                for k in (LATE - 1, NK - 1):
                    val += jnp.dot(xs[k, 384:512, :], w[k * KC:(k + 1) * KC, col:col + n], preferred_element_type=F32)
                for s in range(2):
                    put_qkv(6 + s, col, n, val[s * BLK:(s + 1) * BLK])

    inv_sqrt = E ** -0.5

    def o_copy(b, half, dev_cp):
        lohi, part = b // 4, pl.ds(half * HALF, HALF)
        return remote(osend.at[b, part], ofull.at[lohi, part, pl.ds(pl.multiple_of(cp * HE, E), HE)],
                      o_send_sem, o_recv_sem.at[jnp.where(lohi == tp, 4, 2 * half + jnp.where(x == dev_cp // 2, 0, 1))], {'cp': dev_cp, 'tp': tp})

    def attend(b):
        length = 128 * (b // 2 + 1)
        ri = lax.broadcasted_iota(jnp.int32, (BLK, 128), 0) + BLK * (b % 2)
        ci = lax.broadcasted_iota(jnp.int32, (BLK, 128), 1)
        mask = ci <= ri
        heads = range(HEADS)
        q = [qkv[b * BLK:(b + 1) * BLK, h * E:(h + 1) * E] for h in heads]
        kk = [qkv[0:length, HE + h * E:HE + (h + 1) * E] for h in heads]
        v = [qkv[0:length, 2 * HE + h * E:2 * HE + (h + 1) * E] for h in heads]
        s = [lax.dot_general(q[h], kk[h], (((1,), (1,)), ((), ())), preferred_element_type=F32) * inv_sqrt for h in heads]
        last = [jnp.where(mask, s[h][:, length - 128:], NEG_BIG) for h in heads]
        s = [last[h] if length == 128 else jnp.concatenate([s[h][:, :length - 128], last[h]], axis=1) for h in heads]
        m = [jnp.max(s[h], axis=-1, keepdims=True) for h in heads]
        p = [jnp.exp(s[h] - m[h]) for h in heads]
        l = [jnp.sum(p[h], axis=-1, keepdims=True) for h in heads]
        o = [jnp.dot(p[h].astype(BF16), v[h], preferred_element_type=F32) for h in heads]
        for h in heads:
            osend[b, :, h * E:(h + 1) * E] = (o[h] / l[h]).astype(BF16)
    def send_o(b, half):
        r = jnp.where(b < 4, b, 7 - b)

        @pl.when(cp == r)
        def _():
            part = pl.ds(half * HALF, HALF)
            ofull[b // 4, part, pl.ds(pl.multiple_of(cp * HE, E), HE)] = osend[b, part]

        @pl.when(cp != r)
        def _():
            o_copy(b, half, r).start()

    def wait_o(half, far):
        drain(osend.at[pl.ds(0, 1 + far), pl.ds(0, HALF)], o_recv_sem.at[2 * half + far])

    def attend_blocks(hi):
        def block_at(step):
            first = step < 2
            pair = jnp.where(hi, jnp.where(first, 2 + x, 3 - x), jnp.where(first, 1 - x, x))
            return 2 * pair + jnp.where(hi, step % 2, 1 - step % 2)

        @pl.loop(0, 4)
        def _(step):
            block = block_at(step)
            for b in range(8):
                @pl.when(block == b)
                def _():
                    with jax.named_scope(f'attend{b}'):
                        attend(b)
            send_o(block, 0)

            @pl.when(step > 0)
            def _():
                send_o(block_at(step - 1), 1)

        send_o(block_at(3), 1)

    away, home = 1 - tp, tp

    def y_copy(n, half):
        part = pl.ds(half * HALF, HALF)
        return remote(ysend.at[n, part], yrecv.at[n, part], y_send_sem, y_recv_sem.at[n], yn)

    def project_away():
        near = pl.ds(pl.multiple_of(2 * x * HE, E), 2 * HE)
        far = pl.ds(pl.multiple_of(2 * (1 - x) * HE, E), 2 * HE)
        top, bottom = slice(0, HALF), slice(HALF, BLK)
        drain(wo, wo_sem)
        with jax.named_scope('wait_o_away'):
            wait_o(0, 0)
        with jax.named_scope('proj'):
            ysend[0, top] = jnp.dot(ofull[away, top, near], wo[0, near, :], preferred_element_type=F32)
        with jax.named_scope('wait_o_away'):
            wait_o(0, 1)
        with jax.named_scope('proj'):
            ysend[0, top] += jnp.dot(ofull[away, top, far], wo[0, far, :], preferred_element_type=F32)
        y_copy(0, 0).start()

        @pl.loop(1, NOUT)
        def _(n):
            with jax.named_scope('proj'):
                ysend[n, top] = jnp.dot(ofull[away, top], wo[n], preferred_element_type=F32)
            y_copy(n, 0).start()

        with jax.named_scope('wait_o_away'):
            wait_o(1, 0)
            wait_o(1, 1)

        @pl.loop(0, NOUT)
        def _(n):
            with jax.named_scope('proj'):
                ysend[n, bottom] = jnp.dot(ofull[away, bottom], wo[n], preferred_element_type=F32)
            y_copy(n, 1).start()

    @pl.loop(0, 4)
    def _(stage):
        @pl.when(stage == 2 * tp)
        def _():
            rest_of_rows()

        @pl.when((stage == 1 - tp) | (stage == 3))
        def _():
            attend_blocks((stage < 2) == (tp == 0))

        @pl.when(stage == 2 - tp)
        def _():
            project_away()

    with jax.named_scope('wait_o_home'):
        drain(osend.at[pl.ds(0, 3)], o_recv_sem.at[4])

    def kept(n):
        return acc.at[pl.ds(pl.multiple_of(n % 6 * BLK, BLK), BLK), pl.ds(pl.multiple_of(n // 6 * NC, NC), NC)]

    @pl.loop(0, NOUT)
    def _(n):
        kept(n)[...] = jnp.dot(ofull[home], wo[n], preferred_element_type=F32)

    @pl.loop(0, NOUT)
    def _(n):
        with jax.named_scope('wait_y'):
            drain(yrecv.at[n], y_recv_sem.at[n])
        y_ref[:, pl.ds(pl.multiple_of(n * NC, NC), NC)] = (kept(n)[...] + yrecv[n]).astype(BF16)

    drain(xs.at[:, pl.ds(0, 3 * BLK), :], own_send)
    drain(xs.at[:, pl.ds(0, 3 * BLK), :], fwd_send)
    for t in range(2):
        for xx in range(2):
            over_x = DIAG_X * BLK if t else (NK - LATE) * BLK + (1 - xx) * HALF
            over_y = LATE * BLK - xx * HALF if t else (NK - DIAG_X) * BLK

            @pl.when((tp == t) & (x == xx))
            def _():
                drain(xs.at[0, pl.ds(0, over_x), :], dg_send.at[0])
                drain(xs.at[0, pl.ds(0, over_y), :], dg_send.at[1])
    drain(osend.at[pl.ds(0, 6)], o_send_sem)
    drain(ysend, y_send_sem)


def solution(mesh):
    def device_fn(x_loc, w_q, w_k, w_v, w_o):
        dma = pltpu.SemaphoreType.DMA
        heads_major = [jnp.transpose(t, (1, 0, 2)) for t in (w_q, w_k, w_v)]
        return pl.pallas_call(
            kernel,
            name='attention_layer',
            out_shape=pltpu.VMEM((BLK, D), BF16),
            in_specs=[pl.BlockSpec(memory_space=pl.ANY)] * 5,
            out_specs=pl.BlockSpec(memory_space=pltpu.VMEM),
            scratch_shapes=[
                pltpu.VMEM((NK, 512, KC), BF16),
                pltpu.VMEM((D, NQKV), BF16),
                pltpu.VMEM((NOUT, 20 * E, NC), BF16),
                pltpu.VMEM((512, NQKV), BF16),
                pltpu.VMEM((384, NQKV), F32),
                pltpu.VMEM((8, BLK, HE), BF16),
                pltpu.VMEM((2, BLK, 20 * E), BF16),
                pltpu.VMEM((NOUT, BLK, NC), F32),
                pltpu.VMEM((NOUT, BLK, NC), F32),
                dma, dma, dma,
                dma, dma, dma((3, NK)),
                dma, dma((2 * NK + LATE,)), dma((2,)),
                dma, dma((5,)),
                dma, dma((NOUT,)),
            ],
            compiler_params=pltpu.CompilerParams(collective_id=0, has_side_effects=True, vmem_limit_bytes=64 * 1000 * 1000),
        )(x_loc, *heads_major, w_o.reshape(20 * E, D))

    seq_spec = P(('dp', 'cp', 'tp'), None)
    head_spec = P(None, 'tp', None)
    return jax.shard_map(device_fn, mesh=mesh, in_specs=(seq_spec, head_spec, head_spec, head_spec, P('tp', None, None)), out_specs=seq_spec, check_vma=False)
```

```python
import functools

import jax
import jax.numpy as jnp
from jax import lax
from jax.experimental import pallas as pl
from jax.experimental.pallas import tpu as pltpu
from jax.sharding import PartitionSpec as P


BF16, F32 = jnp.bfloat16, jnp.float32
NEG_BIG = -1e30
D = 5120
E = 128
HEADS = 5
HE = HEADS * E
NQKV = 3 * HE
BLK = 64
HALF = BLK // 2
NK = 10
KC = D // NK
LATE = NK // 2
DIAG_X = 7
NOUT = 10
NC = D // NOUT
MESH = pl.DeviceIdType.MESH


def remote(src, dst, send_sem, recv_sem, dev):
    return pltpu.make_async_remote_copy(src_ref=src, dst_ref=dst, send_sem=send_sem, recv_sem=recv_sem, device_id=dev, device_id_type=MESH)


def drain(ref, sem):
    pltpu.make_async_copy(ref, ref, sem).wait()


def kernel(x_hbm, wq_hbm, wk_hbm, wv_hbm, wo_hbm, y_ref, xs, w, wo, qkv, acc, osend, ofull, ysend, yrecv,
           xin_sem, w_sem, wo_sem, own_send, sib_recv, direct_recv, fwd_send, fwd_recv, dg_send, o_send_sem, o_recv_sem,
           y_send_sem, y_recv_sem):
    cp, tp = lax.axis_index('cp'), lax.axis_index('tp')
    x, c = cp // 2, cp % 2
    sib = {'cp': 2 * x + 1 - c, 'tp': tp}
    xn = {'cp': 2 * (1 - x) + c, 'tp': tp}
    xo = {'cp': 2 * (1 - x) + 1 - c, 'tp': tp}
    yn = {'cp': cp, 'tp': 1 - tp}

    def rows(group, core):
        return pl.ds(pl.multiple_of(group * 128 + core * BLK, BLK), BLK)

    def x_in(k):
        return pltpu.make_async_copy(x_hbm.at[:, pl.ds(k * KC, KC)], xs.at[k, rows(0, c), :], xin_sem)

    def w_in(j):
        src = (wq_hbm, wk_hbm, wv_hbm)[j // HEADS].at[cp * HEADS + j % HEADS]
        return pltpu.make_async_copy(src, w.at[:, pl.ds(j * E, E)], w_sem)

    def wo_in(n):
        return pltpu.make_async_copy(wo_hbm.at[:, pl.ds(n * NC, NC)], wo.at[n], wo_sem)

    for k in range(NK):
        x_in(k).start()
    barrier = pltpu.get_barrier_semaphore()
    for dev in (sib, xn, xo, yn):
        pl.semaphore_signal(barrier, inc=1, device_id=dev, device_id_type=MESH)
    drain(xs.at[:, rows(0, c), :], xin_sem)
    for j in range(3 * HEADS):
        w_in(j).start()
    with jax.named_scope('barrier'):
        pl.semaphore_wait(barrier, 4)

    def group_of(kind, t):
        return (1, 2 + t, 3 - t, 0)[kind]

    def own(k, kind):
        dev, t = ((yn, 1 - tp), (xn, tp), None, (sib, tp))[kind]
        return remote(xs.at[k, rows(0, c), :], xs.at[k, rows(group_of(kind, t), c), :], own_send, sib_recv if kind == 3 else direct_recv.at[kind, k], dev)

    def diag(k, over_y):
        dev, src, t = (yn, group_of(1, tp), 1 - tp) if over_y else (xn, group_of(0, tp), tp)
        return remote(xs.at[k, rows(src, c), :], xs.at[k, rows(group_of(2, t), c), :], dg_send.at[int(over_y)], direct_recv.at[2, k], dev)

    def half_diag(over_y):
        dev, src, t = (yn, group_of(1, tp), 1 - tp) if over_y else (xn, group_of(0, tp), tp)
        k, first = LATE - 1, 0 if over_y else HALF
        return remote(xs.at[k, pl.ds(pl.multiple_of(src * 128 + c * BLK + first, HALF), HALF), :],
                      xs.at[k, pl.ds(pl.multiple_of(group_of(2, t) * 128 + c * BLK + first, HALF), HALF), :],
                      dg_send.at[int(over_y)], direct_recv.at[2, k], dev)

    def fwd(k, kind):
        sl = rows(group_of(kind, tp), c)
        second = NK + k % LATE
        sem = (k, jnp.where(tp == 0, k, second), jnp.where(tp == 0, second, NK + LATE + k))[kind]
        return remote(xs.at[k, sl, :], xs.at[k, sl, :], fwd_send, fwd_recv.at[sem], sib)

    def direct_wait(k, kind):
        drain(xs.at[k, rows(group_of(kind, tp), c), :], direct_recv.at[kind, k])

    def sends_diag_x(k):
        return jnp.where(tp == 0, k >= LATE, k < DIAG_X)

    def sends_half_x(k):
        return (tp == 0) & (x == 0) & (k == LATE - 1)

    def sends_diag_y(k):
        return jnp.where(tp == 0, k >= DIAG_X, k < LATE - x)

    def sends_half_y(k):
        return (tp == 1) & (x == 1) & (k == LATE - 1)

    def handle(k, kind):
        direct_wait(k, kind)
        fwd(k, kind).start()
        if kind == 0:
            @pl.when(sends_diag_x(k))
            def _():
                diag(k, False).start()

            @pl.when(sends_half_x(k))
            def _():
                half_diag(False).start()
        if kind == 1:
            @pl.when(sends_diag_y(k))
            def _():
                diag(k, True).start()

            @pl.when(sends_half_y(k))
            def _():
                half_diag(True).start()

    for k in range(NK):
        if k < LATE:
            own(k, 1).start()
        else:
            @pl.when(tp == 0)
            def _():
                own(k, 1).start()
        own(k, 0).start()
        own(k, 3).start()

    acc[...] = jnp.zeros_like(acc)

    def nat(xx, core, t):
        b = 2 * xx + core
        return jnp.where(t == 0, b, 7 - b) * BLK

    nat_of = [nat(x, 0, tp), nat(x, 1, tp), nat(x, 0, 1 - tp), nat(x, 1, 1 - tp),
              nat(1 - x, 0, 0), nat(1 - x, 1, 0), nat(1 - x, 0, 1), nat(1 - x, 1, 1)]

    def put_qkv(slot, col, n, val):
        qkv[pl.ds(pl.multiple_of(nat_of[slot], BLK), BLK), pl.ds(col, n)] = val.astype(BF16)

    NSTEPS = ((0, 512), (512, 512), (1024, 512), (1536, 384))

    def own_chip():
        with jax.named_scope('wait_sib'):
            drain(xs.at[:, rows(0, c), :], sib_recv)
        with jax.named_scope('wait_w'):
            drain(w, w_sem)
        for n in range(NOUT):
            wo_in(n).start()
        for col, n in NSTEPS:
            val = jnp.dot(xs[0, 0:128, :], w[0:KC, col:col + n], preferred_element_type=F32)
            for k in range(1, NK):
                val += jnp.dot(xs[k, 0:128, :], w[k * KC:(k + 1) * KC, col:col + n], preferred_element_type=F32)
            put_qkv(0, col, n, val[:BLK])
            put_qkv(1, col, n, val[BLK:])

    def accumulate(chunks, row, m, arow):
        for col, n in NSTEPS:
            val = acc[arow:arow + m, col:col + n]
            for k in chunks:
                val += jnp.dot(xs[k, row:row + m, :], w[pl.ds(pl.multiple_of(k * KC, KC), KC), col:col + n], preferred_element_type=F32)
            acc[arow:arow + m, col:col + n] = val

    def diag_order(m):
        return jnp.where(m < 5, m, jnp.where(m % 2 == 1, 7 + (m - 5) // 2, 5 + (m - 6) // 2))

    def wait_fwd2(j):
        with jax.named_scope('w_fwd2'):
            drain(xs.at[0, pl.ds(384, 128), :], fwd_recv.at[NK + j])

    def pair(j):
        wait_fwd2(j)
        with jax.named_scope('acc_b'):
            accumulate((j, j + LATE), 384, 128, 256)

    @pl.loop(0, NK + 6)
    def _(i):
        @pl.when(i < NK)
        def _():
            with jax.named_scope('h_y'):
                handle(i, 0)

        @pl.when(i < jnp.where(tp == 0, NK, LATE))
        def _():
            with jax.named_scope('h_x'):
                handle(i, 1)

        @pl.when((tp == 1) & (i == DIAG_X - 1))
        def _():
            for k in range(LATE, NK):
                own(k, 1).start()

        @pl.when((tp == 0) & (i >= NK) & (i < NK + LATE))
        def _():
            with jax.named_scope('h_d2'):
                handle(i - NK, 2)
                handle(i - NK + LATE, 2)

        @pl.when((tp == 1) & (i >= 5) & (i < NK + 5))
        def _():
            with jax.named_scope('h_d'):
                handle(diag_order(i - 5), 2)

        @pl.when(i == 2)
        def _():
            own_chip()

        @pl.when((i >= 2) & (i < NK + 2))
        def _():
            k = i - 2

            @pl.when(tp == 0)
            def _():
                with jax.named_scope('w_fwd'):
                    drain(xs.at[k, pl.ds(128, 128), :], fwd_recv.at[k])
                with jax.named_scope('acc_a'):
                    accumulate((k,), 128, 256, 0)

            @pl.when(tp == 1)
            def _():
                with jax.named_scope('w_fwd'):
                    drain(xs.at[k, pl.ds(128, BLK), :], fwd_recv.at[k])
                with jax.named_scope('acc_y'):
                    accumulate((k,), 128, 128, 0)

        @pl.when((tp == 1) & (i >= 6))
        def _():
            k = diag_order(i - 6)
            with jax.named_scope('w_fwd'):
                drain(xs.at[k, pl.ds(256, BLK), :], fwd_recv.at[NK + LATE + k])
            with jax.named_scope('acc_d'):
                accumulate((k,), 256, 128, 128)

        @pl.when((tp == 0) & (i > NK) & (i < NK + LATE))
        def _():
            pair(i - NK - 1)

    for col, n in NSTEPS:
        for s in range(4):
            put_qkv(2 + s, col, n, acc[s * BLK:(s + 1) * BLK, col:col + n])

    def rest_of_rows():
        @pl.when(tp == 1)
        def _():
            @pl.loop(0, LATE)
            def _(j):
                with jax.named_scope('h_x2'):
                    handle(j + LATE, 1)

                @pl.when(j > 0)
                def _():
                    pair(j - 1)

        wait_fwd2(LATE - 1)
        with jax.named_scope('acc_b'):
            for col, n in NSTEPS:
                val = acc[256:384, col:col + n]
                for k in (LATE - 1, NK - 1):
                    val += jnp.dot(xs[k, 384:512, :], w[k * KC:(k + 1) * KC, col:col + n], preferred_element_type=F32)
                for s in range(2):
                    put_qkv(6 + s, col, n, val[s * BLK:(s + 1) * BLK])

    inv_sqrt = E ** -0.5

    def o_copy(b, half, dev_cp):
        lohi, part = b // 4, pl.ds(half * HALF, HALF)
        return remote(osend.at[b, part], ofull.at[lohi, part, pl.ds(pl.multiple_of(cp * HE, E), HE)],
                      o_send_sem, o_recv_sem.at[jnp.where(lohi == tp, 4, 2 * half + jnp.where(x == dev_cp // 2, 0, 1))], {'cp': dev_cp, 'tp': tp})

    def attend(b):
        length = 128 * (b // 2 + 1)
        ri = lax.broadcasted_iota(jnp.int32, (BLK, 128), 0) + BLK * (b % 2)
        ci = lax.broadcasted_iota(jnp.int32, (BLK, 128), 1)
        mask = ci <= ri
        heads = range(HEADS)
        q = [qkv[b * BLK:(b + 1) * BLK, h * E:(h + 1) * E] for h in heads]
        kk = [qkv[0:length, HE + h * E:HE + (h + 1) * E] for h in heads]
        v = [qkv[0:length, 2 * HE + h * E:2 * HE + (h + 1) * E] for h in heads]
        s = [lax.dot_general(q[h], kk[h], (((1,), (1,)), ((), ())), preferred_element_type=F32) * inv_sqrt for h in heads]
        last = [jnp.where(mask, s[h][:, length - 128:], NEG_BIG) for h in heads]
        s = [last[h] if length == 128 else jnp.concatenate([s[h][:, :length - 128], last[h]], axis=1) for h in heads]
        m = [jnp.max(s[h], axis=-1, keepdims=True) for h in heads]
        p = [jnp.exp(s[h] - m[h]) for h in heads]
        l = [jnp.sum(p[h], axis=-1, keepdims=True) for h in heads]
        o = [jnp.dot(p[h].astype(BF16), v[h], preferred_element_type=F32) for h in heads]
        for h in heads:
            osend[b, :, h * E:(h + 1) * E] = (o[h] / l[h]).astype(BF16)
        send_o(b, 0)
    def send_o(b, half):
        r = (b if b < 4 else 7 - b) if isinstance(b, int) else jnp.where(b < 4, b, 7 - b)

        @pl.when(cp == r)
        def _():
            part = pl.ds(half * HALF, HALF)
            ofull[b // 4, part, pl.ds(pl.multiple_of(cp * HE, E), HE)] = osend[b, part]

        @pl.when(cp != r)
        def _():
            o_copy(b, half, r).start()

    def wait_o(half, far):
        drain(osend.at[pl.ds(0, 1 + far), pl.ds(0, HALF)], o_recv_sem.at[2 * half + far])

    def attend_blocks(hi):
        def block_at(step):
            first = step < 2
            pair = jnp.where(hi, jnp.where(first, 2 + x, 3 - x), jnp.where(first, 1 - x, x))
            return 2 * pair + jnp.where(hi, step % 2, 1 - step % 2)

        @pl.loop(0, 4)
        def _(step):
            block = block_at(step)
            for b in range(8):
                @pl.when(block == b)
                def _():
                    with jax.named_scope(f'attend{b}'):
                        attend(b)

            @pl.when(step > 0)
            def _():
                send_o(block_at(step - 1), 1)

        send_o(block_at(3), 1)

    away, home = 1 - tp, tp

    def y_copy(n, half):
        part = pl.ds(half * HALF, HALF)
        return remote(ysend.at[n, part], yrecv.at[n, part], y_send_sem, y_recv_sem.at[n], yn)

    def project_away():
        near = pl.ds(pl.multiple_of(2 * x * HE, E), 2 * HE)
        far = pl.ds(pl.multiple_of(2 * (1 - x) * HE, E), 2 * HE)
        top, bottom = slice(0, HALF), slice(HALF, BLK)
        drain(wo, wo_sem)
        with jax.named_scope('wait_o_away'):
            wait_o(0, 0)
        with jax.named_scope('proj'):
            ysend[0, top] = jnp.dot(ofull[away, top, near], wo[0, near, :], preferred_element_type=F32)
        with jax.named_scope('wait_o_away'):
            wait_o(0, 1)
        with jax.named_scope('proj'):
            ysend[0, top] += jnp.dot(ofull[away, top, far], wo[0, far, :], preferred_element_type=F32)
        y_copy(0, 0).start()

        @pl.loop(1, NOUT)
        def _(n):
            with jax.named_scope('proj'):
                ysend[n, top] = jnp.dot(ofull[away, top], wo[n], preferred_element_type=F32)
            y_copy(n, 0).start()

        with jax.named_scope('wait_o_away'):
            wait_o(1, 0)
            wait_o(1, 1)

        @pl.loop(0, NOUT)
        def _(n):
            with jax.named_scope('proj'):
                ysend[n, bottom] = jnp.dot(ofull[away, bottom], wo[n], preferred_element_type=F32)
            y_copy(n, 1).start()

    @pl.loop(0, 4)
    def _(stage):
        @pl.when(stage == 2 * tp)
        def _():
            rest_of_rows()

        @pl.when((stage == 1 - tp) | (stage == 3))
        def _():
            attend_blocks((stage < 2) == (tp == 0))

        @pl.when(stage == 2 - tp)
        def _():
            project_away()

    with jax.named_scope('wait_o_home'):
        drain(osend.at[pl.ds(0, 3)], o_recv_sem.at[4])

    def kept(n):
        return acc.at[pl.ds(pl.multiple_of(n % 6 * BLK, BLK), BLK), pl.ds(pl.multiple_of(n // 6 * NC, NC), NC)]

    @pl.loop(0, NOUT)
    def _(n):
        kept(n)[...] = jnp.dot(ofull[home], wo[n], preferred_element_type=F32)

    @pl.loop(0, NOUT)
    def _(n):
        with jax.named_scope('wait_y'):
            drain(yrecv.at[n], y_recv_sem.at[n])
        y_ref[:, pl.ds(pl.multiple_of(n * NC, NC), NC)] = (kept(n)[...] + yrecv[n]).astype(BF16)

    drain(xs.at[:, pl.ds(0, 3 * BLK), :], own_send)
    drain(xs.at[:, pl.ds(0, 3 * BLK), :], fwd_send)
    for t in range(2):
        for xx in range(2):
            over_x = DIAG_X * BLK if t else (NK - LATE) * BLK + (1 - xx) * HALF
            over_y = LATE * BLK - xx * HALF if t else (NK - DIAG_X) * BLK

            @pl.when((tp == t) & (x == xx))
            def _():
                drain(xs.at[0, pl.ds(0, over_x), :], dg_send.at[0])
                drain(xs.at[0, pl.ds(0, over_y), :], dg_send.at[1])
    drain(osend.at[pl.ds(0, 6)], o_send_sem)
    drain(ysend, y_send_sem)


def solution(mesh):
    def device_fn(x_loc, w_q, w_k, w_v, w_o):
        dma = pltpu.SemaphoreType.DMA
        heads_major = [jnp.transpose(t, (1, 0, 2)) for t in (w_q, w_k, w_v)]
        return pl.pallas_call(
            kernel,
            name='attention_layer',
            out_shape=pltpu.VMEM((BLK, D), BF16),
            in_specs=[pl.BlockSpec(memory_space=pl.ANY)] * 5,
            out_specs=pl.BlockSpec(memory_space=pltpu.VMEM),
            scratch_shapes=[
                pltpu.VMEM((NK, 512, KC), BF16),
                pltpu.VMEM((D, NQKV), BF16),
                pltpu.VMEM((NOUT, 20 * E, NC), BF16),
                pltpu.VMEM((512, NQKV), BF16),
                pltpu.VMEM((384, NQKV), F32),
                pltpu.VMEM((8, BLK, HE), BF16),
                pltpu.VMEM((2, BLK, 20 * E), BF16),
                pltpu.VMEM((NOUT, BLK, NC), F32),
                pltpu.VMEM((NOUT, BLK, NC), F32),
                dma, dma, dma,
                dma, dma, dma((3, NK)),
                dma, dma((2 * NK + LATE,)), dma((2,)),
                dma, dma((5,)),
                dma, dma((NOUT,)),
            ],
            compiler_params=pltpu.CompilerParams(collective_id=0, has_side_effects=True, vmem_limit_bytes=64 * 1000 * 1000),
        )(x_loc, *heads_major, w_o.reshape(20 * E, D))

    seq_spec = P(('dp', 'cp', 'tp'), None)
    head_spec = P(None, 'tp', None)
    return jax.shard_map(device_fn, mesh=mesh, in_specs=(seq_spec, head_spec, head_spec, head_spec, P('tp', None, None)), out_specs=seq_spec, check_vma=False)
```

```python
import functools

import jax
import jax.numpy as jnp
from jax import lax
from jax.experimental import pallas as pl
from jax.experimental.pallas import tpu as pltpu
from jax.sharding import PartitionSpec as P


BF16, F32 = jnp.bfloat16, jnp.float32
NEG_BIG = -1e30
D = 5120
E = 128
HEADS = 5
HE = HEADS * E
NQKV = 3 * HE
BLK = 64
HALF = BLK // 2
NK = 10
KC = D // NK
LATE = NK // 2
DIAG_X = 7
NOUT = 10
NC = D // NOUT
MESH = pl.DeviceIdType.MESH


def remote(src, dst, send_sem, recv_sem, dev):
    return pltpu.make_async_remote_copy(src_ref=src, dst_ref=dst, send_sem=send_sem, recv_sem=recv_sem, device_id=dev, device_id_type=MESH)


def drain(ref, sem):
    pltpu.make_async_copy(ref, ref, sem).wait()


def kernel(x_hbm, wq_hbm, wk_hbm, wv_hbm, wo_hbm, y_ref, xs, w, wo, qkv, acc, osend, ofull, ysend, yrecv,
           xin_sem, w_sem, wo_sem, own_send, sib_recv, direct_recv, fwd_send, fwd_recv, dg_send, o_send_sem, o_recv_sem,
           y_send_sem, y_recv_sem):
    cp, tp = lax.axis_index('cp'), lax.axis_index('tp')
    x, c = cp // 2, cp % 2
    sib = {'cp': 2 * x + 1 - c, 'tp': tp}
    xn = {'cp': 2 * (1 - x) + c, 'tp': tp}
    xo = {'cp': 2 * (1 - x) + 1 - c, 'tp': tp}
    yn = {'cp': cp, 'tp': 1 - tp}

    def rows(group, core):
        return pl.ds(pl.multiple_of(group * 128 + core * BLK, BLK), BLK)

    def x_in(k):
        return pltpu.make_async_copy(x_hbm.at[:, pl.ds(k * KC, KC)], xs.at[k, rows(0, c), :], xin_sem)

    def w_in(j):
        src = (wq_hbm, wk_hbm, wv_hbm)[j // HEADS].at[cp * HEADS + j % HEADS]
        return pltpu.make_async_copy(src, w.at[:, pl.ds(j * E, E)], w_sem)

    def wo_in(n):
        return pltpu.make_async_copy(wo_hbm.at[:, pl.ds(n * NC, NC)], wo.at[n], wo_sem)

    for k in range(NK):
        x_in(k).start()
    barrier = pltpu.get_barrier_semaphore()
    for dev in (sib, xn, xo, yn):
        pl.semaphore_signal(barrier, inc=1, device_id=dev, device_id_type=MESH)
    drain(xs.at[:, rows(0, c), :], xin_sem)
    for j in range(3 * HEADS):
        w_in(j).start()
    with jax.named_scope('barrier'):
        pl.semaphore_wait(barrier, 4)

    def group_of(kind, t):
        return (1, 2 + t, 3 - t, 0)[kind]

    def own(k, kind):
        dev, t = ((yn, 1 - tp), (xn, tp), None, (sib, tp))[kind]
        return remote(xs.at[k, rows(0, c), :], xs.at[k, rows(group_of(kind, t), c), :], own_send, sib_recv if kind == 3 else direct_recv.at[kind, k], dev)

    def diag(k, over_y):
        dev, src, t = (yn, group_of(1, tp), 1 - tp) if over_y else (xn, group_of(0, tp), tp)
        return remote(xs.at[k, rows(src, c), :], xs.at[k, rows(group_of(2, t), c), :], dg_send.at[int(over_y)], direct_recv.at[2, k], dev)

    def half_diag(over_y):
        dev, src, t = (yn, group_of(1, tp), 1 - tp) if over_y else (xn, group_of(0, tp), tp)
        k, first = LATE - 1, 0 if over_y else HALF
        return remote(xs.at[k, pl.ds(pl.multiple_of(src * 128 + c * BLK + first, HALF), HALF), :],
                      xs.at[k, pl.ds(pl.multiple_of(group_of(2, t) * 128 + c * BLK + first, HALF), HALF), :],
                      dg_send.at[int(over_y)], direct_recv.at[2, k], dev)

    def fwd(k, kind):
        sl = rows(group_of(kind, tp), c)
        second = NK + k % LATE
        sem = (k, jnp.where(tp == 0, k, second), jnp.where(tp == 0, second, NK + LATE + k))[kind]
        return remote(xs.at[k, sl, :], xs.at[k, sl, :], fwd_send, fwd_recv.at[sem], sib)

    def direct_wait(k, kind):
        drain(xs.at[k, rows(group_of(kind, tp), c), :], direct_recv.at[kind, k])

    def sends_diag_x(k):
        return jnp.where(tp == 0, k >= LATE, k < DIAG_X)

    def sends_half_x(k):
        return (tp == 0) & (x == 0) & (k == LATE - 1)

    def sends_diag_y(k):
        return jnp.where(tp == 0, k >= DIAG_X, k < LATE - x)

    def sends_half_y(k):
        return (tp == 1) & (x == 1) & (k == LATE - 1)

    def handle(k, kind):
        direct_wait(k, kind)
        fwd(k, kind).start()
        if kind == 0:
            @pl.when(sends_diag_x(k))
            def _():
                diag(k, False).start()

            @pl.when(sends_half_x(k))
            def _():
                half_diag(False).start()
        if kind == 1:
            @pl.when(sends_diag_y(k))
            def _():
                diag(k, True).start()

            @pl.when(sends_half_y(k))
            def _():
                half_diag(True).start()

    for k in range(NK):
        if k < LATE:
            own(k, 1).start()
        else:
            @pl.when(tp == 0)
            def _():
                own(k, 1).start()
        own(k, 0).start()
        own(k, 3).start()

    acc[...] = jnp.zeros_like(acc)

    def nat(xx, core, t):
        b = 2 * xx + core
        return jnp.where(t == 0, b, 7 - b) * BLK

    nat_of = [nat(x, 0, tp), nat(x, 1, tp), nat(x, 0, 1 - tp), nat(x, 1, 1 - tp),
              nat(1 - x, 0, 0), nat(1 - x, 1, 0), nat(1 - x, 0, 1), nat(1 - x, 1, 1)]

    def put_qkv(slot, col, n, val):
        qkv[pl.ds(pl.multiple_of(nat_of[slot], BLK), BLK), pl.ds(col, n)] = val.astype(BF16)

    NSTEPS = ((0, 512), (512, 512), (1024, 512), (1536, 384))

    def own_chip():
        with jax.named_scope('wait_sib'):
            drain(xs.at[:, rows(0, c), :], sib_recv)
        with jax.named_scope('wait_w'):
            drain(w, w_sem)
        for n in range(NOUT):
            wo_in(n).start()
        for col, n in NSTEPS:
            val = jnp.dot(xs[0, 0:128, :], w[0:KC, col:col + n], preferred_element_type=F32)
            for k in range(1, NK):
                val += jnp.dot(xs[k, 0:128, :], w[k * KC:(k + 1) * KC, col:col + n], preferred_element_type=F32)
            put_qkv(0, col, n, val[:BLK])
            put_qkv(1, col, n, val[BLK:])

    def accumulate(chunks, row, m, arow):
        for col, n in NSTEPS:
            val = acc[arow:arow + m, col:col + n]
            for k in chunks:
                val += jnp.dot(xs[k, row:row + m, :], w[pl.ds(pl.multiple_of(k * KC, KC), KC), col:col + n], preferred_element_type=F32)
            acc[arow:arow + m, col:col + n] = val

    def diag_order(m):
        return jnp.where(m < 5, m, jnp.where(m % 2 == 1, 7 + (m - 5) // 2, 5 + (m - 6) // 2))

    def wait_fwd2(j):
        with jax.named_scope('w_fwd2'):
            drain(xs.at[0, pl.ds(384, 128), :], fwd_recv.at[NK + j])

    def pair(j):
        wait_fwd2(j)
        with jax.named_scope('acc_b'):
            accumulate((j, j + LATE), 384, 128, 256)

    @pl.loop(0, NK + 6)
    def _(i):
        @pl.when(i < NK)
        def _():
            with jax.named_scope('h_y'):
                handle(i, 0)

        @pl.when(i < jnp.where(tp == 0, NK, LATE))
        def _():
            with jax.named_scope('h_x'):
                handle(i, 1)

        @pl.when((tp == 1) & (i == DIAG_X - 1))
        def _():
            for k in range(LATE, NK):
                own(k, 1).start()

        @pl.when((tp == 0) & (i >= NK) & (i < NK + LATE))
        def _():
            with jax.named_scope('h_d2'):
                handle(i - NK, 2)
                handle(i - NK + LATE, 2)

        @pl.when((tp == 1) & (i >= 5) & (i < NK + 5))
        def _():
            with jax.named_scope('h_d'):
                handle(diag_order(i - 5), 2)

        @pl.when(i == 2)
        def _():
            own_chip()

        @pl.when((i >= 2) & (i < NK + 2))
        def _():
            k = i - 2

            @pl.when(tp == 0)
            def _():
                with jax.named_scope('w_fwd'):
                    drain(xs.at[k, pl.ds(128, 128), :], fwd_recv.at[k])
                with jax.named_scope('acc_a'):
                    accumulate((k,), 128, 256, 0)

            @pl.when(tp == 1)
            def _():
                with jax.named_scope('w_fwd'):
                    drain(xs.at[k, pl.ds(128, BLK), :], fwd_recv.at[k])
                with jax.named_scope('acc_y'):
                    accumulate((k,), 128, 128, 0)

        @pl.when((tp == 1) & (i >= 6))
        def _():
            k = diag_order(i - 6)
            with jax.named_scope('w_fwd'):
                drain(xs.at[k, pl.ds(256, BLK), :], fwd_recv.at[NK + LATE + k])
            with jax.named_scope('acc_d'):
                accumulate((k,), 256, 128, 128)

        @pl.when((tp == 0) & (i > NK) & (i < NK + LATE))
        def _():
            pair(i - NK - 1)

    for col, n in NSTEPS:
        for s in range(4):
            put_qkv(2 + s, col, n, acc[s * BLK:(s + 1) * BLK, col:col + n])

    def rest_of_rows():
        @pl.when(tp == 1)
        def _():
            @pl.loop(0, LATE)
            def _(j):
                with jax.named_scope('h_x2'):
                    handle(j + LATE, 1)

                @pl.when(j > 0)
                def _():
                    pair(j - 1)

        wait_fwd2(LATE - 1)
        with jax.named_scope('acc_b'):
            for col, n in NSTEPS:
                val = acc[256:384, col:col + n]
                for k in (LATE - 1, NK - 1):
                    val += jnp.dot(xs[k, 384:512, :], w[k * KC:(k + 1) * KC, col:col + n], preferred_element_type=F32)
                for s in range(2):
                    put_qkv(6 + s, col, n, val[s * BLK:(s + 1) * BLK])

    inv_sqrt = E ** -0.5

    def o_copy(b, half, dev_cp):
        lohi, part = b // 4, pl.ds(half * HALF, HALF)
        return remote(osend.at[b, part], ofull.at[lohi, part, pl.ds(pl.multiple_of(cp * HE, E), HE)],
                      o_send_sem, o_recv_sem.at[jnp.where(lohi == tp, 4, 2 * half + jnp.where(x == dev_cp // 2, 0, 1))], {'cp': dev_cp, 'tp': tp})

    def attend(b):
        length = 128 * (b // 2 + 1)
        ri = lax.broadcasted_iota(jnp.int32, (BLK, 128), 0) + BLK * (b % 2)
        ci = lax.broadcasted_iota(jnp.int32, (BLK, 128), 1)
        mask = ci <= ri
        heads = range(HEADS)
        q = [qkv[b * BLK:(b + 1) * BLK, h * E:(h + 1) * E] for h in heads]
        kk = [qkv[0:length, HE + h * E:HE + (h + 1) * E] for h in heads]
        v = [qkv[0:length, 2 * HE + h * E:2 * HE + (h + 1) * E] for h in heads]
        s = [lax.dot_general(q[h], kk[h], (((1,), (1,)), ((), ())), preferred_element_type=F32) * inv_sqrt for h in heads]
        last = [jnp.where(mask, s[h][:, length - 128:], NEG_BIG) for h in heads]
        s = [last[h] if length == 128 else jnp.concatenate([s[h][:, :length - 128], last[h]], axis=1) for h in heads]
        m = [jnp.max(s[h], axis=-1, keepdims=True) for h in heads]
        p = [jnp.exp(s[h] - m[h]) for h in heads]
        l = [jnp.sum(p[h], axis=-1, keepdims=True) for h in heads]
        o = [jnp.dot(p[h].astype(BF16), v[h], preferred_element_type=F32) for h in heads]
        for h in heads:
            osend[b, :, h * E:(h + 1) * E] = (o[h] / l[h]).astype(BF16)
    def send_o(b, half):
        r = jnp.where(b < 4, b, 7 - b)

        @pl.when(cp == r)
        def _():
            part = pl.ds(half * HALF, HALF)
            ofull[b // 4, part, pl.ds(pl.multiple_of(cp * HE, E), HE)] = osend[b, part]

        @pl.when(cp != r)
        def _():
            o_copy(b, half, r).start()

    def wait_o(half, far):
        drain(osend.at[pl.ds(0, 1 + far), pl.ds(0, HALF)], o_recv_sem.at[2 * half + far])

    def attend_blocks(hi):
        def block_at(step):
            first, odd = step < 2, step % 2
            pair = jnp.where(hi, jnp.where(first, 2 + x, 3 - x), jnp.where(first, 1 - x, x))
            return 2 * pair + jnp.where(hi, odd, 1 - odd)

        @pl.loop(0, 4)
        def _(step):
            block = block_at(step)
            for b in range(8):
                @pl.when(block == b)
                def _():
                    with jax.named_scope(f'attend{b}'):
                        attend(b)

            for at, sends in enumerate((((0, 0),), ((0, 1),), ((1, 0), (1, 1), (2, 0), (2, 1)), ((3, 0), (3, 1)))):
                @pl.when(step == at)
                def _():
                    for which, half in sends:
                        send_o(block_at(which), half)

    away, home = 1 - tp, tp

    def y_copy(n, half):
        part = pl.ds(half * HALF, HALF)
        return remote(ysend.at[n, part], yrecv.at[n, part], y_send_sem, y_recv_sem.at[n], yn)

    def project_away():
        near = pl.ds(pl.multiple_of(2 * x * HE, E), 2 * HE)
        far = pl.ds(pl.multiple_of(2 * (1 - x) * HE, E), 2 * HE)
        top, bottom = slice(0, HALF), slice(HALF, BLK)
        drain(wo, wo_sem)
        with jax.named_scope('wait_o_away'):
            wait_o(0, 0)
        with jax.named_scope('proj'):
            ysend[0, top] = jnp.dot(ofull[away, top, near], wo[0, near, :], preferred_element_type=F32)
        with jax.named_scope('wait_o_away'):
            wait_o(0, 1)
        with jax.named_scope('proj'):
            ysend[0, top] += jnp.dot(ofull[away, top, far], wo[0, far, :], preferred_element_type=F32)
        y_copy(0, 0).start()

        @pl.loop(1, NOUT)
        def _(n):
            with jax.named_scope('proj'):
                ysend[n, top] = jnp.dot(ofull[away, top], wo[n], preferred_element_type=F32)
            y_copy(n, 0).start()

        with jax.named_scope('wait_o_away'):
            wait_o(1, 0)
            wait_o(1, 1)

        @pl.loop(0, NOUT)
        def _(n):
            with jax.named_scope('proj'):
                ysend[n, bottom] = jnp.dot(ofull[away, bottom], wo[n], preferred_element_type=F32)
            y_copy(n, 1).start()

    @pl.loop(0, 4)
    def _(stage):
        @pl.when(stage == 2 * tp)
        def _():
            rest_of_rows()

        @pl.when((stage == 1 - tp) | (stage == 3))
        def _():
            attend_blocks((stage < 2) == (tp == 0))

        @pl.when(stage == 2 - tp)
        def _():
            project_away()

    with jax.named_scope('wait_o_home'):
        drain(osend.at[pl.ds(0, 3)], o_recv_sem.at[4])

    def kept(n):
        return acc.at[pl.ds(pl.multiple_of(n % 6 * BLK, BLK), BLK), pl.ds(pl.multiple_of(n // 6 * NC, NC), NC)]

    @pl.loop(0, NOUT)
    def _(n):
        kept(n)[...] = jnp.dot(ofull[home], wo[n], preferred_element_type=F32)

    @pl.loop(0, NOUT)
    def _(n):
        with jax.named_scope('wait_y'):
            drain(yrecv.at[n], y_recv_sem.at[n])
        y_ref[:, pl.ds(pl.multiple_of(n * NC, NC), NC)] = (kept(n)[...] + yrecv[n]).astype(BF16)

    drain(xs.at[:, pl.ds(0, 3 * BLK), :], own_send)
    drain(xs.at[:, pl.ds(0, 3 * BLK), :], fwd_send)
    for t in range(2):
        for xx in range(2):
            over_x = DIAG_X * BLK if t else (NK - LATE) * BLK + (1 - xx) * HALF
            over_y = LATE * BLK - xx * HALF if t else (NK - DIAG_X) * BLK

            @pl.when((tp == t) & (x == xx))
            def _():
                drain(xs.at[0, pl.ds(0, over_x), :], dg_send.at[0])
                drain(xs.at[0, pl.ds(0, over_y), :], dg_send.at[1])
    drain(osend.at[pl.ds(0, 6)], o_send_sem)
    drain(ysend, y_send_sem)


def solution(mesh):
    def device_fn(x_loc, w_q, w_k, w_v, w_o):
        dma = pltpu.SemaphoreType.DMA
        heads_major = [jnp.transpose(t, (1, 0, 2)) for t in (w_q, w_k, w_v)]
        return pl.pallas_call(
            kernel,
            name='attention_layer',
            out_shape=pltpu.VMEM((BLK, D), BF16),
            in_specs=[pl.BlockSpec(memory_space=pl.ANY)] * 5,
            out_specs=pl.BlockSpec(memory_space=pltpu.VMEM),
            scratch_shapes=[
                pltpu.VMEM((NK, 512, KC), BF16),
                pltpu.VMEM((D, NQKV), BF16),
                pltpu.VMEM((NOUT, 20 * E, NC), BF16),
                pltpu.VMEM((512, NQKV), BF16),
                pltpu.VMEM((384, NQKV), F32),
                pltpu.VMEM((8, BLK, HE), BF16),
                pltpu.VMEM((2, BLK, 20 * E), BF16),
                pltpu.VMEM((NOUT, BLK, NC), F32),
                pltpu.VMEM((NOUT, BLK, NC), F32),
                dma, dma, dma,
                dma, dma, dma((3, NK)),
                dma, dma((2 * NK + LATE,)), dma((2,)),
                dma, dma((5,)),
                dma, dma((NOUT,)),
            ],
            compiler_params=pltpu.CompilerParams(collective_id=0, has_side_effects=True, vmem_limit_bytes=64 * 1000 * 1000),
        )(x_loc, *heads_major, w_o.reshape(20 * E, D))

    seq_spec = P(('dp', 'cp', 'tp'), None)
    head_spec = P(None, 'tp', None)
    return jax.shard_map(device_fn, mesh=mesh, in_specs=(seq_spec, head_spec, head_spec, head_spec, P('tp', None, None)), out_specs=seq_spec, check_vma=False)
```

```python
import functools

import jax
import jax.numpy as jnp
from jax import lax
from jax.experimental import pallas as pl
from jax.experimental.pallas import tpu as pltpu
from jax.sharding import PartitionSpec as P


BF16, F32 = jnp.bfloat16, jnp.float32
NEG_BIG = -1e30
D = 5120
E = 128
HEADS = 5
HE = HEADS * E
NQKV = 3 * HE
BLK = 64
HALF = BLK // 2
NK = 10
KC = D // NK
LATE = NK // 2
DIAG_X = 7
NOUT = 10
NC = D // NOUT
MESH = pl.DeviceIdType.MESH


def remote(src, dst, send_sem, recv_sem, dev):
    return pltpu.make_async_remote_copy(src_ref=src, dst_ref=dst, send_sem=send_sem, recv_sem=recv_sem, device_id=dev, device_id_type=MESH)


def drain(ref, sem):
    pltpu.make_async_copy(ref, ref, sem).wait()


def kernel(x_hbm, wq_hbm, wk_hbm, wv_hbm, wo_hbm, y_ref, xs, w, wo, qkv, acc, osend, ofull, ysend, yrecv,
           xin_sem, w_sem, wo_sem, own_send, sib_recv, direct_recv, fwd_send, fwd_recv, dg_send, o_send_sem, o_recv_sem,
           y_send_sem, y_recv_sem):
    cp, tp = lax.axis_index('cp'), lax.axis_index('tp')
    x, c = cp // 2, cp % 2
    sib = {'cp': 2 * x + 1 - c, 'tp': tp}
    xn = {'cp': 2 * (1 - x) + c, 'tp': tp}
    xo = {'cp': 2 * (1 - x) + 1 - c, 'tp': tp}
    yn = {'cp': cp, 'tp': 1 - tp}

    def rows(group, core):
        return pl.ds(pl.multiple_of(group * 128 + core * BLK, BLK), BLK)

    def x_in(k):
        return pltpu.make_async_copy(x_hbm.at[:, pl.ds(k * KC, KC)], xs.at[k, rows(0, c), :], xin_sem)

    def w_in(j):
        src = (wq_hbm, wk_hbm, wv_hbm)[j // HEADS].at[cp * HEADS + j % HEADS]
        return pltpu.make_async_copy(src, w.at[:, pl.ds(j * E, E)], w_sem)

    def wo_in(n):
        return pltpu.make_async_copy(wo_hbm.at[:, pl.ds(n * NC, NC)], wo.at[n], wo_sem)

    for k in range(NK):
        x_in(k).start()
    barrier = pltpu.get_barrier_semaphore()
    for dev in (sib, xn, xo, yn):
        pl.semaphore_signal(barrier, inc=1, device_id=dev, device_id_type=MESH)
    drain(xs.at[:, rows(0, c), :], xin_sem)
    for j in range(3 * HEADS):
        w_in(j).start()
    with jax.named_scope('barrier'):
        pl.semaphore_wait(barrier, 4)

    def group_of(kind, t):
        return (1, 2 + t, 3 - t, 0)[kind]

    def own(k, kind):
        dev, t = ((yn, 1 - tp), (xn, tp), None, (sib, tp))[kind]
        return remote(xs.at[k, rows(0, c), :], xs.at[k, rows(group_of(kind, t), c), :], own_send, sib_recv if kind == 3 else direct_recv.at[kind, k], dev)

    def diag(k, over_y):
        dev, src, t = (yn, group_of(1, tp), 1 - tp) if over_y else (xn, group_of(0, tp), tp)
        return remote(xs.at[k, rows(src, c), :], xs.at[k, rows(group_of(2, t), c), :], dg_send.at[int(over_y)], direct_recv.at[2, k], dev)

    def half_diag(over_y):
        dev, src, t = (yn, group_of(1, tp), 1 - tp) if over_y else (xn, group_of(0, tp), tp)
        k, first = LATE - 1, 0 if over_y else HALF
        return remote(xs.at[k, pl.ds(pl.multiple_of(src * 128 + c * BLK + first, HALF), HALF), :],
                      xs.at[k, pl.ds(pl.multiple_of(group_of(2, t) * 128 + c * BLK + first, HALF), HALF), :],
                      dg_send.at[int(over_y)], direct_recv.at[2, k], dev)

    def fwd(k, kind):
        sl = rows(group_of(kind, tp), c)
        second = NK + k % LATE
        sem = (k, jnp.where(tp == 0, k, second), jnp.where(tp == 0, second, NK + LATE + k))[kind]
        return remote(xs.at[k, sl, :], xs.at[k, sl, :], fwd_send, fwd_recv.at[sem], sib)

    def direct_wait(k, kind):
        drain(xs.at[k, rows(group_of(kind, tp), c), :], direct_recv.at[kind, k])

    def sends_diag_x(k):
        return jnp.where(tp == 0, k >= LATE, k < DIAG_X)

    def sends_half_x(k):
        return (tp == 0) & (x == 0) & (k == LATE - 1)

    def sends_diag_y(k):
        return jnp.where(tp == 0, k >= DIAG_X, k < LATE - x)

    def sends_half_y(k):
        return (tp == 1) & (x == 1) & (k == LATE - 1)

    def handle(k, kind):
        direct_wait(k, kind)
        fwd(k, kind).start()
        if kind == 0:
            @pl.when(sends_diag_x(k))
            def _():
                diag(k, False).start()

            @pl.when(sends_half_x(k))
            def _():
                half_diag(False).start()
        if kind == 1:
            @pl.when(sends_diag_y(k))
            def _():
                diag(k, True).start()

            @pl.when(sends_half_y(k))
            def _():
                half_diag(True).start()

    for k in range(NK):
        if k < LATE:
            own(k, 1).start()
        else:
            @pl.when(tp == 0)
            def _():
                own(k, 1).start()
        own(k, 0).start()
        own(k, 3).start()

    acc[...] = jnp.zeros_like(acc)

    def nat(xx, core, t):
        b = 2 * xx + core
        return jnp.where(t == 0, b, 7 - b) * BLK

    nat_of = [nat(x, 0, tp), nat(x, 1, tp), nat(x, 0, 1 - tp), nat(x, 1, 1 - tp),
              nat(1 - x, 0, 0), nat(1 - x, 1, 0), nat(1 - x, 0, 1), nat(1 - x, 1, 1)]

    def put_qkv(slot, col, n, val):
        qkv[pl.ds(pl.multiple_of(nat_of[slot], BLK), BLK), pl.ds(col, n)] = val.astype(BF16)

    NSTEPS = ((0, 512), (512, 512), (1024, 512), (1536, 384))

    def own_chip():
        with jax.named_scope('wait_sib'):
            drain(xs.at[:, rows(0, c), :], sib_recv)
        with jax.named_scope('wait_w'):
            drain(w, w_sem)
        for n in range(NOUT):
            wo_in(n).start()
        for col, n in NSTEPS:
            val = jnp.dot(xs[0, 0:128, :], w[0:KC, col:col + n], preferred_element_type=F32)
            for k in range(1, NK):
                val += jnp.dot(xs[k, 0:128, :], w[k * KC:(k + 1) * KC, col:col + n], preferred_element_type=F32)
            put_qkv(0, col, n, val[:BLK])
            put_qkv(1, col, n, val[BLK:])

    def accumulate(chunks, row, m, arow):
        for col, n in NSTEPS:
            val = acc[arow:arow + m, col:col + n]
            for k in chunks:
                val += jnp.dot(xs[k, row:row + m, :], w[pl.ds(pl.multiple_of(k * KC, KC), KC), col:col + n], preferred_element_type=F32)
            acc[arow:arow + m, col:col + n] = val

    def diag_order(m):
        return jnp.where(m < 5, m, jnp.where(m % 2 == 1, 7 + (m - 5) // 2, 5 + (m - 6) // 2))

    def wait_fwd2(j):
        with jax.named_scope('w_fwd2'):
            drain(xs.at[0, pl.ds(384, 128), :], fwd_recv.at[NK + j])

    def pair(j):
        wait_fwd2(j)
        with jax.named_scope('acc_b'):
            accumulate((j, j + LATE), 384, 128, 256)

    @pl.loop(0, NK + 6)
    def _(i):
        @pl.when(i < NK)
        def _():
            with jax.named_scope('h_y'):
                handle(i, 0)

        @pl.when(i < jnp.where(tp == 0, NK, LATE))
        def _():
            with jax.named_scope('h_x'):
                handle(i, 1)

        @pl.when((tp == 1) & (i == DIAG_X - 1))
        def _():
            for k in range(LATE, NK):
                own(k, 1).start()

        @pl.when((tp == 0) & (i >= NK) & (i < NK + LATE))
        def _():
            with jax.named_scope('h_d2'):
                handle(i - NK, 2)
                handle(i - NK + LATE, 2)

        @pl.when((tp == 1) & (i >= 5) & (i < NK + 5))
        def _():
            with jax.named_scope('h_d'):
                handle(diag_order(i - 5), 2)

        @pl.when(i == 2)
        def _():
            own_chip()

        @pl.when((i >= 2) & (i < NK + 2))
        def _():
            k = i - 2

            @pl.when(tp == 0)
            def _():
                with jax.named_scope('w_fwd'):
                    drain(xs.at[k, pl.ds(128, 128), :], fwd_recv.at[k])
                with jax.named_scope('acc_a'):
                    accumulate((k,), 128, 256, 0)

            @pl.when(tp == 1)
            def _():
                with jax.named_scope('w_fwd'):
                    drain(xs.at[k, pl.ds(128, BLK), :], fwd_recv.at[k])
                with jax.named_scope('acc_y'):
                    accumulate((k,), 128, 128, 0)

        @pl.when((tp == 1) & (i >= 6))
        def _():
            k = diag_order(i - 6)
            with jax.named_scope('w_fwd'):
                drain(xs.at[k, pl.ds(256, BLK), :], fwd_recv.at[NK + LATE + k])
            with jax.named_scope('acc_d'):
                accumulate((k,), 256, 128, 128)

        @pl.when((tp == 0) & (i > NK) & (i < NK + LATE))
        def _():
            pair(i - NK - 1)

    for col, n in NSTEPS:
        for s in range(4):
            put_qkv(2 + s, col, n, acc[s * BLK:(s + 1) * BLK, col:col + n])

    def rest_of_rows():
        @pl.when(tp == 1)
        def _():
            @pl.loop(0, LATE)
            def _(j):
                with jax.named_scope('h_x2'):
                    handle(j + LATE, 1)

                @pl.when(j > 0)
                def _():
                    pair(j - 1)

        wait_fwd2(LATE - 1)
        with jax.named_scope('acc_b'):
            for col, n in NSTEPS:
                val = acc[256:384, col:col + n]
                for k in (LATE - 1, NK - 1):
                    val += jnp.dot(xs[k, 384:512, :], w[k * KC:(k + 1) * KC, col:col + n], preferred_element_type=F32)
                for s in range(2):
                    put_qkv(6 + s, col, n, val[s * BLK:(s + 1) * BLK])

    inv_sqrt = E ** -0.5

    def o_copy(b, half, dev_cp):
        lohi, part = b // 4, pl.ds(half * HALF, HALF)
        return remote(osend.at[b, part], ofull.at[lohi, part, pl.ds(pl.multiple_of(cp * HE, E), HE)],
                      o_send_sem, o_recv_sem.at[jnp.where(lohi == tp, 4, 2 * half + jnp.where(x == dev_cp // 2, 0, 1))], {'cp': dev_cp, 'tp': tp})

    def attend(b):
        length = 128 * (b // 2 + 1)
        ri = lax.broadcasted_iota(jnp.int32, (BLK, 128), 0) + BLK * (b % 2)
        ci = lax.broadcasted_iota(jnp.int32, (BLK, 128), 1)
        mask = ci <= ri
        heads = range(HEADS)
        q = [qkv[b * BLK:(b + 1) * BLK, h * E:(h + 1) * E] for h in heads]
        kk = [qkv[0:length, HE + h * E:HE + (h + 1) * E] for h in heads]
        v = [qkv[0:length, 2 * HE + h * E:2 * HE + (h + 1) * E] for h in heads]
        s = [lax.dot_general(q[h], kk[h], (((1,), (1,)), ((), ())), preferred_element_type=F32) * inv_sqrt for h in heads]
        last = [jnp.where(mask, s[h][:, length - 128:], NEG_BIG) for h in heads]
        s = [last[h] if length == 128 else jnp.concatenate([s[h][:, :length - 128], last[h]], axis=1) for h in heads]
        m = [jnp.max(s[h], axis=-1, keepdims=True) for h in heads]
        p = [jnp.exp(s[h] - m[h]) for h in heads]
        l = [jnp.sum(p[h], axis=-1, keepdims=True) for h in heads]
        o = [jnp.dot(p[h].astype(BF16), v[h], preferred_element_type=F32) for h in heads]
        for h in heads:
            osend[b, :, h * E:(h + 1) * E] = (o[h] / l[h]).astype(BF16)
    def send_o(b, half):
        r = jnp.where(b < 4, b, 7 - b)

        @pl.when(cp == r)
        def _():
            part = pl.ds(half * HALF, HALF)
            ofull[b // 4, part, pl.ds(pl.multiple_of(cp * HE, E), HE)] = osend[b, part]

        @pl.when(cp != r)
        def _():
            o_copy(b, half, r).start()

    def wait_o(half, far):
        drain(osend.at[pl.ds(0, 1 + far), pl.ds(0, HALF)], o_recv_sem.at[2 * half + far])

    def attend_blocks(hi):
        def block_at(step):
            first, odd = step < 2, step % 2
            pair = jnp.where(hi, jnp.where(first, 2 + x, 3 - x), jnp.where(first, 1 - x, x))
            return 2 * pair + jnp.where(hi, 1 - odd, odd)

        @pl.loop(0, 4)
        def _(step):
            block = block_at(step)
            for b in range(8):
                @pl.when(block == b)
                def _():
                    with jax.named_scope(f'attend{b}'):
                        attend(b)

            for at, sends in enumerate((((0, 0),), ((0, 1),), ((1, 0), (1, 1), (2, 0), (2, 1)), ((3, 0), (3, 1)))):
                @pl.when(step == at)
                def _():
                    for which, half in sends:
                        send_o(block_at(which), half)

    away, home = 1 - tp, tp

    def y_copy(n, half):
        part = pl.ds(half * HALF, HALF)
        return remote(ysend.at[n, part], yrecv.at[n, part], y_send_sem, y_recv_sem.at[n], yn)

    def project_away():
        near = pl.ds(pl.multiple_of(2 * x * HE, E), 2 * HE)
        far = pl.ds(pl.multiple_of(2 * (1 - x) * HE, E), 2 * HE)
        top, bottom = slice(0, HALF), slice(HALF, BLK)
        drain(wo, wo_sem)
        with jax.named_scope('wait_o_away'):
            wait_o(0, 0)
        with jax.named_scope('proj'):
            ysend[0, top] = jnp.dot(ofull[away, top, near], wo[0, near, :], preferred_element_type=F32)
        with jax.named_scope('wait_o_away'):
            wait_o(0, 1)
        with jax.named_scope('proj'):
            ysend[0, top] += jnp.dot(ofull[away, top, far], wo[0, far, :], preferred_element_type=F32)
        y_copy(0, 0).start()

        @pl.loop(1, NOUT)
        def _(n):
            with jax.named_scope('proj'):
                ysend[n, top] = jnp.dot(ofull[away, top], wo[n], preferred_element_type=F32)
            y_copy(n, 0).start()

        with jax.named_scope('wait_o_away'):
            wait_o(1, 0)
            wait_o(1, 1)

        @pl.loop(0, NOUT)
        def _(n):
            with jax.named_scope('proj'):
                ysend[n, bottom] = jnp.dot(ofull[away, bottom], wo[n], preferred_element_type=F32)
            y_copy(n, 1).start()

    @pl.loop(0, 4)
    def _(stage):
        @pl.when(stage == 2 * tp)
        def _():
            rest_of_rows()

        @pl.when((stage == 1 - tp) | (stage == 3))
        def _():
            attend_blocks((stage < 2) == (tp == 0))

        @pl.when(stage == 2 - tp)
        def _():
            project_away()

    with jax.named_scope('wait_o_home'):
        drain(osend.at[pl.ds(0, 3)], o_recv_sem.at[4])

    def kept(n):
        return acc.at[pl.ds(pl.multiple_of(n % 6 * BLK, BLK), BLK), pl.ds(pl.multiple_of(n // 6 * NC, NC), NC)]

    @pl.loop(0, NOUT)
    def _(n):
        kept(n)[...] = jnp.dot(ofull[home], wo[n], preferred_element_type=F32)

    @pl.loop(0, NOUT)
    def _(n):
        with jax.named_scope('wait_y'):
            drain(yrecv.at[n], y_recv_sem.at[n])
        y_ref[:, pl.ds(pl.multiple_of(n * NC, NC), NC)] = (kept(n)[...] + yrecv[n]).astype(BF16)

    drain(xs.at[:, pl.ds(0, 3 * BLK), :], own_send)
    drain(xs.at[:, pl.ds(0, 3 * BLK), :], fwd_send)
    for t in range(2):
        for xx in range(2):
            over_x = DIAG_X * BLK if t else (NK - LATE) * BLK + (1 - xx) * HALF
            over_y = LATE * BLK - xx * HALF if t else (NK - DIAG_X) * BLK

            @pl.when((tp == t) & (x == xx))
            def _():
                drain(xs.at[0, pl.ds(0, over_x), :], dg_send.at[0])
                drain(xs.at[0, pl.ds(0, over_y), :], dg_send.at[1])
    drain(osend.at[pl.ds(0, 6)], o_send_sem)
    drain(ysend, y_send_sem)


def solution(mesh):
    def device_fn(x_loc, w_q, w_k, w_v, w_o):
        dma = pltpu.SemaphoreType.DMA
        heads_major = [jnp.transpose(t, (1, 0, 2)) for t in (w_q, w_k, w_v)]
        return pl.pallas_call(
            kernel,
            name='attention_layer',
            out_shape=pltpu.VMEM((BLK, D), BF16),
            in_specs=[pl.BlockSpec(memory_space=pl.ANY)] * 5,
            out_specs=pl.BlockSpec(memory_space=pltpu.VMEM),
            scratch_shapes=[
                pltpu.VMEM((NK, 512, KC), BF16),
                pltpu.VMEM((D, NQKV), BF16),
                pltpu.VMEM((NOUT, 20 * E, NC), BF16),
                pltpu.VMEM((512, NQKV), BF16),
                pltpu.VMEM((384, NQKV), F32),
                pltpu.VMEM((8, BLK, HE), BF16),
                pltpu.VMEM((2, BLK, 20 * E), BF16),
                pltpu.VMEM((NOUT, BLK, NC), F32),
                pltpu.VMEM((NOUT, BLK, NC), F32),
                dma, dma, dma,
                dma, dma, dma((3, NK)),
                dma, dma((2 * NK + LATE,)), dma((2,)),
                dma, dma((5,)),
                dma, dma((NOUT,)),
            ],
            compiler_params=pltpu.CompilerParams(collective_id=0, has_side_effects=True, vmem_limit_bytes=64 * 1000 * 1000),
        )(x_loc, *heads_major, w_o.reshape(20 * E, D))

    seq_spec = P(('dp', 'cp', 'tp'), None)
    head_spec = P(None, 'tp', None)
    return jax.shard_map(device_fn, mesh=mesh, in_specs=(seq_spec, head_spec, head_spec, head_spec, P('tp', None, None)), out_specs=seq_spec, check_vma=False)
```

```python
import functools

import jax
import jax.numpy as jnp
from jax import lax
from jax.experimental import pallas as pl
from jax.experimental.pallas import tpu as pltpu
from jax.sharding import PartitionSpec as P


BF16, F32 = jnp.bfloat16, jnp.float32
NEG_BIG = -1e30
D = 5120
E = 128
HEADS = 5
HE = HEADS * E
NQKV = 3 * HE
BLK = 64
HALF = BLK // 2
NK = 10
KC = D // NK
LATE = NK // 2
DIAG_X = 7
NOUT = 10
NC = D // NOUT
MESH = pl.DeviceIdType.MESH


def remote(src, dst, send_sem, recv_sem, dev):
    return pltpu.make_async_remote_copy(src_ref=src, dst_ref=dst, send_sem=send_sem, recv_sem=recv_sem, device_id=dev, device_id_type=MESH)


def drain(ref, sem):
    pltpu.make_async_copy(ref, ref, sem).wait()


def kernel(x_hbm, wq_hbm, wk_hbm, wv_hbm, wo_hbm, y_ref, xs, w, wo, qkv, acc, osend, ofull, ysend, yrecv,
           xin_sem, w_sem, wo_sem, own_send, sib_recv, direct_recv, fwd_send, fwd_recv, dg_send, o_send_sem, o_recv_sem,
           y_send_sem, y_recv_sem):
    cp, tp = lax.axis_index('cp'), lax.axis_index('tp')
    x, c = cp // 2, cp % 2
    sib = {'cp': 2 * x + 1 - c, 'tp': tp}
    xn = {'cp': 2 * (1 - x) + c, 'tp': tp}
    xo = {'cp': 2 * (1 - x) + 1 - c, 'tp': tp}
    yn = {'cp': cp, 'tp': 1 - tp}

    def rows(group, core):
        return pl.ds(pl.multiple_of(group * 128 + core * BLK, BLK), BLK)

    def x_in(k):
        return pltpu.make_async_copy(x_hbm.at[:, pl.ds(k * KC, KC)], xs.at[k, rows(0, c), :], xin_sem)

    def w_in(j):
        src = (wq_hbm, wk_hbm, wv_hbm)[j // HEADS].at[cp * HEADS + j % HEADS]
        return pltpu.make_async_copy(src, w.at[:, pl.ds(j * E, E)], w_sem)

    def wo_in(n):
        return pltpu.make_async_copy(wo_hbm.at[:, pl.ds(n * NC, NC)], wo.at[n], wo_sem)

    for k in range(NK):
        x_in(k).start()
    barrier = pltpu.get_barrier_semaphore()
    for dev in (sib, xn, xo, yn):
        pl.semaphore_signal(barrier, inc=1, device_id=dev, device_id_type=MESH)
    drain(xs.at[:, rows(0, c), :], xin_sem)
    for j in range(3 * HEADS):
        w_in(j).start()
    with jax.named_scope('barrier'):
        pl.semaphore_wait(barrier, 4)

    def group_of(kind, t):
        return (1, 2 + t, 3 - t, 0)[kind]

    def own(k, kind):
        dev, t = ((yn, 1 - tp), (xn, tp), None, (sib, tp))[kind]
        return remote(xs.at[k, rows(0, c), :], xs.at[k, rows(group_of(kind, t), c), :], own_send, sib_recv if kind == 3 else direct_recv.at[kind, k], dev)

    def diag(k, over_y):
        dev, src, t = (yn, group_of(1, tp), 1 - tp) if over_y else (xn, group_of(0, tp), tp)
        return remote(xs.at[k, rows(src, c), :], xs.at[k, rows(group_of(2, t), c), :], dg_send.at[int(over_y)], direct_recv.at[2, k], dev)

    def half_diag(over_y):
        dev, src, t = (yn, group_of(1, tp), 1 - tp) if over_y else (xn, group_of(0, tp), tp)
        k, first = LATE - 1, 0 if over_y else HALF
        return remote(xs.at[k, pl.ds(pl.multiple_of(src * 128 + c * BLK + first, HALF), HALF), :],
                      xs.at[k, pl.ds(pl.multiple_of(group_of(2, t) * 128 + c * BLK + first, HALF), HALF), :],
                      dg_send.at[int(over_y)], direct_recv.at[2, k], dev)

    def fwd(k, kind):
        sl = rows(group_of(kind, tp), c)
        second = NK + k % LATE
        sem = (k, jnp.where(tp == 0, k, second), jnp.where(tp == 0, second, NK + LATE + k))[kind]
        return remote(xs.at[k, sl, :], xs.at[k, sl, :], fwd_send, fwd_recv.at[sem], sib)

    def direct_wait(k, kind):
        drain(xs.at[k, rows(group_of(kind, tp), c), :], direct_recv.at[kind, k])

    def sends_diag_x(k):
        return jnp.where(tp == 0, k >= LATE, k < DIAG_X)

    def sends_half_x(k):
        return (tp == 0) & (x == 0) & (k == LATE - 1)

    def sends_diag_y(k):
        return jnp.where(tp == 0, k >= DIAG_X, k < LATE - x)

    def sends_half_y(k):
        return (tp == 1) & (x == 1) & (k == LATE - 1)

    def handle(k, kind):
        direct_wait(k, kind)
        fwd(k, kind).start()
        if kind == 0:
            @pl.when(sends_diag_x(k))
            def _():
                diag(k, False).start()

            @pl.when(sends_half_x(k))
            def _():
                half_diag(False).start()
        if kind == 1:
            @pl.when(sends_diag_y(k))
            def _():
                diag(k, True).start()

            @pl.when(sends_half_y(k))
            def _():
                half_diag(True).start()

    for k in range(NK):
        if k < LATE:
            own(k, 1).start()
        else:
            @pl.when(tp == 0)
            def _():
                own(k, 1).start()
        own(k, 0).start()
        own(k, 3).start()

    acc[...] = jnp.zeros_like(acc)

    def nat(xx, core, t):
        b = 2 * xx + core
        return jnp.where(t == 0, b, 7 - b) * BLK

    nat_of = [nat(x, 0, tp), nat(x, 1, tp), nat(x, 0, 1 - tp), nat(x, 1, 1 - tp),
              nat(1 - x, 0, 0), nat(1 - x, 1, 0), nat(1 - x, 0, 1), nat(1 - x, 1, 1)]

    def put_qkv(slot, col, n, val):
        qkv[pl.ds(pl.multiple_of(nat_of[slot], BLK), BLK), pl.ds(col, n)] = val.astype(BF16)

    NSTEPS = ((0, 512), (512, 512), (1024, 512), (1536, 384))

    def own_chip():
        with jax.named_scope('wait_sib'):
            drain(xs.at[:, rows(0, c), :], sib_recv)
        with jax.named_scope('wait_w'):
            drain(w, w_sem)
        for n in range(NOUT):
            wo_in(n).start()
        for col, n in NSTEPS:
            val = jnp.dot(xs[0, 0:128, :], w[0:KC, col:col + n], preferred_element_type=F32)
            for k in range(1, NK):
                val += jnp.dot(xs[k, 0:128, :], w[k * KC:(k + 1) * KC, col:col + n], preferred_element_type=F32)
            put_qkv(0, col, n, val[:BLK])
            put_qkv(1, col, n, val[BLK:])

    def accumulate(chunks, row, m, arow):
        for col, n in NSTEPS:
            val = acc[arow:arow + m, col:col + n]
            for k in chunks:
                val += jnp.dot(xs[k, row:row + m, :], w[pl.ds(pl.multiple_of(k * KC, KC), KC), col:col + n], preferred_element_type=F32)
            acc[arow:arow + m, col:col + n] = val

    def diag_order(m):
        return jnp.where(m < 5, m, jnp.where(m % 2 == 1, 7 + (m - 5) // 2, 5 + (m - 6) // 2))

    def wait_fwd2(j):
        with jax.named_scope('w_fwd2'):
            drain(xs.at[0, pl.ds(384, 128), :], fwd_recv.at[NK + j])

    def pair(j):
        wait_fwd2(j)
        with jax.named_scope('acc_b'):
            accumulate((j, j + LATE), 384, 128, 256)

    @pl.loop(0, NK + 6)
    def _(i):
        @pl.when(i < NK)
        def _():
            with jax.named_scope('h_y'):
                handle(i, 0)

        @pl.when(i < jnp.where(tp == 0, NK, LATE))
        def _():
            with jax.named_scope('h_x'):
                handle(i, 1)

        @pl.when((tp == 1) & (i == DIAG_X - 1))
        def _():
            for k in range(LATE, NK):
                own(k, 1).start()

        @pl.when((tp == 0) & (i >= NK) & (i < NK + LATE))
        def _():
            with jax.named_scope('h_d2'):
                handle(i - NK, 2)
                handle(i - NK + LATE, 2)

        @pl.when((tp == 1) & (i >= 5) & (i < NK + 5))
        def _():
            with jax.named_scope('h_d'):
                handle(diag_order(i - 5), 2)

        @pl.when(i == 2)
        def _():
            own_chip()

        @pl.when((i >= 2) & (i < NK + 2))
        def _():
            k = i - 2

            @pl.when(tp == 0)
            def _():
                with jax.named_scope('w_fwd'):
                    drain(xs.at[k, pl.ds(128, 128), :], fwd_recv.at[k])
                with jax.named_scope('acc_a'):
                    accumulate((k,), 128, 256, 0)

            @pl.when(tp == 1)
            def _():
                with jax.named_scope('w_fwd'):
                    drain(xs.at[k, pl.ds(128, BLK), :], fwd_recv.at[k])
                with jax.named_scope('acc_y'):
                    accumulate((k,), 128, 128, 0)

        @pl.when((tp == 1) & (i >= 6))
        def _():
            k = diag_order(i - 6)
            with jax.named_scope('w_fwd'):
                drain(xs.at[k, pl.ds(256, BLK), :], fwd_recv.at[NK + LATE + k])
            with jax.named_scope('acc_d'):
                accumulate((k,), 256, 128, 128)

        @pl.when((tp == 0) & (i > NK) & (i < NK + LATE))
        def _():
            pair(i - NK - 1)

    for col, n in NSTEPS:
        for s in range(4):
            put_qkv(2 + s, col, n, acc[s * BLK:(s + 1) * BLK, col:col + n])

    def rest_of_rows():
        @pl.when(tp == 1)
        def _():
            @pl.loop(0, LATE)
            def _(j):
                with jax.named_scope('h_x2'):
                    handle(j + LATE, 1)

                @pl.when(j > 0)
                def _():
                    pair(j - 1)

        wait_fwd2(LATE - 1)
        with jax.named_scope('acc_b'):
            for col, n in NSTEPS:
                val = acc[256:384, col:col + n]
                for k in (LATE - 1, NK - 1):
                    val += jnp.dot(xs[k, 384:512, :], w[k * KC:(k + 1) * KC, col:col + n], preferred_element_type=F32)
                for s in range(2):
                    put_qkv(6 + s, col, n, val[s * BLK:(s + 1) * BLK])

    inv_sqrt = E ** -0.5

    def o_copy(b, half, dev_cp):
        lohi, part = b // 4, pl.ds(half * HALF, HALF)
        return remote(osend.at[b, part], ofull.at[lohi, part, pl.ds(pl.multiple_of(cp * HE, E), HE)],
                      o_send_sem, o_recv_sem.at[jnp.where(lohi == tp, 4, 2 * half + jnp.where(x == dev_cp // 2, 0, 1))], {'cp': dev_cp, 'tp': tp})

    def attend(b):
        length = 128 * (b // 2 + 1)
        ri = lax.broadcasted_iota(jnp.int32, (BLK, 128), 0) + BLK * (b % 2)
        ci = lax.broadcasted_iota(jnp.int32, (BLK, 128), 1)
        mask = ci <= ri
        heads = range(HEADS)
        q = [qkv[b * BLK:(b + 1) * BLK, h * E:(h + 1) * E] for h in heads]
        kk = [qkv[0:length, HE + h * E:HE + (h + 1) * E] for h in heads]
        v = [qkv[0:length, 2 * HE + h * E:2 * HE + (h + 1) * E] for h in heads]
        s = [lax.dot_general(q[h], kk[h], (((1,), (1,)), ((), ())), preferred_element_type=F32) * inv_sqrt for h in heads]
        last = [jnp.where(mask, s[h][:, length - 128:], NEG_BIG) for h in heads]
        s = [last[h] if length == 128 else jnp.concatenate([s[h][:, :length - 128], last[h]], axis=1) for h in heads]
        m = [jnp.max(s[h], axis=-1, keepdims=True) for h in heads]
        p = [jnp.exp(s[h] - m[h]) for h in heads]
        l = [jnp.sum(p[h], axis=-1, keepdims=True) for h in heads]
        o = [jnp.dot(p[h].astype(BF16), v[h], preferred_element_type=F32) for h in heads]
        for h in heads:
            osend[b, :, h * E:(h + 1) * E] = (o[h] / l[h]).astype(BF16)
    def send_o(b, half):
        r = jnp.where(b < 4, b, 7 - b)

        @pl.when(cp == r)
        def _():
            part = pl.ds(half * HALF, HALF)
            ofull[b // 4, part, pl.ds(pl.multiple_of(cp * HE, E), HE)] = osend[b, part]

        @pl.when(cp != r)
        def _():
            o_copy(b, half, r).start()

    def wait_o(half, far):
        drain(osend.at[pl.ds(0, 1 + far), pl.ds(0, HALF)], o_recv_sem.at[2 * half + far])

    def attend_blocks(hi):
        def block_at(step):
            first, odd = step < 2, step % 2
            pair = jnp.where(hi, jnp.where(first, 2 + x, 3 - x), jnp.where(first, 1 - x, x))
            return 2 * pair + jnp.where(hi, odd, 1 - odd)

        @pl.loop(0, 4)
        def _(step):
            block = block_at(step)
            for b in range(8):
                @pl.when(block == b)
                def _():
                    with jax.named_scope(f'attend{b}'):
                        attend(b)

            for at, sends in enumerate((((0, 0),), ((0, 1),), ((1, 0), (1, 1), (2, 0), (2, 1)), ((3, 0), (3, 1)))):
                @pl.when(step == at)
                def _():
                    for which, half in sends:
                        send_o(block_at(which), half)

    away, home = 1 - tp, tp

    def y_copy(n, half):
        part = pl.ds(half * HALF, HALF)
        return remote(ysend.at[n, part], yrecv.at[n, part], y_send_sem, y_recv_sem.at[n], yn)

    top, bottom = slice(0, HALF), slice(HALF, BLK)

    def project_away():
        near = pl.ds(pl.multiple_of(2 * x * HE, E), 2 * HE)
        far = pl.ds(pl.multiple_of(2 * (1 - x) * HE, E), 2 * HE)
        drain(wo, wo_sem)
        with jax.named_scope('wait_o_away'):
            wait_o(0, 0)
        with jax.named_scope('proj'):
            ysend[0, top] = jnp.dot(ofull[away, top, near], wo[0, near, :], preferred_element_type=F32)
        with jax.named_scope('wait_o_away'):
            wait_o(0, 1)
        with jax.named_scope('proj'):
            ysend[0, top] += jnp.dot(ofull[away, top, far], wo[0, far, :], preferred_element_type=F32)
        y_copy(0, 0).start()

        @pl.loop(1, NOUT)
        def _(n):
            with jax.named_scope('proj'):
                ysend[n, top] = jnp.dot(ofull[away, top], wo[n], preferred_element_type=F32)
            y_copy(n, 0).start()

    def project_rest():
        with jax.named_scope('wait_o_away'):
            wait_o(1, 0)
            wait_o(1, 1)

        @pl.loop(0, NOUT)
        def _(n):
            with jax.named_scope('proj'):
                ysend[n, bottom] = jnp.dot(ofull[away, bottom], wo[n], preferred_element_type=F32)
            y_copy(n, 1).start()

    @pl.loop(0, 4)
    def _(stage):
        @pl.when(stage == 2 * tp)
        def _():
            rest_of_rows()

        @pl.when((stage == 1 - tp) | (stage == 3))
        def _():
            attend_blocks((stage < 2) == (tp == 0))

        @pl.when(stage == 2 - tp)
        def _():
            project_away()

            @pl.when((tp == 1) | (c == 0))
            def _():
                project_rest()

    with jax.named_scope('wait_o_home'):
        drain(osend.at[pl.ds(0, 3)], o_recv_sem.at[4])

    @pl.when((tp == 0) & (c == 1))
    def _():
        project_rest()

    def kept(n):
        return acc.at[pl.ds(pl.multiple_of(n % 6 * BLK, BLK), BLK), pl.ds(pl.multiple_of(n // 6 * NC, NC), NC)]

    @pl.loop(0, NOUT)
    def _(n):
        kept(n)[...] = jnp.dot(ofull[home], wo[n], preferred_element_type=F32)

    @pl.loop(0, NOUT)
    def _(n):
        with jax.named_scope('wait_y'):
            drain(yrecv.at[n], y_recv_sem.at[n])
        y_ref[:, pl.ds(pl.multiple_of(n * NC, NC), NC)] = (kept(n)[...] + yrecv[n]).astype(BF16)

    drain(xs.at[:, pl.ds(0, 3 * BLK), :], own_send)
    drain(xs.at[:, pl.ds(0, 3 * BLK), :], fwd_send)
    for t in range(2):
        for xx in range(2):
            over_x = DIAG_X * BLK if t else (NK - LATE) * BLK + (1 - xx) * HALF
            over_y = LATE * BLK - xx * HALF if t else (NK - DIAG_X) * BLK

            @pl.when((tp == t) & (x == xx))
            def _():
                drain(xs.at[0, pl.ds(0, over_x), :], dg_send.at[0])
                drain(xs.at[0, pl.ds(0, over_y), :], dg_send.at[1])
    drain(osend.at[pl.ds(0, 6)], o_send_sem)
    drain(ysend, y_send_sem)


def solution(mesh):
    def device_fn(x_loc, w_q, w_k, w_v, w_o):
        dma = pltpu.SemaphoreType.DMA
        heads_major = [jnp.transpose(t, (1, 0, 2)) for t in (w_q, w_k, w_v)]
        return pl.pallas_call(
            kernel,
            name='attention_layer',
            out_shape=pltpu.VMEM((BLK, D), BF16),
            in_specs=[pl.BlockSpec(memory_space=pl.ANY)] * 5,
            out_specs=pl.BlockSpec(memory_space=pltpu.VMEM),
            scratch_shapes=[
                pltpu.VMEM((NK, 512, KC), BF16),
                pltpu.VMEM((D, NQKV), BF16),
                pltpu.VMEM((NOUT, 20 * E, NC), BF16),
                pltpu.VMEM((512, NQKV), BF16),
                pltpu.VMEM((384, NQKV), F32),
                pltpu.VMEM((8, BLK, HE), BF16),
                pltpu.VMEM((2, BLK, 20 * E), BF16),
                pltpu.VMEM((NOUT, BLK, NC), F32),
                pltpu.VMEM((NOUT, BLK, NC), F32),
                dma, dma, dma,
                dma, dma, dma((3, NK)),
                dma, dma((2 * NK + LATE,)), dma((2,)),
                dma, dma((5,)),
                dma, dma((NOUT,)),
            ],
            compiler_params=pltpu.CompilerParams(collective_id=0, has_side_effects=True, vmem_limit_bytes=64 * 1000 * 1000),
        )(x_loc, *heads_major, w_o.reshape(20 * E, D))

    seq_spec = P(('dp', 'cp', 'tp'), None)
    head_spec = P(None, 'tp', None)
    return jax.shard_map(device_fn, mesh=mesh, in_specs=(seq_spec, head_spec, head_spec, head_spec, P('tp', None, None)), out_specs=seq_spec, check_vma=False)
```

```python
import functools

import jax
import jax.numpy as jnp
from jax import lax
from jax.experimental import pallas as pl
from jax.experimental.pallas import tpu as pltpu
from jax.sharding import PartitionSpec as P


BF16, F32 = jnp.bfloat16, jnp.float32
NEG_BIG = -1e30
D = 5120
E = 128
HEADS = 5
HE = HEADS * E
NQKV = 3 * HE
BLK = 64
HALF = BLK // 2
NK = 10
KC = D // NK
LATE = NK // 2
DIAG_X = 7
NOUT = 10
NC = D // NOUT
MESH = pl.DeviceIdType.MESH


def remote(src, dst, send_sem, recv_sem, dev):
    return pltpu.make_async_remote_copy(src_ref=src, dst_ref=dst, send_sem=send_sem, recv_sem=recv_sem, device_id=dev, device_id_type=MESH)


def drain(ref, sem):
    pltpu.make_async_copy(ref, ref, sem).wait()


def kernel(x_hbm, wq_hbm, wk_hbm, wv_hbm, wo_hbm, y_ref, xs, w, wo, qkv, acc, osend, ofull, ysend, yrecv,
           xin_sem, w_sem, wo_sem, own_send, sib_recv, direct_recv, fwd_send, fwd_recv, dg_send, o_send_sem, o_recv_sem,
           y_send_sem, y_recv_sem):
    cp, tp = lax.axis_index('cp'), lax.axis_index('tp')
    x, c = cp // 2, cp % 2
    sib = {'cp': 2 * x + 1 - c, 'tp': tp}
    xn = {'cp': 2 * (1 - x) + c, 'tp': tp}
    xo = {'cp': 2 * (1 - x) + 1 - c, 'tp': tp}
    yn = {'cp': cp, 'tp': 1 - tp}

    def rows(group, core):
        return pl.ds(pl.multiple_of(group * 128 + core * BLK, BLK), BLK)

    def x_in(k):
        return pltpu.make_async_copy(x_hbm.at[:, pl.ds(k * KC, KC)], xs.at[k, rows(0, c), :], xin_sem)

    def w_in(j):
        src = (wq_hbm, wk_hbm, wv_hbm)[j // HEADS].at[cp * HEADS + j % HEADS]
        return pltpu.make_async_copy(src, w.at[:, pl.ds(j * E, E)], w_sem)

    def wo_in(n):
        return pltpu.make_async_copy(wo_hbm.at[:, pl.ds(n * NC, NC)], wo.at[n], wo_sem)

    for k in range(NK):
        x_in(k).start()
    barrier = pltpu.get_barrier_semaphore()
    for dev in (sib, xn, xo, yn):
        pl.semaphore_signal(barrier, inc=1, device_id=dev, device_id_type=MESH)
    drain(xs.at[:, rows(0, c), :], xin_sem)
    for j in range(3 * HEADS):
        w_in(j).start()
    with jax.named_scope('barrier'):
        pl.semaphore_wait(barrier, 4)

    def group_of(kind, t):
        return (1, 2 + t, 3 - t, 0)[kind]

    def own(k, kind):
        dev, t = ((yn, 1 - tp), (xn, tp), None, (sib, tp))[kind]
        return remote(xs.at[k, rows(0, c), :], xs.at[k, rows(group_of(kind, t), c), :], own_send, sib_recv if kind == 3 else direct_recv.at[kind, k], dev)

    def diag(k, over_y):
        dev, src, t = (yn, group_of(1, tp), 1 - tp) if over_y else (xn, group_of(0, tp), tp)
        return remote(xs.at[k, rows(src, c), :], xs.at[k, rows(group_of(2, t), c), :], dg_send.at[int(over_y)], direct_recv.at[2, k], dev)

    def half_diag(over_y):
        dev, src, t = (yn, group_of(1, tp), 1 - tp) if over_y else (xn, group_of(0, tp), tp)
        k, first = LATE - 1, 0 if over_y else HALF
        return remote(xs.at[k, pl.ds(pl.multiple_of(src * 128 + c * BLK + first, HALF), HALF), :],
                      xs.at[k, pl.ds(pl.multiple_of(group_of(2, t) * 128 + c * BLK + first, HALF), HALF), :],
                      dg_send.at[int(over_y)], direct_recv.at[2, k], dev)

    def fwd(k, kind):
        sl = rows(group_of(kind, tp), c)
        second = NK + k % LATE
        sem = (k, jnp.where(tp == 0, k, second), jnp.where(tp == 0, second, NK + LATE + k))[kind]
        return remote(xs.at[k, sl, :], xs.at[k, sl, :], fwd_send, fwd_recv.at[sem], sib)

    def direct_wait(k, kind):
        drain(xs.at[k, rows(group_of(kind, tp), c), :], direct_recv.at[kind, k])

    def sends_diag_x(k):
        return jnp.where(tp == 0, k >= LATE, k < DIAG_X)

    def sends_half_x(k):
        return (tp == 0) & (x == 0) & (k == LATE - 1)

    def sends_diag_y(k):
        return jnp.where(tp == 0, k >= DIAG_X, k < LATE - x)

    def sends_half_y(k):
        return (tp == 1) & (x == 1) & (k == LATE - 1)

    def handle(k, kind):
        direct_wait(k, kind)
        fwd(k, kind).start()
        if kind == 0:
            @pl.when(sends_diag_x(k))
            def _():
                diag(k, False).start()

            @pl.when(sends_half_x(k))
            def _():
                half_diag(False).start()
        if kind == 1:
            @pl.when(sends_diag_y(k))
            def _():
                diag(k, True).start()

            @pl.when(sends_half_y(k))
            def _():
                half_diag(True).start()

    for k in range(NK):
        if k < LATE:
            own(k, 1).start()
        else:
            @pl.when(tp == 0)
            def _():
                own(k, 1).start()
        own(k, 0).start()
        own(k, 3).start()

    acc[...] = jnp.zeros_like(acc)

    def nat(xx, core, t):
        b = 2 * xx + core
        return jnp.where(t == 0, b, 7 - b) * BLK

    nat_of = [nat(x, 0, tp), nat(x, 1, tp), nat(x, 0, 1 - tp), nat(x, 1, 1 - tp),
              nat(1 - x, 0, 0), nat(1 - x, 1, 0), nat(1 - x, 0, 1), nat(1 - x, 1, 1)]

    def put_qkv(slot, col, n, val):
        qkv[pl.ds(pl.multiple_of(nat_of[slot], BLK), BLK), pl.ds(col, n)] = val.astype(BF16)

    NSTEPS = ((0, 512), (512, 512), (1024, 512), (1536, 384))

    def own_chip():
        with jax.named_scope('wait_sib'):
            drain(xs.at[:, rows(0, c), :], sib_recv)
        with jax.named_scope('wait_w'):
            drain(w, w_sem)
        for n in range(NOUT):
            wo_in(n).start()
        for col, n in NSTEPS:
            val = jnp.dot(xs[0, 0:128, :], w[0:KC, col:col + n], preferred_element_type=F32)
            for k in range(1, NK):
                val += jnp.dot(xs[k, 0:128, :], w[k * KC:(k + 1) * KC, col:col + n], preferred_element_type=F32)
            put_qkv(0, col, n, val[:BLK])
            put_qkv(1, col, n, val[BLK:])

    def accumulate(chunks, row, m, arow):
        for col, n in NSTEPS:
            val = acc[arow:arow + m, col:col + n]
            for k in chunks:
                val += jnp.dot(xs[k, row:row + m, :], w[pl.ds(pl.multiple_of(k * KC, KC), KC), col:col + n], preferred_element_type=F32)
            acc[arow:arow + m, col:col + n] = val

    def diag_order(m):
        return jnp.where(m < 5, m, jnp.where(m % 2 == 1, 7 + (m - 5) // 2, 5 + (m - 6) // 2))

    def wait_fwd2(j):
        with jax.named_scope('w_fwd2'):
            drain(xs.at[0, pl.ds(384, 128), :], fwd_recv.at[NK + j])

    def pair(j):
        wait_fwd2(j)
        with jax.named_scope('acc_b'):
            accumulate((j, j + LATE), 384, 128, 256)

    @pl.loop(0, NK + LATE)
    def _(i):
        @pl.when(i < NK)
        def _():
            with jax.named_scope('h_y'):
                handle(i, 0)

        @pl.when(i < jnp.where(tp == 0, NK, LATE))
        def _():
            with jax.named_scope('h_x'):
                handle(i, 1)

        @pl.when((tp == 1) & (i == DIAG_X - 1))
        def _():
            for k in range(LATE, NK):
                own(k, 1).start()

        @pl.when((tp == 0) & (i >= NK) & (i < NK + LATE))
        def _():
            with jax.named_scope('h_d2'):
                handle(i - NK, 2)
                handle(i - NK + LATE, 2)

        @pl.when((tp == 1) & (i >= 5) & (i < NK + 3))
        def _():
            with jax.named_scope('h_d'):
                handle(diag_order(jnp.where(i == NK + 2, 8, i - 5)), 2)

                @pl.when(i > NK)
                def _():
                    handle(diag_order(jnp.where(i == NK + 2, 9, 7)), 2)

        @pl.when(i == 2)
        def _():
            own_chip()

        @pl.when((i >= 2) & (i < NK + 2))
        def _():
            k = i - 2

            @pl.when(tp == 0)
            def _():
                with jax.named_scope('w_fwd'):
                    drain(xs.at[k, pl.ds(128, 128), :], fwd_recv.at[k])
                with jax.named_scope('acc_a'):
                    accumulate((k,), 128, 256, 0)

            @pl.when(tp == 1)
            def _():
                with jax.named_scope('w_fwd'):
                    drain(xs.at[k, pl.ds(128, BLK), :], fwd_recv.at[k])
                with jax.named_scope('acc_y'):
                    accumulate((k,), 128, 128, 0)

        def wait_d(k):
            with jax.named_scope('w_fwd'):
                drain(xs.at[k, pl.ds(256, BLK), :], fwd_recv.at[NK + LATE + k])

        @pl.when((tp == 1) & (i >= 6) & (i < NK + 2))
        def _():
            k = diag_order(i - 6)
            wait_d(k)
            with jax.named_scope('acc_d'):
                accumulate((k,), 256, 128, 128)

        @pl.when((tp == 1) & (i >= NK + 2) & (i < NK + 4))
        def _():
            k, k2 = i - NK + 3, i - NK + 6
            wait_d(k)
            wait_d(k2)
            with jax.named_scope('acc_d'):
                accumulate((k, k2), 256, 128, 128)

        @pl.when((tp == 0) & (i > NK) & (i < NK + LATE))
        def _():
            pair(i - NK - 1)

    for col, n in NSTEPS:
        for s in range(4):
            put_qkv(2 + s, col, n, acc[s * BLK:(s + 1) * BLK, col:col + n])

    def rest_of_rows():
        @pl.when(tp == 1)
        def _():
            @pl.loop(0, LATE)
            def _(j):
                with jax.named_scope('h_x2'):
                    handle(j + LATE, 1)

                @pl.when(j > 0)
                def _():
                    pair(j - 1)

        wait_fwd2(LATE - 1)
        with jax.named_scope('acc_b'):
            for col, n in NSTEPS:
                val = acc[256:384, col:col + n]
                for k in (LATE - 1, NK - 1):
                    val += jnp.dot(xs[k, 384:512, :], w[k * KC:(k + 1) * KC, col:col + n], preferred_element_type=F32)
                for s in range(2):
                    put_qkv(6 + s, col, n, val[s * BLK:(s + 1) * BLK])

    inv_sqrt = E ** -0.5

    def o_copy(b, half, dev_cp):
        lohi, part = b // 4, pl.ds(half * HALF, HALF)
        return remote(osend.at[b, part], ofull.at[lohi, part, pl.ds(pl.multiple_of(cp * HE, E), HE)],
                      o_send_sem, o_recv_sem.at[jnp.where(lohi == tp, 4, 2 * half + jnp.where(x == dev_cp // 2, 0, 1))], {'cp': dev_cp, 'tp': tp})

    def attend(b):
        length = 128 * (b // 2 + 1)
        ri = lax.broadcasted_iota(jnp.int32, (BLK, 128), 0) + BLK * (b % 2)
        ci = lax.broadcasted_iota(jnp.int32, (BLK, 128), 1)
        mask = ci <= ri
        heads = range(HEADS)
        q = [qkv[b * BLK:(b + 1) * BLK, h * E:(h + 1) * E] for h in heads]
        kk = [qkv[0:length, HE + h * E:HE + (h + 1) * E] for h in heads]
        v = [qkv[0:length, 2 * HE + h * E:2 * HE + (h + 1) * E] for h in heads]
        s = [lax.dot_general(q[h], kk[h], (((1,), (1,)), ((), ())), preferred_element_type=F32) * inv_sqrt for h in heads]
        last = [jnp.where(mask, s[h][:, length - 128:], NEG_BIG) for h in heads]
        s = [last[h] if length == 128 else jnp.concatenate([s[h][:, :length - 128], last[h]], axis=1) for h in heads]
        m = [jnp.max(s[h], axis=-1, keepdims=True) for h in heads]
        p = [jnp.exp(s[h] - m[h]) for h in heads]
        l = [jnp.sum(p[h], axis=-1, keepdims=True) for h in heads]
        o = [jnp.dot(p[h].astype(BF16), v[h], preferred_element_type=F32) for h in heads]
        for h in heads:
            osend[b, :, h * E:(h + 1) * E] = (o[h] / l[h]).astype(BF16)
    def send_o(b, half):
        r = jnp.where(b < 4, b, 7 - b)

        @pl.when(cp == r)
        def _():
            part = pl.ds(half * HALF, HALF)
            ofull[b // 4, part, pl.ds(pl.multiple_of(cp * HE, E), HE)] = osend[b, part]

        @pl.when(cp != r)
        def _():
            o_copy(b, half, r).start()

    def wait_o(half, far):
        drain(osend.at[pl.ds(0, 1 + far), pl.ds(0, HALF)], o_recv_sem.at[2 * half + far])

    def attend_blocks(hi):
        def block_at(step):
            first, odd = step < 2, step % 2
            pair = jnp.where(hi, jnp.where(first, 2 + x, 3 - x), jnp.where(first, 1 - x, x))
            return 2 * pair + jnp.where(hi, odd, 1 - odd)

        @pl.loop(0, 4)
        def _(step):
            block = block_at(step)
            for b in range(8):
                @pl.when(block == b)
                def _():
                    with jax.named_scope(f'attend{b}'):
                        attend(b)

            for at, sends in enumerate((((0, 0),), ((0, 1),), ((1, 0), (1, 1), (2, 0), (2, 1)), ((3, 0), (3, 1)))):
                @pl.when(step == at)
                def _():
                    for which, half in sends:
                        send_o(block_at(which), half)

    away, home = 1 - tp, tp

    def y_copy(n, half):
        part = pl.ds(half * HALF, HALF)
        return remote(ysend.at[n, part], yrecv.at[n, part], y_send_sem, y_recv_sem.at[n], yn)

    top, bottom = slice(0, HALF), slice(HALF, BLK)

    def project_away():
        near = pl.ds(pl.multiple_of(2 * x * HE, E), 2 * HE)
        far = pl.ds(pl.multiple_of(2 * (1 - x) * HE, E), 2 * HE)
        drain(wo, wo_sem)
        with jax.named_scope('wait_o_away'):
            wait_o(0, 0)
        with jax.named_scope('proj'):
            ysend[0, top] = jnp.dot(ofull[away, top, near], wo[0, near, :], preferred_element_type=F32)
        with jax.named_scope('wait_o_away'):
            wait_o(0, 1)
        with jax.named_scope('proj'):
            ysend[0, top] += jnp.dot(ofull[away, top, far], wo[0, far, :], preferred_element_type=F32)
        y_copy(0, 0).start()

        @pl.loop(1, NOUT)
        def _(n):
            with jax.named_scope('proj'):
                ysend[n, top] = jnp.dot(ofull[away, top], wo[n], preferred_element_type=F32)
            y_copy(n, 0).start()

    def project_rest():
        with jax.named_scope('wait_o_away'):
            wait_o(1, 0)
            wait_o(1, 1)

        @pl.loop(0, NOUT)
        def _(n):
            with jax.named_scope('proj'):
                ysend[n, bottom] = jnp.dot(ofull[away, bottom], wo[n], preferred_element_type=F32)
            y_copy(n, 1).start()

    @pl.loop(0, 4)
    def _(stage):
        @pl.when(stage == 2 * tp)
        def _():
            rest_of_rows()

        @pl.when((stage == 1 - tp) | (stage == 3))
        def _():
            attend_blocks((stage < 2) == (tp == 0))

        @pl.when(stage == 2 - tp)
        def _():
            project_away()

            @pl.when((tp == 1) | (c == 0))
            def _():
                project_rest()

    with jax.named_scope('wait_o_home'):
        drain(osend.at[pl.ds(0, 3)], o_recv_sem.at[4])

    @pl.when((tp == 0) & (c == 1))
    def _():
        project_rest()

    def kept(n):
        return acc.at[pl.ds(pl.multiple_of(n % 6 * BLK, BLK), BLK), pl.ds(pl.multiple_of(n // 6 * NC, NC), NC)]

    @pl.loop(0, NOUT)
    def _(n):
        kept(n)[...] = jnp.dot(ofull[home], wo[n], preferred_element_type=F32)

    @pl.loop(0, NOUT)
    def _(n):
        with jax.named_scope('wait_y'):
            drain(yrecv.at[n], y_recv_sem.at[n])
        y_ref[:, pl.ds(pl.multiple_of(n * NC, NC), NC)] = (kept(n)[...] + yrecv[n]).astype(BF16)

    drain(xs.at[:, pl.ds(0, 3 * BLK), :], own_send)
    drain(xs.at[:, pl.ds(0, 3 * BLK), :], fwd_send)
    for t in range(2):
        for xx in range(2):
            over_x = DIAG_X * BLK if t else (NK - LATE) * BLK + (1 - xx) * HALF
            over_y = LATE * BLK - xx * HALF if t else (NK - DIAG_X) * BLK

            @pl.when((tp == t) & (x == xx))
            def _():
                drain(xs.at[0, pl.ds(0, over_x), :], dg_send.at[0])
                drain(xs.at[0, pl.ds(0, over_y), :], dg_send.at[1])
    drain(osend.at[pl.ds(0, 6)], o_send_sem)
    drain(ysend, y_send_sem)


def solution(mesh):
    def device_fn(x_loc, w_q, w_k, w_v, w_o):
        dma = pltpu.SemaphoreType.DMA
        heads_major = [jnp.transpose(t, (1, 0, 2)) for t in (w_q, w_k, w_v)]
        return pl.pallas_call(
            kernel,
            name='attention_layer',
            out_shape=pltpu.VMEM((BLK, D), BF16),
            in_specs=[pl.BlockSpec(memory_space=pl.ANY)] * 5,
            out_specs=pl.BlockSpec(memory_space=pltpu.VMEM),
            scratch_shapes=[
                pltpu.VMEM((NK, 512, KC), BF16),
                pltpu.VMEM((D, NQKV), BF16),
                pltpu.VMEM((NOUT, 20 * E, NC), BF16),
                pltpu.VMEM((512, NQKV), BF16),
                pltpu.VMEM((384, NQKV), F32),
                pltpu.VMEM((8, BLK, HE), BF16),
                pltpu.VMEM((2, BLK, 20 * E), BF16),
                pltpu.VMEM((NOUT, BLK, NC), F32),
                pltpu.VMEM((NOUT, BLK, NC), F32),
                dma, dma, dma,
                dma, dma, dma((3, NK)),
                dma, dma((2 * NK + LATE,)), dma((2,)),
                dma, dma((5,)),
                dma, dma((NOUT,)),
            ],
            compiler_params=pltpu.CompilerParams(collective_id=0, has_side_effects=True, vmem_limit_bytes=64 * 1000 * 1000),
        )(x_loc, *heads_major, w_o.reshape(20 * E, D))

    seq_spec = P(('dp', 'cp', 'tp'), None)
    head_spec = P(None, 'tp', None)
    return jax.shard_map(device_fn, mesh=mesh, in_specs=(seq_spec, head_spec, head_spec, head_spec, P('tp', None, None)), out_specs=seq_spec, check_vma=False)
```

```python
import functools

import jax
import jax.numpy as jnp
from jax import lax
from jax.experimental import pallas as pl
from jax.experimental.pallas import tpu as pltpu
from jax.sharding import PartitionSpec as P


BF16, F32 = jnp.bfloat16, jnp.float32
NEG_BIG = -1e30
D = 5120
E = 128
HEADS = 5
HE = HEADS * E
NQKV = 3 * HE
BLK = 64
HALF = BLK // 2
NK = 10
KC = D // NK
LATE = NK // 2
DIAG_X = 7
NOUT = 10
NC = D // NOUT
MESH = pl.DeviceIdType.MESH


def remote(src, dst, send_sem, recv_sem, dev):
    return pltpu.make_async_remote_copy(src_ref=src, dst_ref=dst, send_sem=send_sem, recv_sem=recv_sem, device_id=dev, device_id_type=MESH)


def drain(ref, sem):
    pltpu.make_async_copy(ref, ref, sem).wait()


def kernel(x_hbm, wq_hbm, wk_hbm, wv_hbm, wo_hbm, y_ref, xs, w, wo, qkv, acc, osend, ofull, ysend, yrecv,
           xin_sem, w_sem, wo_sem, own_send, sib_recv, direct_recv, fwd_send, fwd_recv, dg_send, o_send_sem, o_recv_sem,
           y_send_sem, y_recv_sem):
    cp, tp = lax.axis_index('cp'), lax.axis_index('tp')
    x, c = cp // 2, cp % 2
    sib = {'cp': 2 * x + 1 - c, 'tp': tp}
    xn = {'cp': 2 * (1 - x) + c, 'tp': tp}
    xo = {'cp': 2 * (1 - x) + 1 - c, 'tp': tp}
    yn = {'cp': cp, 'tp': 1 - tp}

    def rows(group, core):
        return pl.ds(pl.multiple_of(group * 128 + core * BLK, BLK), BLK)

    def x_in(k):
        return pltpu.make_async_copy(x_hbm.at[:, pl.ds(k * KC, KC)], xs.at[k, rows(0, c), :], xin_sem)

    def w_in(j):
        src = (wq_hbm, wk_hbm, wv_hbm)[j // HEADS].at[cp * HEADS + j % HEADS]
        return pltpu.make_async_copy(src, w.at[:, pl.ds(j * E, E)], w_sem)

    def wo_in(n):
        return pltpu.make_async_copy(wo_hbm.at[:, pl.ds(n * NC, NC)], wo.at[n], wo_sem)

    for k in range(NK):
        x_in(k).start()
    barrier = pltpu.get_barrier_semaphore()
    for dev in (sib, xn, xo, yn):
        pl.semaphore_signal(barrier, inc=1, device_id=dev, device_id_type=MESH)
    drain(xs.at[:, rows(0, c), :], xin_sem)
    for j in range(3 * HEADS):
        w_in(j).start()
    with jax.named_scope('barrier'):
        pl.semaphore_wait(barrier, 4)

    def group_of(kind, t):
        return (1, 2 + t, 3 - t, 0)[kind]

    def own(k, kind):
        dev, t = ((yn, 1 - tp), (xn, tp), None, (sib, tp))[kind]
        return remote(xs.at[k, rows(0, c), :], xs.at[k, rows(group_of(kind, t), c), :], own_send, sib_recv if kind == 3 else direct_recv.at[kind, k], dev)

    def diag(k, over_y):
        dev, src, t = (yn, group_of(1, tp), 1 - tp) if over_y else (xn, group_of(0, tp), tp)
        return remote(xs.at[k, rows(src, c), :], xs.at[k, rows(group_of(2, t), c), :], dg_send.at[int(over_y)], direct_recv.at[2, k], dev)

    def half_diag(over_y):
        dev, src, t = (yn, group_of(1, tp), 1 - tp) if over_y else (xn, group_of(0, tp), tp)
        k, first = LATE - 1, 0 if over_y else HALF
        return remote(xs.at[k, pl.ds(pl.multiple_of(src * 128 + c * BLK + first, HALF), HALF), :],
                      xs.at[k, pl.ds(pl.multiple_of(group_of(2, t) * 128 + c * BLK + first, HALF), HALF), :],
                      dg_send.at[int(over_y)], direct_recv.at[2, k], dev)

    def fwd(k, kind):
        sl = rows(group_of(kind, tp), c)
        second = NK + k % LATE
        sem = (k, jnp.where(tp == 0, k, second), jnp.where(tp == 0, second, NK + LATE + k))[kind]
        return remote(xs.at[k, sl, :], xs.at[k, sl, :], fwd_send, fwd_recv.at[sem], sib)

    def direct_wait(k, kind):
        drain(xs.at[k, rows(group_of(kind, tp), c), :], direct_recv.at[kind, k])

    def sends_diag_x(k):
        return jnp.where(tp == 0, k >= LATE, k < DIAG_X)

    def sends_half_x(k):
        return (tp == 0) & (x == 0) & (k == LATE - 1)

    def sends_diag_y(k):
        return jnp.where(tp == 0, k >= DIAG_X, k < LATE - x)

    def sends_half_y(k):
        return (tp == 1) & (x == 1) & (k == LATE - 1)

    def handle(k, kind):
        direct_wait(k, kind)
        fwd(k, kind).start()
        if kind == 0:
            @pl.when(sends_diag_x(k))
            def _():
                diag(k, False).start()

            @pl.when(sends_half_x(k))
            def _():
                half_diag(False).start()
        if kind == 1:
            @pl.when(sends_diag_y(k))
            def _():
                diag(k, True).start()

            @pl.when(sends_half_y(k))
            def _():
                half_diag(True).start()

    for k in range(NK):
        if k < LATE:
            own(k, 1).start()
        else:
            @pl.when(tp == 0)
            def _():
                own(k, 1).start()
        own(k, 0).start()
        own(k, 3).start()

    acc[...] = jnp.zeros_like(acc)

    def nat(xx, core, t):
        b = 2 * xx + core
        return jnp.where(t == 0, b, 7 - b) * BLK

    nat_of = [nat(x, 0, tp), nat(x, 1, tp), nat(x, 0, 1 - tp), nat(x, 1, 1 - tp),
              nat(1 - x, 0, 0), nat(1 - x, 1, 0), nat(1 - x, 0, 1), nat(1 - x, 1, 1)]

    def put_qkv(slot, col, n, val):
        qkv[pl.ds(pl.multiple_of(nat_of[slot], BLK), BLK), pl.ds(col, n)] = val.astype(BF16)

    NSTEPS = ((0, 512), (512, 512), (1024, 512), (1536, 384))

    def own_chip():
        with jax.named_scope('wait_sib'):
            drain(xs.at[:, rows(0, c), :], sib_recv)
        with jax.named_scope('wait_w'):
            drain(w, w_sem)
        for n in range(NOUT):
            wo_in(n).start()
        for col, n in NSTEPS:
            val = jnp.dot(xs[0, 0:128, :], w[0:KC, col:col + n], preferred_element_type=F32)
            for k in range(1, NK):
                val += jnp.dot(xs[k, 0:128, :], w[k * KC:(k + 1) * KC, col:col + n], preferred_element_type=F32)
            put_qkv(0, col, n, val[:BLK])
            put_qkv(1, col, n, val[BLK:])

    def accumulate(chunks, row, m, arow):
        for col, n in NSTEPS:
            val = acc[arow:arow + m, col:col + n]
            for k in chunks:
                val += jnp.dot(xs[k, row:row + m, :], w[pl.ds(pl.multiple_of(k * KC, KC), KC), col:col + n], preferred_element_type=F32)
            acc[arow:arow + m, col:col + n] = val

    def diag_order(m):
        return jnp.where(m < 5, m, jnp.where(m % 2 == 1, 7 + (m - 5) // 2, 5 + (m - 6) // 2))

    def wait_fwd2(j):
        with jax.named_scope('w_fwd2'):
            drain(xs.at[0, pl.ds(384, 128), :], fwd_recv.at[NK + j])

    def pair(j):
        wait_fwd2(j)
        with jax.named_scope('acc_b'):
            accumulate((j, j + LATE), 384, 128, 256)

    @pl.loop(0, NK + LATE)
    def _(i):
        @pl.when(i < NK)
        def _():
            with jax.named_scope('h_y'):
                handle(i, 0)

        @pl.when(i < jnp.where(tp == 0, NK, LATE))
        def _():
            with jax.named_scope('h_x'):
                handle(i, 1)

        @pl.when((tp == 0) & (i >= NK) & (i < NK + LATE))
        def _():
            with jax.named_scope('h_d2'):
                handle(i - NK, 2)
                handle(i - NK + LATE, 2)

        @pl.when((tp == 1) & (i >= 5) & (i < NK + 3))
        def _():
            with jax.named_scope('h_d'):
                handle(diag_order(jnp.where(i == NK + 2, 8, i - 5)), 2)

                @pl.when(i > NK)
                def _():
                    handle(diag_order(jnp.where(i == NK + 2, 9, 7)), 2)

        @pl.when(i == 2)
        def _():
            own_chip()

        @pl.when((i >= 2) & (i < NK + 2))
        def _():
            k = i - 2

            @pl.when(tp == 0)
            def _():
                with jax.named_scope('w_fwd'):
                    drain(xs.at[k, pl.ds(128, 128), :], fwd_recv.at[k])
                with jax.named_scope('acc_a'):
                    accumulate((k,), 128, 256, 0)

            @pl.when(tp == 1)
            def _():
                with jax.named_scope('w_fwd'):
                    drain(xs.at[k, pl.ds(128, BLK), :], fwd_recv.at[k])
                with jax.named_scope('acc_y'):
                    accumulate((k,), 128, 128, 0)

        def wait_d(k):
            with jax.named_scope('w_fwd'):
                drain(xs.at[k, pl.ds(256, BLK), :], fwd_recv.at[NK + LATE + k])

        @pl.when((tp == 1) & (i >= 6) & (i < NK + 2))
        def _():
            k = diag_order(i - 6)
            wait_d(k)
            with jax.named_scope('acc_d'):
                accumulate((k,), 256, 128, 128)

        @pl.when((tp == 1) & (i >= NK + 2) & (i < NK + 4))
        def _():
            k, k2 = i - NK + 3, i - NK + 6
            wait_d(k)
            wait_d(k2)
            with jax.named_scope('acc_d'):
                accumulate((k, k2), 256, 128, 128)

        @pl.when((tp == 0) & (i > NK) & (i < NK + LATE))
        def _():
            pair(i - NK - 1)

    for col, n in NSTEPS:
        for s in range(4):
            put_qkv(2 + s, col, n, acc[s * BLK:(s + 1) * BLK, col:col + n])

    def rest_of_rows():
        @pl.when(tp == 1)
        def _():
            @pl.loop(0, LATE)
            def _(j):
                with jax.named_scope('h_x2'):
                    handle(j + LATE, 1)

                @pl.when(j > 0)
                def _():
                    pair(j - 1)

        wait_fwd2(LATE - 1)
        with jax.named_scope('acc_b'):
            for col, n in NSTEPS:
                val = acc[256:384, col:col + n]
                for k in (LATE - 1, NK - 1):
                    val += jnp.dot(xs[k, 384:512, :], w[k * KC:(k + 1) * KC, col:col + n], preferred_element_type=F32)
                for s in range(2):
                    put_qkv(6 + s, col, n, val[s * BLK:(s + 1) * BLK])

    inv_sqrt = E ** -0.5

    def o_copy(b, half, dev_cp):
        lohi, part = b // 4, pl.ds(half * HALF, HALF)
        return remote(osend.at[b, part], ofull.at[lohi, part, pl.ds(pl.multiple_of(cp * HE, E), HE)],
                      o_send_sem, o_recv_sem.at[jnp.where(lohi == tp, 4, 2 * half + jnp.where(x == dev_cp // 2, 0, 1))], {'cp': dev_cp, 'tp': tp})

    def attend(b):
        length = 128 * (b // 2 + 1)
        ri = lax.broadcasted_iota(jnp.int32, (BLK, 128), 0) + BLK * (b % 2)
        ci = lax.broadcasted_iota(jnp.int32, (BLK, 128), 1)
        mask = ci <= ri
        heads = range(HEADS)
        q = [qkv[b * BLK:(b + 1) * BLK, h * E:(h + 1) * E] for h in heads]
        kk = [qkv[0:length, HE + h * E:HE + (h + 1) * E] for h in heads]
        v = [qkv[0:length, 2 * HE + h * E:2 * HE + (h + 1) * E] for h in heads]
        s = [lax.dot_general(q[h], kk[h], (((1,), (1,)), ((), ())), preferred_element_type=F32) * inv_sqrt for h in heads]
        last = [jnp.where(mask, s[h][:, length - 128:], NEG_BIG) for h in heads]
        s = [last[h] if length == 128 else jnp.concatenate([s[h][:, :length - 128], last[h]], axis=1) for h in heads]
        m = [jnp.max(s[h], axis=-1, keepdims=True) for h in heads]
        p = [jnp.exp(s[h] - m[h]) for h in heads]
        l = [jnp.sum(p[h], axis=-1, keepdims=True) for h in heads]
        o = [jnp.dot(p[h].astype(BF16), v[h], preferred_element_type=F32) for h in heads]
        for h in heads:
            osend[b, :, h * E:(h + 1) * E] = (o[h] / l[h]).astype(BF16)
    def send_o(b, half):
        r = jnp.where(b < 4, b, 7 - b)

        @pl.when(cp == r)
        def _():
            part = pl.ds(half * HALF, HALF)
            ofull[b // 4, part, pl.ds(pl.multiple_of(cp * HE, E), HE)] = osend[b, part]

        @pl.when(cp != r)
        def _():
            o_copy(b, half, r).start()

    def wait_o(half, far):
        drain(osend.at[pl.ds(0, 1 + far), pl.ds(0, HALF)], o_recv_sem.at[2 * half + far])

    def attend_blocks(hi):
        def block_at(step):
            first, odd = step < 2, step % 2
            pair = jnp.where(hi, jnp.where(first, 2 + x, 3 - x), jnp.where(first, 1 - x, x))
            return 2 * pair + jnp.where(hi, odd, 1 - odd)

        @pl.loop(0, 4)
        def _(step):
            block = block_at(step)
            for b in range(8):
                @pl.when(block == b)
                def _():
                    with jax.named_scope(f'attend{b}'):
                        attend(b)

            for at, sends in enumerate((((0, 0),), ((0, 1),), ((1, 0), (1, 1), (2, 0), (2, 1)), ((3, 0), (3, 1)))):
                @pl.when(step == at)
                def _():
                    for which, half in sends:
                        send_o(block_at(which), half)

    away, home = 1 - tp, tp

    def y_copy(n, half):
        part = pl.ds(half * HALF, HALF)
        return remote(ysend.at[n, part], yrecv.at[n, part], y_send_sem, y_recv_sem.at[n], yn)

    top, bottom = slice(0, HALF), slice(HALF, BLK)

    def project_away():
        near = pl.ds(pl.multiple_of(2 * x * HE, E), 2 * HE)
        far = pl.ds(pl.multiple_of(2 * (1 - x) * HE, E), 2 * HE)
        drain(wo, wo_sem)
        with jax.named_scope('wait_o_away'):
            wait_o(0, 0)
        with jax.named_scope('proj'):
            ysend[0, top] = jnp.dot(ofull[away, top, near], wo[0, near, :], preferred_element_type=F32)
        with jax.named_scope('wait_o_away'):
            wait_o(0, 1)
        with jax.named_scope('proj'):
            ysend[0, top] += jnp.dot(ofull[away, top, far], wo[0, far, :], preferred_element_type=F32)
        y_copy(0, 0).start()

        @pl.loop(1, NOUT)
        def _(n):
            with jax.named_scope('proj'):
                ysend[n, top] = jnp.dot(ofull[away, top], wo[n], preferred_element_type=F32)
            y_copy(n, 0).start()

    def project_rest():
        with jax.named_scope('wait_o_away'):
            wait_o(1, 0)
            wait_o(1, 1)

        @pl.loop(0, NOUT)
        def _(n):
            with jax.named_scope('proj'):
                ysend[n, bottom] = jnp.dot(ofull[away, bottom], wo[n], preferred_element_type=F32)
            y_copy(n, 1).start()

    @pl.loop(0, 4)
    def _(stage):
        @pl.when(stage == 2 * tp)
        def _():
            rest_of_rows()

        @pl.when((stage == 1 - tp) | (stage == 3))
        def _():
            attend_blocks((stage < 2) == (tp == 0))

            @pl.when((tp == 1) & (stage == 0))
            def _():
                for k in range(LATE, NK):
                    own(k, 1).start()

        @pl.when(stage == 2 - tp)
        def _():
            project_away()

            @pl.when((tp == 1) | (c == 0))
            def _():
                project_rest()

    with jax.named_scope('wait_o_home'):
        drain(osend.at[pl.ds(0, 3)], o_recv_sem.at[4])

    @pl.when((tp == 0) & (c == 1))
    def _():
        project_rest()

    def kept(n):
        return acc.at[pl.ds(pl.multiple_of(n % 6 * BLK, BLK), BLK), pl.ds(pl.multiple_of(n // 6 * NC, NC), NC)]

    @pl.loop(0, NOUT)
    def _(n):
        kept(n)[...] = jnp.dot(ofull[home], wo[n], preferred_element_type=F32)

    @pl.loop(0, NOUT)
    def _(n):
        with jax.named_scope('wait_y'):
            drain(yrecv.at[n], y_recv_sem.at[n])
        y_ref[:, pl.ds(pl.multiple_of(n * NC, NC), NC)] = (kept(n)[...] + yrecv[n]).astype(BF16)

    drain(xs.at[:, pl.ds(0, 3 * BLK), :], own_send)
    drain(xs.at[:, pl.ds(0, 3 * BLK), :], fwd_send)
    for t in range(2):
        for xx in range(2):
            over_x = DIAG_X * BLK if t else (NK - LATE) * BLK + (1 - xx) * HALF
            over_y = LATE * BLK - xx * HALF if t else (NK - DIAG_X) * BLK

            @pl.when((tp == t) & (x == xx))
            def _():
                drain(xs.at[0, pl.ds(0, over_x), :], dg_send.at[0])
                drain(xs.at[0, pl.ds(0, over_y), :], dg_send.at[1])
    drain(osend.at[pl.ds(0, 6)], o_send_sem)
    drain(ysend, y_send_sem)


def solution(mesh):
    def device_fn(x_loc, w_q, w_k, w_v, w_o):
        dma = pltpu.SemaphoreType.DMA
        heads_major = [jnp.transpose(t, (1, 0, 2)) for t in (w_q, w_k, w_v)]
        return pl.pallas_call(
            kernel,
            name='attention_layer',
            out_shape=pltpu.VMEM((BLK, D), BF16),
            in_specs=[pl.BlockSpec(memory_space=pl.ANY)] * 5,
            out_specs=pl.BlockSpec(memory_space=pltpu.VMEM),
            scratch_shapes=[
                pltpu.VMEM((NK, 512, KC), BF16),
                pltpu.VMEM((D, NQKV), BF16),
                pltpu.VMEM((NOUT, 20 * E, NC), BF16),
                pltpu.VMEM((512, NQKV), BF16),
                pltpu.VMEM((384, NQKV), F32),
                pltpu.VMEM((8, BLK, HE), BF16),
                pltpu.VMEM((2, BLK, 20 * E), BF16),
                pltpu.VMEM((NOUT, BLK, NC), F32),
                pltpu.VMEM((NOUT, BLK, NC), F32),
                dma, dma, dma,
                dma, dma, dma((3, NK)),
                dma, dma((2 * NK + LATE,)), dma((2,)),
                dma, dma((5,)),
                dma, dma((NOUT,)),
            ],
            compiler_params=pltpu.CompilerParams(collective_id=0, has_side_effects=True, vmem_limit_bytes=64 * 1000 * 1000),
        )(x_loc, *heads_major, w_o.reshape(20 * E, D))

    seq_spec = P(('dp', 'cp', 'tp'), None)
    head_spec = P(None, 'tp', None)
    return jax.shard_map(device_fn, mesh=mesh, in_specs=(seq_spec, head_spec, head_spec, head_spec, P('tp', None, None)), out_specs=seq_spec, check_vma=False)
```

```python
import functools

import jax
import jax.numpy as jnp
from jax import lax
from jax.experimental import pallas as pl
from jax.experimental.pallas import tpu as pltpu
from jax.sharding import PartitionSpec as P

BF16, F32 = jnp.bfloat16, jnp.float32
NEG_BIG = -1e30
D = 5120
E = 128
HEADS = 5
HE = HEADS * E
NQKV = 3 * HE
BLK = 64
HALF = BLK // 2
NK = 10
KC = D // NK
LATE = NK // 2
DIAG_X = 7
NOUT = 10
NC = D // NOUT
MESH = pl.DeviceIdType.MESH


def remote(src, dst, send_sem, recv_sem, dev):
    return pltpu.make_async_remote_copy(src_ref=src, dst_ref=dst, send_sem=send_sem, recv_sem=recv_sem, device_id=dev, device_id_type=MESH)


def drain(ref, sem):
    pltpu.make_async_copy(ref, ref, sem).wait()


def kernel(x_hbm, wq_hbm, wk_hbm, wv_hbm, wo_hbm, y_ref, xs, w, wo, qkv, acc, osend, ofull, ysend, yrecv,
           in_sem, x_send, sib_recv, direct_recv, fwd_recv, dg_send, o_send_sem, o_recv_sem,
           y_send_sem, y_recv_sem):
    cp, tp = lax.axis_index('cp'), lax.axis_index('tp')
    x, c = cp // 2, cp % 2
    sib = {'cp': 2 * x + 1 - c, 'tp': tp}
    xn = {'cp': 2 * (1 - x) + c, 'tp': tp}
    xo = {'cp': 2 * (1 - x) + 1 - c, 'tp': tp}
    yn = {'cp': cp, 'tp': 1 - tp}

    def rows(group, core):
        return pl.ds(pl.multiple_of(group * 128 + core * BLK, BLK), BLK)

    def x_in(k):
        return pltpu.make_async_copy(x_hbm.at[:, pl.ds(k * KC, KC)], xs.at[k, rows(0, c), :], in_sem)

    def w_in(j):
        src = (wq_hbm, wk_hbm, wv_hbm)[j // HEADS].at[cp * HEADS + j % HEADS]
        return pltpu.make_async_copy(src, w.at[:, pl.ds(j * E, E)], in_sem)

    def wo_in(n):
        return pltpu.make_async_copy(wo_hbm.at[:, pl.ds(n * NC, NC)], wo.at[n], in_sem)

    for k in range(NK):
        x_in(k).start()
    barrier = pltpu.get_barrier_semaphore()
    for dev in (sib, xn, xo, yn):
        pl.semaphore_signal(barrier, inc=1, device_id=dev, device_id_type=MESH)
    drain(xs.at[:, rows(0, c), :], in_sem)
    for j in range(3 * HEADS):
        w_in(j).start()
    with jax.named_scope('barrier'):
        pl.semaphore_wait(barrier, 4)

    def group_of(kind, t):
        return (1, 2 + t, 3 - t, 0)[kind]

    def own(k, kind):
        dev, t = ((yn, 1 - tp), (xn, tp), None, (sib, tp))[kind]
        return remote(xs.at[k, rows(0, c), :], xs.at[k, rows(group_of(kind, t), c), :], x_send, sib_recv if kind == 3 else direct_recv.at[kind, k], dev)

    def diag(k, over_y):
        dev, src, t = (yn, group_of(1, tp), 1 - tp) if over_y else (xn, group_of(0, tp), tp)
        return remote(xs.at[k, rows(src, c), :], xs.at[k, rows(group_of(2, t), c), :], dg_send, direct_recv.at[2, k], dev)

    def half_diag(over_y):
        dev, src, t = (yn, group_of(1, tp), 1 - tp) if over_y else (xn, group_of(0, tp), tp)
        k, first = LATE - 1, 0 if over_y else HALF
        return remote(xs.at[k, pl.ds(pl.multiple_of(src * 128 + c * BLK + first, HALF), HALF), :],
                      xs.at[k, pl.ds(pl.multiple_of(group_of(2, t) * 128 + c * BLK + first, HALF), HALF), :],
                      dg_send, direct_recv.at[2, k], dev)

    def fwd(k, kind):
        sl = rows(group_of(kind, tp), c)
        second = NK + k % LATE
        sem = (k, jnp.where(tp == 0, k, second), jnp.where(tp == 0, second, NK + LATE + k))[kind]
        return remote(xs.at[k, sl, :], xs.at[k, sl, :], x_send, fwd_recv.at[sem], sib)

    def direct_wait(k, kind):
        drain(xs.at[k, rows(group_of(kind, tp), c), :], direct_recv.at[kind, k])

    def sends_diag_x(k):
        return jnp.where(tp == 0, k >= LATE, k < DIAG_X)

    def sends_half_x(k):
        return (tp == 0) & (x == 0) & (k == LATE - 1)

    def sends_diag_y(k):
        return jnp.where(tp == 0, k >= DIAG_X, k < LATE - x)

    def sends_half_y(k):
        return (tp == 1) & (x == 1) & (k == LATE - 1)

    def handle(k, kind):
        direct_wait(k, kind)
        fwd(k, kind).start()
        if kind == 0:
            @pl.when(sends_diag_x(k))
            def _():
                diag(k, False).start()

            @pl.when(sends_half_x(k))
            def _():
                half_diag(False).start()
        if kind == 1:
            @pl.when(sends_diag_y(k))
            def _():
                diag(k, True).start()

            @pl.when(sends_half_y(k))
            def _():
                half_diag(True).start()

    for k in range(NK):
        if k < LATE:
            own(k, 1).start()
        else:
            @pl.when(tp == 0)
            def _():
                own(k, 1).start()
        own(k, 0).start()
        own(k, 3).start()

    acc[...] = jnp.zeros_like(acc)

    def nat(xx, core, t):
        b = 2 * xx + core
        return jnp.where(t == 0, b, 7 - b) * BLK

    nat_of = [nat(x, 0, tp), nat(x, 1, tp), nat(x, 0, 1 - tp), nat(x, 1, 1 - tp),
              nat(1 - x, 0, 0), nat(1 - x, 1, 0), nat(1 - x, 0, 1), nat(1 - x, 1, 1)]

    def put_qkv(slot, col, n, val):
        qkv[pl.ds(pl.multiple_of(nat_of[slot], BLK), BLK), pl.ds(col, n)] = val.astype(BF16)

    NSTEPS = ((0, 512), (512, 512), (1024, 512), (1536, 384))

    def own_chip():
        with jax.named_scope('wait_sib'):
            drain(xs.at[:, rows(0, c), :], sib_recv)
        with jax.named_scope('wait_w'):
            drain(w, in_sem)
        for n in range(NOUT):
            wo_in(n).start()
        for col, n in NSTEPS:
            val = jnp.dot(xs[0, 0:128, :], w[0:KC, col:col + n], preferred_element_type=F32)
            for k in range(1, NK):
                val += jnp.dot(xs[k, 0:128, :], w[k * KC:(k + 1) * KC, col:col + n], preferred_element_type=F32)
            put_qkv(0, col, n, val[:BLK])
            put_qkv(1, col, n, val[BLK:])

    def accumulate(chunks, row, m, arow):
        for col, n in NSTEPS:
            val = acc[arow:arow + m, col:col + n]
            for k in chunks:
                val += jnp.dot(xs[k, row:row + m, :], w[pl.ds(pl.multiple_of(k * KC, KC), KC), col:col + n], preferred_element_type=F32)
            acc[arow:arow + m, col:col + n] = val

    def diag_order(m):
        return jnp.where(m < 5, m, jnp.where(m % 2 == 1, 7 + (m - 5) // 2, 5 + (m - 6) // 2))

    def wait_fwd2(j):
        with jax.named_scope('w_fwd2'):
            drain(xs.at[0, pl.ds(384, 128), :], fwd_recv.at[NK + j])

    def pair(j):
        wait_fwd2(j)
        with jax.named_scope('acc_b'):
            accumulate((j, j + LATE), 384, 128, 256)

    @pl.loop(0, NK + LATE)
    def _(i):
        @pl.when(i < NK)
        def _():
            with jax.named_scope('h_y'):
                handle(i, 0)

        @pl.when(i < jnp.where(tp == 0, NK, LATE))
        def _():
            with jax.named_scope('h_x'):
                handle(i, 1)

        @pl.when((tp == 0) & (i >= NK) & (i < NK + LATE))
        def _():
            with jax.named_scope('h_d2'):
                handle(i - NK, 2)
                handle(i - NK + LATE, 2)

        @pl.when((tp == 1) & (i >= 5) & (i < NK + 3))
        def _():
            with jax.named_scope('h_d'):
                handle(diag_order(jnp.where(i == NK + 2, 8, i - 5)), 2)

                @pl.when(i > NK)
                def _():
                    handle(diag_order(jnp.where(i == NK + 2, 9, 7)), 2)

        @pl.when(i == 2)
        def _():
            own_chip()

        @pl.when((i >= 2) & (i < NK + 2))
        def _():
            k = i - 2

            @pl.when(tp == 0)
            def _():
                with jax.named_scope('w_fwd'):
                    drain(xs.at[k, pl.ds(128, 128), :], fwd_recv.at[k])
                with jax.named_scope('acc_a'):
                    accumulate((k,), 128, 256, 0)

            @pl.when(tp == 1)
            def _():
                with jax.named_scope('w_fwd'):
                    drain(xs.at[k, pl.ds(128, BLK), :], fwd_recv.at[k])
                with jax.named_scope('acc_y'):
                    accumulate((k,), 128, 128, 0)

        def wait_d(k):
            with jax.named_scope('w_fwd'):
                drain(xs.at[k, pl.ds(256, BLK), :], fwd_recv.at[NK + LATE + k])

        @pl.when((tp == 1) & (i >= 6) & (i < NK + 2))
        def _():
            k = diag_order(i - 6)
            wait_d(k)
            with jax.named_scope('acc_d'):
                accumulate((k,), 256, 128, 128)

        @pl.when((tp == 1) & (i >= NK + 2) & (i < NK + 4))
        def _():
            k, k2 = i - NK + 3, i - NK + 6
            wait_d(k)
            wait_d(k2)
            with jax.named_scope('acc_d'):
                accumulate((k, k2), 256, 128, 128)

        @pl.when((tp == 0) & (i > NK) & (i < NK + LATE))
        def _():
            pair(i - NK - 1)

    for col, n in NSTEPS:
        for s in range(4):
            put_qkv(2 + s, col, n, acc[s * BLK:(s + 1) * BLK, col:col + n])

    def rest_of_rows():
        @pl.when(tp == 1)
        def _():
            @pl.loop(0, LATE)
            def _(j):
                with jax.named_scope('h_x2'):
                    handle(j + LATE, 1)

                @pl.when(j > 0)
                def _():
                    pair(j - 1)

        wait_fwd2(LATE - 1)
        with jax.named_scope('acc_b'):
            for col, n in NSTEPS:
                val = acc[256:384, col:col + n]
                for k in (LATE - 1, NK - 1):
                    val += jnp.dot(xs[k, 384:512, :], w[k * KC:(k + 1) * KC, col:col + n], preferred_element_type=F32)
                for s in range(2):
                    put_qkv(6 + s, col, n, val[s * BLK:(s + 1) * BLK])

    inv_sqrt = E ** -0.5

    def o_copy(b, half, dev_cp):
        lohi, part = b // 4, pl.ds(half * HALF, HALF)
        return remote(osend.at[b, part], ofull.at[lohi, part, pl.ds(pl.multiple_of(cp * HE, E), HE)],
                      o_send_sem, o_recv_sem.at[jnp.where(lohi == tp, 4, 2 * half + jnp.where(x == dev_cp // 2, 0, 1))], {'cp': dev_cp, 'tp': tp})

    def attend(b):
        length = 128 * (b // 2 + 1)
        ri = lax.broadcasted_iota(jnp.int32, (BLK, 128), 0) + BLK * (b % 2)
        ci = lax.broadcasted_iota(jnp.int32, (BLK, 128), 1)
        mask = ci <= ri
        heads = range(HEADS)
        q = [qkv[b * BLK:(b + 1) * BLK, h * E:(h + 1) * E] for h in heads]
        kk = [qkv[0:length, HE + h * E:HE + (h + 1) * E] for h in heads]
        v = [qkv[0:length, 2 * HE + h * E:2 * HE + (h + 1) * E] for h in heads]
        s = [lax.dot_general(q[h], kk[h], (((1,), (1,)), ((), ())), preferred_element_type=F32) * inv_sqrt for h in heads]
        last = [jnp.where(mask, s[h][:, length - 128:], NEG_BIG) for h in heads]
        s = [last[h] if length == 128 else jnp.concatenate([s[h][:, :length - 128], last[h]], axis=1) for h in heads]
        m = [jnp.max(s[h], axis=-1, keepdims=True) for h in heads]
        p = [jnp.exp(s[h] - m[h]) for h in heads]
        l = [jnp.sum(p[h], axis=-1, keepdims=True) for h in heads]
        o = [jnp.dot(p[h].astype(BF16), v[h], preferred_element_type=F32) for h in heads]
        for h in heads:
            osend[b, :, h * E:(h + 1) * E] = (o[h] / l[h]).astype(BF16)
    def send_o(b, half):
        r = jnp.where(b < 4, b, 7 - b)

        @pl.when(cp == r)
        def _():
            part = pl.ds(half * HALF, HALF)
            ofull[b // 4, part, pl.ds(pl.multiple_of(cp * HE, E), HE)] = osend[b, part]

        @pl.when(cp != r)
        def _():
            o_copy(b, half, r).start()

    def wait_o(half, far):
        drain(osend.at[pl.ds(0, 1 + far), pl.ds(0, HALF)], o_recv_sem.at[2 * half + far])

    def attend_blocks(hi):
        def block_at(step):
            first, odd = step < 2, step % 2
            pair = jnp.where(hi, jnp.where(first, 2 + x, 3 - x), jnp.where(first, 1 - x, x))
            return 2 * pair + jnp.where(hi, odd, 1 - odd)

        @pl.loop(0, 4)
        def _(step):
            block = block_at(step)
            for b in range(8):
                @pl.when(block == b)
                def _():
                    with jax.named_scope(f'attend{b}'):
                        attend(b)

            for at, sends in enumerate((((0, 0),), ((0, 1),), ((1, 0), (1, 1), (2, 0), (2, 1)), ((3, 0), (3, 1)))):
                @pl.when(step == at)
                def _():
                    for which, half in sends:
                        send_o(block_at(which), half)

    away, home = 1 - tp, tp

    def y_copy(n, half):
        part = pl.ds(half * HALF, HALF)
        return remote(ysend.at[n, part], yrecv.at[n, part], y_send_sem, y_recv_sem.at[n], yn)

    top, bottom = slice(0, HALF), slice(HALF, BLK)

    def project_away():
        near = pl.ds(pl.multiple_of(2 * x * HE, E), 2 * HE)
        far = pl.ds(pl.multiple_of(2 * (1 - x) * HE, E), 2 * HE)
        drain(wo, in_sem)
        with jax.named_scope('wait_o_away'):
            wait_o(0, 0)
        with jax.named_scope('proj'):
            ysend[0, top] = jnp.dot(ofull[away, top, near], wo[0, near, :], preferred_element_type=F32)
        with jax.named_scope('wait_o_away'):
            wait_o(0, 1)
        with jax.named_scope('proj'):
            ysend[0, top] += jnp.dot(ofull[away, top, far], wo[0, far, :], preferred_element_type=F32)
        y_copy(0, 0).start()

        @pl.loop(1, NOUT)
        def _(n):
            with jax.named_scope('proj'):
                ysend[n, top] = jnp.dot(ofull[away, top], wo[n], preferred_element_type=F32)
            y_copy(n, 0).start()

    def project_rest():
        with jax.named_scope('wait_o_away'):
            wait_o(1, 0)
            wait_o(1, 1)

        @pl.loop(0, NOUT)
        def _(n):
            with jax.named_scope('proj'):
                ysend[n, bottom] = jnp.dot(ofull[away, bottom], wo[n], preferred_element_type=F32)
            y_copy(n, 1).start()

    @pl.loop(0, 4)
    def _(stage):
        @pl.when(stage == 2 * tp)
        def _():
            rest_of_rows()

        @pl.when((stage == 1 - tp) | (stage == 3))
        def _():
            attend_blocks((stage < 2) == (tp == 0))

            @pl.when((tp == 1) & (stage == 0))
            def _():
                for k in range(LATE, NK):
                    own(k, 1).start()

        @pl.when(stage == 2 - tp)
        def _():
            project_away()

            @pl.when((tp == 1) | (c == 0))
            def _():
                project_rest()

    with jax.named_scope('wait_o_home'):
        drain(osend.at[pl.ds(0, 3)], o_recv_sem.at[4])

    @pl.when((tp == 0) & (c == 1))
    def _():
        project_rest()

    def kept(n):
        return acc.at[pl.ds(pl.multiple_of(n % 6 * BLK, BLK), BLK), pl.ds(pl.multiple_of(n // 6 * NC, NC), NC)]

    @pl.loop(0, NOUT)
    def _(n):
        kept(n)[...] = jnp.dot(ofull[home], wo[n], preferred_element_type=F32)

    @pl.loop(0, NOUT)
    def _(n):
        with jax.named_scope('wait_y'):
            drain(yrecv.at[n], y_recv_sem.at[n])
        y_ref[:, pl.ds(pl.multiple_of(n * NC, NC), NC)] = (kept(n)[...] + yrecv[n]).astype(BF16)

    drain(xs.at[:, pl.ds(0, 6 * BLK), :], x_send)
    for t in range(2):
        for xx in range(2):
            over_x = DIAG_X * BLK if t else (NK - LATE) * BLK + (1 - xx) * HALF
            over_y = LATE * BLK - xx * HALF if t else (NK - DIAG_X) * BLK

            @pl.when((tp == t) & (x == xx))
            def _():
                drain(xs.at[pl.ds(0, 2), pl.ds(0, (over_x + over_y) // 2), :], dg_send)
    drain(osend.at[pl.ds(0, 6)], o_send_sem)
    drain(ysend, y_send_sem)


def solution(mesh):
    def device_fn(x_loc, w_q, w_k, w_v, w_o):
        dma = pltpu.SemaphoreType.DMA
        heads_major = [jnp.transpose(t, (1, 0, 2)) for t in (w_q, w_k, w_v)]
        return pl.pallas_call(
            kernel,
            name='attention_layer',
            out_shape=pltpu.VMEM((BLK, D), BF16),
            in_specs=[pl.BlockSpec(memory_space=pl.ANY)] * 5,
            out_specs=pl.BlockSpec(memory_space=pltpu.VMEM),
            scratch_shapes=[
                pltpu.VMEM((NK, 512, KC), BF16),
                pltpu.VMEM((D, NQKV), BF16),
                pltpu.VMEM((NOUT, 20 * E, NC), BF16),
                pltpu.VMEM((512, NQKV), BF16),
                pltpu.VMEM((384, NQKV), F32),
                pltpu.VMEM((8, BLK, HE), BF16),
                pltpu.VMEM((2, BLK, 20 * E), BF16),
                pltpu.VMEM((NOUT, BLK, NC), F32),
                pltpu.VMEM((NOUT, BLK, NC), F32),
                dma, dma, dma, dma((3, NK)), dma((2 * NK + LATE,)), dma,
                dma, dma((5,)),
                dma, dma((NOUT,)),
            ],
            compiler_params=pltpu.CompilerParams(collective_id=0, has_side_effects=True, vmem_limit_bytes=64 * 1000 * 1000),
        )(x_loc, *heads_major, w_o.reshape(20 * E, D))

    seq_spec = P(('dp', 'cp', 'tp'), None)
    head_spec = P(None, 'tp', None)
    return jax.shard_map(device_fn, mesh=mesh, in_specs=(seq_spec, head_spec, head_spec, head_spec, P('tp', None, None)), out_specs=seq_spec, check_vma=False)
```

```python
import functools

import jax
import jax.numpy as jnp
from jax import lax
from jax.experimental import pallas as pl
from jax.experimental.pallas import tpu as pltpu
from jax.sharding import PartitionSpec as P

BF16, F32 = jnp.bfloat16, jnp.float32
NEG_BIG = -1e30
D = 5120
E = 128
HEADS = 5
HE = HEADS * E
NQKV = 3 * HE
BLK = 64
HALF = BLK // 2
NK = 10
KC = D // NK
LATE = NK // 2
DIAG_X = 7
NOUT = 10
NC = D // NOUT
MESH = pl.DeviceIdType.MESH


def remote(src, dst, send_sem, recv_sem, dev):
    return pltpu.make_async_remote_copy(src_ref=src, dst_ref=dst, send_sem=send_sem, recv_sem=recv_sem, device_id=dev, device_id_type=MESH)


def drain(ref, sem):
    pltpu.make_async_copy(ref, ref, sem).wait()


def kernel(x_hbm, wq_hbm, wk_hbm, wv_hbm, wo_hbm, y_ref, xs, w, wo, qkv, acc, osend, ofull, ysend, yrecv,
           in_sem, in_sem2, x_send, sib_recv, direct_recv, fwd_recv, dg_send, o_send_sem, o_recv_sem,
           y_send_sem, y_recv_sem):
    cp, tp = lax.axis_index('cp'), lax.axis_index('tp')
    x, c = cp // 2, cp % 2
    sib = {'cp': 2 * x + 1 - c, 'tp': tp}
    xn = {'cp': 2 * (1 - x) + c, 'tp': tp}
    xo = {'cp': 2 * (1 - x) + 1 - c, 'tp': tp}
    yn = {'cp': cp, 'tp': 1 - tp}

    def rows(group, core):
        return pl.ds(pl.multiple_of(group * 128 + core * BLK, BLK), BLK)

    def x_in(k):
        return pltpu.make_async_copy(x_hbm.at[:, pl.ds(k * KC, KC)], xs.at[k, rows(0, c), :], in_sem if k < 2 else in_sem2)

    def w_in(j):
        src = (wq_hbm, wk_hbm, wv_hbm)[j // HEADS].at[cp * HEADS + j % HEADS]
        return pltpu.make_async_copy(src, w.at[:, pl.ds(j * E, E)], in_sem)

    def wo_in(n):
        return pltpu.make_async_copy(wo_hbm.at[:, pl.ds(n * NC, NC)], wo.at[n], in_sem)

    for k in range(NK):
        x_in(k).start()
    barrier = pltpu.get_barrier_semaphore()
    for dev in (sib, xn, xo, yn):
        pl.semaphore_signal(barrier, inc=1, device_id=dev, device_id_type=MESH)
    drain(xs.at[pl.ds(0, 2), rows(0, c), :], in_sem)
    with jax.named_scope('barrier'):
        pl.semaphore_wait(barrier, 4)

    def group_of(kind, t):
        return (1, 2 + t, 3 - t, 0)[kind]

    def own(k, kind):
        dev, t = ((yn, 1 - tp), (xn, tp), None, (sib, tp))[kind]
        return remote(xs.at[k, rows(0, c), :], xs.at[k, rows(group_of(kind, t), c), :], x_send, sib_recv if kind == 3 else direct_recv.at[kind, k], dev)

    def diag(k, over_y):
        dev, src, t = (yn, group_of(1, tp), 1 - tp) if over_y else (xn, group_of(0, tp), tp)
        return remote(xs.at[k, rows(src, c), :], xs.at[k, rows(group_of(2, t), c), :], dg_send, direct_recv.at[2, k], dev)

    def half_diag(over_y):
        dev, src, t = (yn, group_of(1, tp), 1 - tp) if over_y else (xn, group_of(0, tp), tp)
        k, first = LATE - 1, 0 if over_y else HALF
        return remote(xs.at[k, pl.ds(pl.multiple_of(src * 128 + c * BLK + first, HALF), HALF), :],
                      xs.at[k, pl.ds(pl.multiple_of(group_of(2, t) * 128 + c * BLK + first, HALF), HALF), :],
                      dg_send, direct_recv.at[2, k], dev)

    def fwd(k, kind):
        sl = rows(group_of(kind, tp), c)
        second = NK + k % LATE
        sem = (k, jnp.where(tp == 0, k, second), jnp.where(tp == 0, second, NK + LATE + k))[kind]
        return remote(xs.at[k, sl, :], xs.at[k, sl, :], x_send, fwd_recv.at[sem], sib)

    def direct_wait(k, kind):
        drain(xs.at[k, rows(group_of(kind, tp), c), :], direct_recv.at[kind, k])

    def sends_diag_x(k):
        return jnp.where(tp == 0, k >= LATE, k < DIAG_X)

    def sends_half_x(k):
        return (tp == 0) & (x == 0) & (k == LATE - 1)

    def sends_diag_y(k):
        return jnp.where(tp == 0, k >= DIAG_X, k < LATE - x)

    def sends_half_y(k):
        return (tp == 1) & (x == 1) & (k == LATE - 1)

    def handle(k, kind):
        direct_wait(k, kind)
        fwd(k, kind).start()
        if kind == 0:
            @pl.when(sends_diag_x(k))
            def _():
                diag(k, False).start()

            @pl.when(sends_half_x(k))
            def _():
                half_diag(False).start()
        if kind == 1:
            @pl.when(sends_diag_y(k))
            def _():
                diag(k, True).start()

            @pl.when(sends_half_y(k))
            def _():
                half_diag(True).start()

    for k in range(NK):
        if k == 2:
            drain(xs.at[pl.ds(2, NK - 2), rows(0, c), :], in_sem2)
            for j in range(3 * HEADS):
                w_in(j).start()
        if k < LATE:
            own(k, 1).start()
        else:
            @pl.when(tp == 0)
            def _():
                own(k, 1).start()
        own(k, 0).start()
        own(k, 3).start()

    acc[...] = jnp.zeros_like(acc)

    def nat(xx, core, t):
        b = 2 * xx + core
        return jnp.where(t == 0, b, 7 - b) * BLK

    nat_of = [nat(x, 0, tp), nat(x, 1, tp), nat(x, 0, 1 - tp), nat(x, 1, 1 - tp),
              nat(1 - x, 0, 0), nat(1 - x, 1, 0), nat(1 - x, 0, 1), nat(1 - x, 1, 1)]

    def put_qkv(slot, col, n, val):
        qkv[pl.ds(pl.multiple_of(nat_of[slot], BLK), BLK), pl.ds(col, n)] = val.astype(BF16)

    NSTEPS = ((0, 512), (512, 512), (1024, 512), (1536, 384))

    def own_chip():
        with jax.named_scope('wait_sib'):
            drain(xs.at[:, rows(0, c), :], sib_recv)
        with jax.named_scope('wait_w'):
            drain(w, in_sem)
        for n in range(NOUT):
            wo_in(n).start()
        for col, n in NSTEPS:
            val = jnp.dot(xs[0, 0:128, :], w[0:KC, col:col + n], preferred_element_type=F32)
            for k in range(1, NK):
                val += jnp.dot(xs[k, 0:128, :], w[k * KC:(k + 1) * KC, col:col + n], preferred_element_type=F32)
            put_qkv(0, col, n, val[:BLK])
            put_qkv(1, col, n, val[BLK:])

    def accumulate(chunks, row, m, arow):
        for col, n in NSTEPS:
            val = acc[arow:arow + m, col:col + n]
            for k in chunks:
                val += jnp.dot(xs[k, row:row + m, :], w[pl.ds(pl.multiple_of(k * KC, KC), KC), col:col + n], preferred_element_type=F32)
            acc[arow:arow + m, col:col + n] = val

    def diag_order(m):
        return jnp.where(m < 5, m, jnp.where(m % 2 == 1, 7 + (m - 5) // 2, 5 + (m - 6) // 2))

    def wait_fwd2(j):
        with jax.named_scope('w_fwd2'):
            drain(xs.at[0, pl.ds(384, 128), :], fwd_recv.at[NK + j])

    def pair(j):
        wait_fwd2(j)
        with jax.named_scope('acc_b'):
            accumulate((j, j + LATE), 384, 128, 256)

    @pl.loop(0, NK + LATE)
    def _(i):
        @pl.when(i < NK)
        def _():
            with jax.named_scope('h_y'):
                handle(i, 0)

        @pl.when(i < jnp.where(tp == 0, NK, LATE))
        def _():
            with jax.named_scope('h_x'):
                handle(i, 1)

        @pl.when((tp == 0) & (i >= NK) & (i < NK + LATE))
        def _():
            with jax.named_scope('h_d2'):
                handle(i - NK, 2)
                handle(i - NK + LATE, 2)

        @pl.when((tp == 1) & (i >= 5) & (i < NK + 3))
        def _():
            with jax.named_scope('h_d'):
                handle(diag_order(jnp.where(i == NK + 2, 8, i - 5)), 2)

                @pl.when(i > NK)
                def _():
                    handle(diag_order(jnp.where(i == NK + 2, 9, 7)), 2)

        @pl.when(i == 2)
        def _():
            own_chip()

        @pl.when((i >= 2) & (i < NK + 2))
        def _():
            k = i - 2

            @pl.when(tp == 0)
            def _():
                with jax.named_scope('w_fwd'):
                    drain(xs.at[k, pl.ds(128, 128), :], fwd_recv.at[k])
                with jax.named_scope('acc_a'):
                    accumulate((k,), 128, 256, 0)

            @pl.when(tp == 1)
            def _():
                with jax.named_scope('w_fwd'):
                    drain(xs.at[k, pl.ds(128, BLK), :], fwd_recv.at[k])
                with jax.named_scope('acc_y'):
                    accumulate((k,), 128, 128, 0)

        def wait_d(k):
            with jax.named_scope('w_fwd'):
                drain(xs.at[k, pl.ds(256, BLK), :], fwd_recv.at[NK + LATE + k])

        @pl.when((tp == 1) & (i >= 6) & (i < NK + 2))
        def _():
            k = diag_order(i - 6)
            wait_d(k)
            with jax.named_scope('acc_d'):
                accumulate((k,), 256, 128, 128)

        @pl.when((tp == 1) & (i >= NK + 2) & (i < NK + 4))
        def _():
            k, k2 = i - NK + 3, i - NK + 6
            wait_d(k)
            wait_d(k2)
            with jax.named_scope('acc_d'):
                accumulate((k, k2), 256, 128, 128)

        @pl.when((tp == 0) & (i > NK) & (i < NK + LATE))
        def _():
            pair(i - NK - 1)

    for col, n in NSTEPS:
        for s in range(4):
            put_qkv(2 + s, col, n, acc[s * BLK:(s + 1) * BLK, col:col + n])

    def rest_of_rows():
        @pl.when(tp == 1)
        def _():
            @pl.loop(0, LATE)
            def _(j):
                with jax.named_scope('h_x2'):
                    handle(j + LATE, 1)

                @pl.when(j > 0)
                def _():
                    pair(j - 1)

        wait_fwd2(LATE - 1)
        with jax.named_scope('acc_b'):
            for col, n in NSTEPS:
                val = acc[256:384, col:col + n]
                for k in (LATE - 1, NK - 1):
                    val += jnp.dot(xs[k, 384:512, :], w[k * KC:(k + 1) * KC, col:col + n], preferred_element_type=F32)
                for s in range(2):
                    put_qkv(6 + s, col, n, val[s * BLK:(s + 1) * BLK])

    inv_sqrt = E ** -0.5

    def o_copy(b, half, dev_cp):
        lohi, part = b // 4, pl.ds(half * HALF, HALF)
        return remote(osend.at[b, part], ofull.at[lohi, part, pl.ds(pl.multiple_of(cp * HE, E), HE)],
                      o_send_sem, o_recv_sem.at[jnp.where(lohi == tp, 4, 2 * half + jnp.where(x == dev_cp // 2, 0, 1))], {'cp': dev_cp, 'tp': tp})

    def attend(b):
        length = 128 * (b // 2 + 1)
        ri = lax.broadcasted_iota(jnp.int32, (BLK, 128), 0) + BLK * (b % 2)
        ci = lax.broadcasted_iota(jnp.int32, (BLK, 128), 1)
        mask = ci <= ri
        heads = range(HEADS)
        q = [qkv[b * BLK:(b + 1) * BLK, h * E:(h + 1) * E] for h in heads]
        kk = [qkv[0:length, HE + h * E:HE + (h + 1) * E] for h in heads]
        v = [qkv[0:length, 2 * HE + h * E:2 * HE + (h + 1) * E] for h in heads]
        s = [lax.dot_general(q[h], kk[h], (((1,), (1,)), ((), ())), preferred_element_type=F32) * inv_sqrt for h in heads]
        last = [jnp.where(mask, s[h][:, length - 128:], NEG_BIG) for h in heads]
        s = [last[h] if length == 128 else jnp.concatenate([s[h][:, :length - 128], last[h]], axis=1) for h in heads]
        m = [jnp.max(s[h], axis=-1, keepdims=True) for h in heads]
        p = [jnp.exp(s[h] - m[h]) for h in heads]
        l = [jnp.sum(p[h], axis=-1, keepdims=True) for h in heads]
        o = [jnp.dot(p[h].astype(BF16), v[h], preferred_element_type=F32) for h in heads]
        for h in heads:
            osend[b, :, h * E:(h + 1) * E] = (o[h] / l[h]).astype(BF16)
    def send_o(b, half):
        r = jnp.where(b < 4, b, 7 - b)

        @pl.when(cp == r)
        def _():
            part = pl.ds(half * HALF, HALF)
            ofull[b // 4, part, pl.ds(pl.multiple_of(cp * HE, E), HE)] = osend[b, part]

        @pl.when(cp != r)
        def _():
            o_copy(b, half, r).start()

    def wait_o(half, far):
        drain(osend.at[pl.ds(0, 1 + far), pl.ds(0, HALF)], o_recv_sem.at[2 * half + far])

    def attend_blocks(hi):
        def block_at(step):
            first, odd = step < 2, step % 2
            pair = jnp.where(hi, jnp.where(first, 2 + x, 3 - x), jnp.where(first, 1 - x, x))
            return 2 * pair + jnp.where(hi, odd, 1 - odd)

        @pl.loop(0, 4)
        def _(step):
            block = block_at(step)
            for b in range(8):
                @pl.when(block == b)
                def _():
                    with jax.named_scope(f'attend{b}'):
                        attend(b)

            for at, sends in enumerate((((0, 0),), ((0, 1),), ((1, 0), (1, 1), (2, 0), (2, 1)), ((3, 0), (3, 1)))):
                @pl.when(step == at)
                def _():
                    for which, half in sends:
                        send_o(block_at(which), half)

    away, home = 1 - tp, tp

    def y_copy(n, half):
        part = pl.ds(half * HALF, HALF)
        return remote(ysend.at[n, part], yrecv.at[n, part], y_send_sem, y_recv_sem.at[n], yn)

    top, bottom = slice(0, HALF), slice(HALF, BLK)

    def project_away():
        near = pl.ds(pl.multiple_of(2 * x * HE, E), 2 * HE)
        far = pl.ds(pl.multiple_of(2 * (1 - x) * HE, E), 2 * HE)
        drain(wo, in_sem)
        with jax.named_scope('wait_o_away'):
            wait_o(0, 0)
        with jax.named_scope('proj'):
            ysend[0, top] = jnp.dot(ofull[away, top, near], wo[0, near, :], preferred_element_type=F32)
        with jax.named_scope('wait_o_away'):
            wait_o(0, 1)
        with jax.named_scope('proj'):
            ysend[0, top] += jnp.dot(ofull[away, top, far], wo[0, far, :], preferred_element_type=F32)
        y_copy(0, 0).start()

        @pl.loop(1, NOUT)
        def _(n):
            with jax.named_scope('proj'):
                ysend[n, top] = jnp.dot(ofull[away, top], wo[n], preferred_element_type=F32)
            y_copy(n, 0).start()

    def project_rest():
        with jax.named_scope('wait_o_away'):
            wait_o(1, 0)
            wait_o(1, 1)

        @pl.loop(0, NOUT)
        def _(n):
            with jax.named_scope('proj'):
                ysend[n, bottom] = jnp.dot(ofull[away, bottom], wo[n], preferred_element_type=F32)
            y_copy(n, 1).start()

    @pl.loop(0, 4)
    def _(stage):
        @pl.when(stage == 2 * tp)
        def _():
            rest_of_rows()

        @pl.when((stage == 1 - tp) | (stage == 3))
        def _():
            attend_blocks((stage < 2) == (tp == 0))

            @pl.when((tp == 1) & (stage == 0))
            def _():
                for k in range(LATE, NK):
                    own(k, 1).start()

        @pl.when(stage == 2 - tp)
        def _():
            project_away()

            @pl.when((tp == 1) | (c == 0))
            def _():
                project_rest()

    with jax.named_scope('wait_o_home'):
        drain(osend.at[pl.ds(0, 3)], o_recv_sem.at[4])

    @pl.when((tp == 0) & (c == 1))
    def _():
        project_rest()

    def kept(n):
        return acc.at[pl.ds(pl.multiple_of(n % 6 * BLK, BLK), BLK), pl.ds(pl.multiple_of(n // 6 * NC, NC), NC)]

    @pl.loop(0, NOUT)
    def _(n):
        kept(n)[...] = jnp.dot(ofull[home], wo[n], preferred_element_type=F32)

    @pl.loop(0, NOUT)
    def _(n):
        with jax.named_scope('wait_y'):
            drain(yrecv.at[n], y_recv_sem.at[n])
        y_ref[:, pl.ds(pl.multiple_of(n * NC, NC), NC)] = (kept(n)[...] + yrecv[n]).astype(BF16)

    drain(xs.at[:, pl.ds(0, 6 * BLK), :], x_send)
    for t in range(2):
        for xx in range(2):
            over_x = DIAG_X * BLK if t else (NK - LATE) * BLK + (1 - xx) * HALF
            over_y = LATE * BLK - xx * HALF if t else (NK - DIAG_X) * BLK

            @pl.when((tp == t) & (x == xx))
            def _():
                drain(xs.at[pl.ds(0, 2), pl.ds(0, (over_x + over_y) // 2), :], dg_send)
    drain(osend.at[pl.ds(0, 6)], o_send_sem)
    drain(ysend, y_send_sem)


def solution(mesh):
    def device_fn(x_loc, w_q, w_k, w_v, w_o):
        dma = pltpu.SemaphoreType.DMA
        heads_major = [jnp.transpose(t, (1, 0, 2)) for t in (w_q, w_k, w_v)]
        return pl.pallas_call(
            kernel,
            name='attention_layer',
            out_shape=pltpu.VMEM((BLK, D), BF16),
            in_specs=[pl.BlockSpec(memory_space=pl.ANY)] * 5,
            out_specs=pl.BlockSpec(memory_space=pltpu.VMEM),
            scratch_shapes=[
                pltpu.VMEM((NK, 512, KC), BF16),
                pltpu.VMEM((D, NQKV), BF16),
                pltpu.VMEM((NOUT, 20 * E, NC), BF16),
                pltpu.VMEM((512, NQKV), BF16),
                pltpu.VMEM((384, NQKV), F32),
                pltpu.VMEM((8, BLK, HE), BF16),
                pltpu.VMEM((2, BLK, 20 * E), BF16),
                pltpu.VMEM((NOUT, BLK, NC), F32),
                pltpu.VMEM((NOUT, BLK, NC), F32),
                dma, dma, dma, dma, dma((3, NK)), dma((2 * NK + LATE,)), dma,
                dma, dma((5,)),
                dma, dma((NOUT,)),
            ],
            compiler_params=pltpu.CompilerParams(collective_id=0, has_side_effects=True, vmem_limit_bytes=64 * 1000 * 1000),
        )(x_loc, *heads_major, w_o.reshape(20 * E, D))

    seq_spec = P(('dp', 'cp', 'tp'), None)
    head_spec = P(None, 'tp', None)
    return jax.shard_map(device_fn, mesh=mesh, in_specs=(seq_spec, head_spec, head_spec, head_spec, P('tp', None, None)), out_specs=seq_spec, check_vma=False)
```

```python
import functools

import jax
import jax.numpy as jnp
from jax import lax
from jax.experimental import pallas as pl
from jax.experimental.pallas import tpu as pltpu
from jax.sharding import PartitionSpec as P

BF16, F32 = jnp.bfloat16, jnp.float32
NEG_BIG = -1e30
D = 5120
E = 128
HEADS = 5
HE = HEADS * E
NQKV = 3 * HE
BLK = 64
HALF = BLK // 2
NK = 10
KC = D // NK
LATE = NK // 2
DIAG_X = 7
NOUT = 10
NC = D // NOUT
MESH = pl.DeviceIdType.MESH


def remote(src, dst, send_sem, recv_sem, dev):
    return pltpu.make_async_remote_copy(src_ref=src, dst_ref=dst, send_sem=send_sem, recv_sem=recv_sem, device_id=dev, device_id_type=MESH)


def drain(ref, sem):
    pltpu.make_async_copy(ref, ref, sem).wait()


def kernel(x_hbm, wq_hbm, wk_hbm, wv_hbm, wo_hbm, y_ref, xs, w, wo, qkv, acc, osend, ofull, ysend, yrecv,
           in_sem, in_sem2, x_send, sib_recv, direct_recv, fwd_recv, dg_send, o_send_sem, o_recv_sem,
           y_send_sem, y_recv_sem):
    cp, tp = lax.axis_index('cp'), lax.axis_index('tp')
    x, c = cp // 2, cp % 2
    sib = {'cp': 2 * x + 1 - c, 'tp': tp}
    xn = {'cp': 2 * (1 - x) + c, 'tp': tp}
    xo = {'cp': 2 * (1 - x) + 1 - c, 'tp': tp}
    yn = {'cp': cp, 'tp': 1 - tp}

    def rows(group, core):
        return pl.ds(pl.multiple_of(group * 128 + core * BLK, BLK), BLK)

    def x_in(k):
        return pltpu.make_async_copy(x_hbm.at[:, pl.ds(k * KC, KC)], xs.at[k, rows(0, c), :], in_sem if k < 2 else in_sem2)

    def w_in(j):
        src = (wq_hbm, wk_hbm, wv_hbm)[j // HEADS].at[cp * HEADS + j % HEADS]
        return pltpu.make_async_copy(src, w.at[:, pl.ds(j * E, E)], in_sem)

    def wo_in(n):
        return pltpu.make_async_copy(wo_hbm.at[:, pl.ds(n * NC, NC)], wo.at[n], in_sem)

    for k in range(NK):
        x_in(k).start()
    barrier = pltpu.get_barrier_semaphore()
    for dev in (sib, xn, xo, yn):
        pl.semaphore_signal(barrier, inc=1, device_id=dev, device_id_type=MESH)
    drain(xs.at[pl.ds(0, 2), rows(0, c), :], in_sem)
    with jax.named_scope('barrier'):
        pl.semaphore_wait(barrier, 4)

    def group_of(kind, t):
        return (1, 2 + t, 3 - t, 0)[kind]

    def own(k, kind):
        dev, t = ((yn, 1 - tp), (xn, tp), None, (sib, tp))[kind]
        return remote(xs.at[k, rows(0, c), :], xs.at[k, rows(group_of(kind, t), c), :], x_send, sib_recv if kind == 3 else direct_recv.at[kind, k], dev)

    def diag(k, over_y):
        dev, src, t = (yn, group_of(1, tp), 1 - tp) if over_y else (xn, group_of(0, tp), tp)
        return remote(xs.at[k, rows(src, c), :], xs.at[k, rows(group_of(2, t), c), :], dg_send, direct_recv.at[2, k], dev)

    def half_diag(over_y):
        dev, src, t = (yn, group_of(1, tp), 1 - tp) if over_y else (xn, group_of(0, tp), tp)
        k, first = LATE - 1, 0 if over_y else HALF
        return remote(xs.at[k, pl.ds(pl.multiple_of(src * 128 + c * BLK + first, HALF), HALF), :],
                      xs.at[k, pl.ds(pl.multiple_of(group_of(2, t) * 128 + c * BLK + first, HALF), HALF), :],
                      dg_send, direct_recv.at[2, k], dev)

    def fwd(k, kind):
        sl = rows(group_of(kind, tp), c)
        second = NK + k % LATE
        sem = (k, jnp.where(tp == 0, k, second), jnp.where(tp == 0, second, NK + LATE + k))[kind]
        return remote(xs.at[k, sl, :], xs.at[k, sl, :], x_send, fwd_recv.at[sem], sib)

    def direct_wait(k, kind):
        drain(xs.at[k, rows(group_of(kind, tp), c), :], direct_recv.at[kind, k])

    def sends_diag_x(k):
        return jnp.where(tp == 0, k >= LATE, k < DIAG_X)

    def sends_half_x(k):
        return (tp == 0) & (x == 0) & (k == LATE - 1)

    def sends_diag_y(k):
        return jnp.where(tp == 0, k >= DIAG_X, k < LATE - x)

    def sends_half_y(k):
        return (tp == 1) & (x == 1) & (k == LATE - 1)

    def handle(k, kind):
        direct_wait(k, kind)
        fwd(k, kind).start()
        if kind == 0:
            @pl.when(sends_diag_x(k))
            def _():
                diag(k, False).start()

            @pl.when(sends_half_x(k))
            def _():
                half_diag(False).start()
        if kind == 1:
            @pl.when(sends_diag_y(k))
            def _():
                diag(k, True).start()

            @pl.when(sends_half_y(k))
            def _():
                half_diag(True).start()

    for k in range(NK):
        if k == 2:
            drain(xs.at[pl.ds(2, NK - 2), rows(0, c), :], in_sem2)
            for j in range(3 * HEADS):
                w_in(j).start()
        if k < LATE:
            own(k, 1).start()
        else:
            @pl.when(tp == 0)
            def _():
                own(k, 1).start()
        own(k, 0).start()
        own(k, 3).start()

    acc[...] = jnp.zeros_like(acc)

    def nat(xx, core, t):
        b = 2 * xx + core
        return jnp.where(t == 0, b, 7 - b) * BLK

    nat_of = [nat(x, 0, tp), nat(x, 1, tp), nat(x, 0, 1 - tp), nat(x, 1, 1 - tp),
              nat(1 - x, 0, 0), nat(1 - x, 1, 0), nat(1 - x, 0, 1), nat(1 - x, 1, 1)]

    def put_qkv(slot, col, n, val):
        qkv[pl.ds(pl.multiple_of(nat_of[slot], BLK), BLK), pl.ds(col, n)] = val.astype(BF16)

    NSTEPS = ((0, 512), (512, 512), (1024, 512), (1536, 384))

    def own_chip():
        with jax.named_scope('wait_sib'):
            drain(xs.at[:, rows(0, c), :], sib_recv)
        with jax.named_scope('wait_w'):
            drain(w, in_sem)
        for n in range(NOUT):
            wo_in(n).start()
        for col, n in NSTEPS:
            val = jnp.dot(xs[0, 0:128, :], w[0:KC, col:col + n], preferred_element_type=F32)
            for k in range(1, NK):
                val += jnp.dot(xs[k, 0:128, :], w[k * KC:(k + 1) * KC, col:col + n], preferred_element_type=F32)
            put_qkv(0, col, n, val[:BLK])
            put_qkv(1, col, n, val[BLK:])

    def accumulate(chunks, row, m, arow):
        for col, n in NSTEPS:
            val = acc[arow:arow + m, col:col + n]
            for k in chunks:
                val += jnp.dot(xs[k, row:row + m, :], w[pl.ds(pl.multiple_of(k * KC, KC), KC), col:col + n], preferred_element_type=F32)
            acc[arow:arow + m, col:col + n] = val

    def diag_order(m):
        return jnp.where(m < 5, m, jnp.where(m % 2 == 1, 7 + (m - 5) // 2, 5 + (m - 6) // 2))

    def wait_fwd2(j):
        with jax.named_scope('w_fwd2'):
            drain(xs.at[0, pl.ds(384, 128), :], fwd_recv.at[NK + j])

    def pair(j):
        wait_fwd2(j)
        with jax.named_scope('acc_b'):
            accumulate((j, j + LATE), 384, 128, 256)

    @pl.loop(0, NK + LATE)
    def _(i):
        @pl.when(i < NK)
        def _():
            with jax.named_scope('h_y'):
                handle(i, 0)

        @pl.when(i < jnp.where(tp == 0, NK, LATE))
        def _():
            with jax.named_scope('h_x'):
                handle(i, 1)

        @pl.when((tp == 0) & (i >= NK) & (i < NK + LATE))
        def _():
            with jax.named_scope('h_d2'):
                handle(i - NK, 2)
                handle(i - NK + LATE, 2)

        @pl.when((tp == 1) & (i >= 5) & (i < NK + 3))
        def _():
            with jax.named_scope('h_d'):
                handle(diag_order(jnp.where(i == NK + 2, 8, i - 5)), 2)

                @pl.when(i > NK)
                def _():
                    handle(diag_order(jnp.where(i == NK + 2, 9, 7)), 2)

        @pl.when(i == 2)
        def _():
            own_chip()

        @pl.when((i >= 2) & (i < NK + 2))
        def _():
            k = i - 2

            @pl.when(tp == 0)
            def _():
                with jax.named_scope('w_fwd'):
                    drain(xs.at[k, pl.ds(128, 128), :], fwd_recv.at[k])
                with jax.named_scope('acc_a'):
                    accumulate((k,), 128, 256, 0)

            @pl.when(tp == 1)
            def _():
                with jax.named_scope('w_fwd'):
                    drain(xs.at[k, pl.ds(128, BLK), :], fwd_recv.at[k])
                with jax.named_scope('acc_y'):
                    accumulate((k,), 128, 128, 0)

        def wait_d(k):
            with jax.named_scope('w_fwd'):
                drain(xs.at[k, pl.ds(256, BLK), :], fwd_recv.at[NK + LATE + k])

        @pl.when((tp == 1) & (i >= 6) & (i < NK + 2))
        def _():
            k = diag_order(i - 6)
            wait_d(k)
            with jax.named_scope('acc_d'):
                accumulate((k,), 256, 128, 128)

        @pl.when((tp == 1) & (i >= NK + 2) & (i < NK + 4))
        def _():
            k, k2 = i - NK + 3, i - NK + 6
            wait_d(k)
            wait_d(k2)
            with jax.named_scope('acc_d'):
                accumulate((k, k2), 256, 128, 128)

        @pl.when((tp == 0) & (i > NK) & (i < NK + LATE))
        def _():
            pair(i - NK - 1)

    for col, n in NSTEPS:
        for s in range(4):
            put_qkv(2 + s, col, n, acc[s * BLK:(s + 1) * BLK, col:col + n])

    def rest_of_rows():
        @pl.when(tp == 1)
        def _():
            @pl.loop(0, LATE)
            def _(j):
                with jax.named_scope('h_x2'):
                    handle(j + LATE, 1)

                @pl.when(j > 0)
                def _():
                    pair(j - 1)

        wait_fwd2(LATE - 1)
        with jax.named_scope('acc_b'):
            for col, n in NSTEPS:
                val = acc[256:384, col:col + n]
                for k in (LATE - 1, NK - 1):
                    val += jnp.dot(xs[k, 384:512, :], w[k * KC:(k + 1) * KC, col:col + n], preferred_element_type=F32)
                for s in range(2):
                    put_qkv(6 + s, col, n, val[s * BLK:(s + 1) * BLK])

    inv_sqrt = E ** -0.5

    def o_copy(b, half, dev_cp):
        lohi, part = b // 4, pl.ds(half * HALF, HALF)
        return remote(osend.at[b, part], ofull.at[lohi, part, pl.ds(pl.multiple_of(cp * HE, E), HE)],
                      o_send_sem, o_recv_sem.at[jnp.where(lohi == tp, 4, 2 * half + jnp.where(x == dev_cp // 2, 0, 1))], {'cp': dev_cp, 'tp': tp})

    def attend(b):
        length = 128 * (b // 2 + 1)
        ri = lax.broadcasted_iota(jnp.int32, (BLK, 128), 0) + BLK * (b % 2)
        ci = lax.broadcasted_iota(jnp.int32, (BLK, 128), 1)
        mask = ci <= ri
        heads = range(HEADS)
        q = [qkv[b * BLK:(b + 1) * BLK, h * E:(h + 1) * E] for h in heads]
        kk = [qkv[0:length, HE + h * E:HE + (h + 1) * E] for h in heads]
        v = [qkv[0:length, 2 * HE + h * E:2 * HE + (h + 1) * E] for h in heads]
        s = [lax.dot_general(q[h], kk[h], (((1,), (1,)), ((), ())), preferred_element_type=F32) * inv_sqrt for h in heads]
        last = [jnp.where(mask, s[h][:, length - 128:], NEG_BIG) for h in heads]
        s = [last[h] if length == 128 else jnp.concatenate([s[h][:, :length - 128], last[h]], axis=1) for h in heads]
        m = [jnp.max(s[h], axis=-1, keepdims=True) for h in heads]
        p = [jnp.exp(s[h] - m[h]) for h in heads]
        l = [jnp.sum(p[h], axis=-1, keepdims=True) for h in heads]
        o = [jnp.dot(p[h].astype(BF16), v[h], preferred_element_type=F32) for h in heads]
        for h in heads:
            osend[b, :, h * E:(h + 1) * E] = (o[h] / l[h]).astype(BF16)
    def send_o(b, half):
        r = jnp.where(b < 4, b, 7 - b)

        @pl.when(cp == r)
        def _():
            part = pl.ds(half * HALF, HALF)
            ofull[b // 4, part, pl.ds(pl.multiple_of(cp * HE, E), HE)] = osend[b, part]

        @pl.when(cp != r)
        def _():
            o_copy(b, half, r).start()

    def wait_o(half, far):
        drain(osend.at[pl.ds(0, 1 + far), pl.ds(0, HALF)], o_recv_sem.at[2 * half + far])

    def attend_blocks(hi):
        def block_at(step):
            first, odd = step < 2, step % 2
            pair = jnp.where(hi, jnp.where(first, 2 + x, 3 - x), jnp.where(first, 1 - x, x))
            return 2 * pair + jnp.where(hi, odd, 1 - odd)

        @pl.loop(0, 4)
        def _(step):
            block = block_at(step)
            for b in range(8):
                @pl.when(block == b)
                def _():
                    with jax.named_scope(f'attend{b}'):
                        attend(b)

            for at, sends in enumerate((((0, 0),), ((0, 1),), ((1, 0), (1, 1), (2, 0), (2, 1)), ((3, 0), (3, 1)))):
                @pl.when(step == at)
                def _():
                    for which, half in sends:
                        send_o(block_at(which), half)

    away, home = 1 - tp, tp

    def y_copy(n, half):
        part = pl.ds(half * HALF, HALF)
        return remote(ysend.at[n, part], yrecv.at[n, part], y_send_sem, y_recv_sem.at[n], yn)

    top, bottom = slice(0, HALF), slice(HALF, BLK)

    def project_away():
        near = pl.ds(pl.multiple_of(2 * x * HE, E), 2 * HE)
        far = pl.ds(pl.multiple_of(2 * (1 - x) * HE, E), 2 * HE)
        drain(wo, in_sem)
        with jax.named_scope('wait_o_away'):
            wait_o(0, 0)
        with jax.named_scope('proj'):
            ysend[0, top] = jnp.dot(ofull[away, top, near], wo[0, near, :], preferred_element_type=F32)
        with jax.named_scope('wait_o_away'):
            wait_o(0, 1)
        with jax.named_scope('proj'):
            ysend[0, top] += jnp.dot(ofull[away, top, far], wo[0, far, :], preferred_element_type=F32)
        y_copy(0, 0).start()

        @pl.loop(1, NOUT)
        def _(n):
            with jax.named_scope('proj'):
                ysend[n, top] = jnp.dot(ofull[away, top], wo[n], preferred_element_type=F32)
            y_copy(n, 0).start()

    def project_rest():
        with jax.named_scope('wait_o_away'):
            wait_o(1, 0)
            wait_o(1, 1)

        @pl.loop(0, NOUT)
        def _(n):
            with jax.named_scope('proj'):
                ysend[n, bottom] = jnp.dot(ofull[away, bottom], wo[n], preferred_element_type=F32)
            y_copy(n, 1).start()

    @pl.loop(0, 4)
    def _(stage):
        @pl.when(stage == 2 * tp)
        def _():
            rest_of_rows()

        @pl.when((stage == 1 - tp) | (stage == 3))
        def _():
            attend_blocks((stage < 2) == (tp == 0))

            @pl.when((tp == 1) & (stage == 0))
            def _():
                for k in range(LATE, NK):
                    own(k, 1).start()

        @pl.when(stage == 2 - tp)
        def _():
            project_away()

            @pl.when(tp == 1)
            def _():
                project_rest()

    @pl.when((tp == 0) & (c == 0))
    def _():
        project_rest()

    with jax.named_scope('wait_o_home'):
        drain(osend.at[pl.ds(0, 3)], o_recv_sem.at[4])

    def kept(n):
        return acc.at[pl.ds(pl.multiple_of(n % 6 * BLK, BLK), BLK), pl.ds(pl.multiple_of(n // 6 * NC, NC), NC)]

    @pl.loop(0, NOUT)
    def _(n):
        kept(n)[...] = jnp.dot(ofull[home], wo[n], preferred_element_type=F32)

    @pl.when((tp == 0) & (c == 1))
    def _():
        project_rest()

    @pl.loop(0, NOUT)
    def _(n):
        with jax.named_scope('wait_y'):
            drain(yrecv.at[n], y_recv_sem.at[n])
        y_ref[:, pl.ds(pl.multiple_of(n * NC, NC), NC)] = (kept(n)[...] + yrecv[n]).astype(BF16)

    drain(xs.at[:, pl.ds(0, 6 * BLK), :], x_send)
    for t in range(2):
        for xx in range(2):
            over_x = DIAG_X * BLK if t else (NK - LATE) * BLK + (1 - xx) * HALF
            over_y = LATE * BLK - xx * HALF if t else (NK - DIAG_X) * BLK

            @pl.when((tp == t) & (x == xx))
            def _():
                drain(xs.at[pl.ds(0, 2), pl.ds(0, (over_x + over_y) // 2), :], dg_send)
    drain(osend.at[pl.ds(0, 6)], o_send_sem)
    drain(ysend, y_send_sem)


def solution(mesh):
    def device_fn(x_loc, w_q, w_k, w_v, w_o):
        dma = pltpu.SemaphoreType.DMA
        heads_major = [jnp.transpose(t, (1, 0, 2)) for t in (w_q, w_k, w_v)]
        return pl.pallas_call(
            kernel,
            name='attention_layer',
            out_shape=pltpu.VMEM((BLK, D), BF16),
            in_specs=[pl.BlockSpec(memory_space=pl.ANY)] * 5,
            out_specs=pl.BlockSpec(memory_space=pltpu.VMEM),
            scratch_shapes=[
                pltpu.VMEM((NK, 512, KC), BF16),
                pltpu.VMEM((D, NQKV), BF16),
                pltpu.VMEM((NOUT, 20 * E, NC), BF16),
                pltpu.VMEM((512, NQKV), BF16),
                pltpu.VMEM((384, NQKV), F32),
                pltpu.VMEM((8, BLK, HE), BF16),
                pltpu.VMEM((2, BLK, 20 * E), BF16),
                pltpu.VMEM((NOUT, BLK, NC), F32),
                pltpu.VMEM((NOUT, BLK, NC), F32),
                dma, dma, dma, dma, dma((3, NK)), dma((2 * NK + LATE,)), dma,
                dma, dma((5,)),
                dma, dma((NOUT,)),
            ],
            compiler_params=pltpu.CompilerParams(collective_id=0, has_side_effects=True, vmem_limit_bytes=64 * 1000 * 1000),
        )(x_loc, *heads_major, w_o.reshape(20 * E, D))

    seq_spec = P(('dp', 'cp', 'tp'), None)
    head_spec = P(None, 'tp', None)
    return jax.shard_map(device_fn, mesh=mesh, in_specs=(seq_spec, head_spec, head_spec, head_spec, P('tp', None, None)), out_specs=seq_spec, check_vma=False)
```

```python
import functools

import jax
import jax.numpy as jnp
from jax import lax
from jax.experimental import pallas as pl
from jax.experimental.pallas import tpu as pltpu
from jax.sharding import PartitionSpec as P

BF16, F32 = jnp.bfloat16, jnp.float32
NEG_BIG = -1e30
D = 5120
E = 128
HEADS = 5
HE = HEADS * E
NQKV = 3 * HE
BLK = 64
HALF = BLK // 2
NK = 10
KC = D // NK
LATE = NK // 2
DIAG_X = 7
NOUT = 10
NC = D // NOUT
MESH = pl.DeviceIdType.MESH


def remote(src, dst, send_sem, recv_sem, dev):
    return pltpu.make_async_remote_copy(src_ref=src, dst_ref=dst, send_sem=send_sem, recv_sem=recv_sem, device_id=dev, device_id_type=MESH)


def drain(ref, sem):
    pltpu.make_async_copy(ref, ref, sem).wait()


def kernel(x_hbm, wq_hbm, wk_hbm, wv_hbm, wo_hbm, y_ref, xs, w, wo, qkv, acc, osend, ofull, ysend, yrecv,
           in_sem, in_sem2, x_send, sib_recv, direct_recv, fwd_recv, dg_send, o_send_sem, o_recv_sem,
           y_send_sem, y_recv_sem):
    cp, tp = lax.axis_index('cp'), lax.axis_index('tp')
    x, c = cp // 2, cp % 2
    sib = {'cp': 2 * x + 1 - c, 'tp': tp}
    xn = {'cp': 2 * (1 - x) + c, 'tp': tp}
    xo = {'cp': 2 * (1 - x) + 1 - c, 'tp': tp}
    yn = {'cp': cp, 'tp': 1 - tp}

    def rows(group, core):
        return pl.ds(pl.multiple_of(group * 128 + core * BLK, BLK), BLK)

    def x_in(k):
        return pltpu.make_async_copy(x_hbm.at[:, pl.ds(k * KC, KC)], xs.at[k, rows(0, c), :], in_sem if k < 2 else in_sem2)

    def w_in(j):
        src = (wq_hbm, wk_hbm, wv_hbm)[j // HEADS].at[cp * HEADS + j % HEADS]
        return pltpu.make_async_copy(src, w.at[:, pl.ds(j * E, E)], in_sem)

    def wo_in(n):
        return pltpu.make_async_copy(wo_hbm.at[:, pl.ds(n * NC, NC)], wo.at[n], in_sem)

    for k in range(NK):
        x_in(k).start()
    barrier = pltpu.get_barrier_semaphore()
    for dev in (sib, xn, xo, yn):
        pl.semaphore_signal(barrier, inc=1, device_id=dev, device_id_type=MESH)
    drain(xs.at[pl.ds(0, 2), rows(0, c), :], in_sem)
    with jax.named_scope('barrier'):
        pl.semaphore_wait(barrier, 4)

    def group_of(kind, t):
        return (1, 2 + t, 3 - t, 0)[kind]

    def own(k, kind):
        dev, t = ((yn, 1 - tp), (xn, tp), None, (sib, tp))[kind]
        return remote(xs.at[k, rows(0, c), :], xs.at[k, rows(group_of(kind, t), c), :], x_send, sib_recv if kind == 3 else direct_recv.at[kind, k], dev)

    def diag(k, over_y):
        dev, src, t = (yn, group_of(1, tp), 1 - tp) if over_y else (xn, group_of(0, tp), tp)
        return remote(xs.at[k, rows(src, c), :], xs.at[k, rows(group_of(2, t), c), :], dg_send, direct_recv.at[2, k], dev)

    def half_diag(over_y):
        dev, src, t = (yn, group_of(1, tp), 1 - tp) if over_y else (xn, group_of(0, tp), tp)
        k, first = LATE - 1, 0 if over_y else HALF
        return remote(xs.at[k, pl.ds(pl.multiple_of(src * 128 + c * BLK + first, HALF), HALF), :],
                      xs.at[k, pl.ds(pl.multiple_of(group_of(2, t) * 128 + c * BLK + first, HALF), HALF), :],
                      dg_send, direct_recv.at[2, k], dev)

    def fwd(k, kind):
        sl = rows(group_of(kind, tp), c)
        second = NK + k % LATE
        sem = (k, jnp.where(tp == 0, k, second), jnp.where(tp == 0, second, NK + LATE + k))[kind]
        return remote(xs.at[k, sl, :], xs.at[k, sl, :], x_send, fwd_recv.at[sem], sib)

    def direct_wait(k, kind):
        drain(xs.at[k, rows(group_of(kind, tp), c), :], direct_recv.at[kind, k])

    def sends_diag_x(k):
        return jnp.where(tp == 0, k >= LATE, k < DIAG_X)

    def sends_half_x(k):
        return (tp == 0) & (x == 0) & (k == LATE - 1)

    def sends_diag_y(k):
        return jnp.where(tp == 0, k >= DIAG_X, k < LATE - x)

    def sends_half_y(k):
        return (tp == 1) & (x == 1) & (k == LATE - 1)

    def handle(k, kind):
        direct_wait(k, kind)
        fwd(k, kind).start()
        if kind == 0:
            @pl.when(sends_diag_x(k))
            def _():
                diag(k, False).start()

            @pl.when(sends_half_x(k))
            def _():
                half_diag(False).start()
        if kind == 1:
            @pl.when(sends_diag_y(k))
            def _():
                diag(k, True).start()

            @pl.when(sends_half_y(k))
            def _():
                half_diag(True).start()

    for k in range(NK):
        if k == 2:
            drain(xs.at[pl.ds(2, NK - 2), rows(0, c), :], in_sem2)
            for j in range(3 * HEADS):
                w_in(j).start()
        if k < LATE:
            own(k, 1).start()
        else:
            @pl.when(tp == 0)
            def _():
                own(k, 1).start()
        own(k, 0).start()
        own(k, 3).start()

    acc[...] = jnp.zeros_like(acc)

    def nat(xx, core, t):
        b = 2 * xx + core
        return jnp.where(t == 0, b, 7 - b) * BLK

    nat_of = [nat(x, 0, tp), nat(x, 1, tp), nat(x, 0, 1 - tp), nat(x, 1, 1 - tp),
              nat(1 - x, 0, 0), nat(1 - x, 1, 0), nat(1 - x, 0, 1), nat(1 - x, 1, 1)]

    def put_qkv(slot, col, n, val):
        qkv[pl.ds(pl.multiple_of(nat_of[slot], BLK), BLK), pl.ds(col, n)] = val.astype(BF16)

    NSTEPS = ((0, 512), (512, 512), (1024, 512), (1536, 384))

    def own_chip():
        with jax.named_scope('wait_sib'):
            drain(xs.at[:, rows(0, c), :], sib_recv)
        with jax.named_scope('wait_w'):
            drain(w, in_sem)
        for n in range(NOUT):
            wo_in(n).start()
        for col, n in NSTEPS:
            val = jnp.dot(xs[0, 0:128, :], w[0:KC, col:col + n], preferred_element_type=F32)
            for k in range(1, NK):
                val += jnp.dot(xs[k, 0:128, :], w[k * KC:(k + 1) * KC, col:col + n], preferred_element_type=F32)
            put_qkv(0, col, n, val[:BLK])
            put_qkv(1, col, n, val[BLK:])

    def accumulate(chunks, row, m, arow):
        for col, n in NSTEPS:
            val = acc[arow:arow + m, col:col + n]
            for k in chunks:
                val += jnp.dot(xs[k, row:row + m, :], w[pl.ds(pl.multiple_of(k * KC, KC), KC), col:col + n], preferred_element_type=F32)
            acc[arow:arow + m, col:col + n] = val

    def diag_order(m):
        return jnp.where(m < 5, m, jnp.where(m % 2 == 1, 7 + (m - 5) // 2, 5 + (m - 6) // 2))

    def wait_fwd2(j):
        with jax.named_scope('w_fwd2'):
            drain(xs.at[0, pl.ds(384, 128), :], fwd_recv.at[NK + j])

    def pair(j):
        wait_fwd2(j)
        with jax.named_scope('acc_b'):
            accumulate((j, j + LATE), 384, 128, 256)

    @pl.loop(0, NK + LATE)
    def _(i):
        @pl.when(i < NK)
        def _():
            with jax.named_scope('h_y'):
                handle(i, 0)

        @pl.when(i < jnp.where(tp == 0, NK, LATE))
        def _():
            with jax.named_scope('h_x'):
                handle(i, 1)

        @pl.when((tp == 0) & (i >= NK) & (i < NK + LATE))
        def _():
            with jax.named_scope('h_d2'):
                handle(i - NK, 2)
                handle(i - NK + LATE, 2)

        @pl.when((tp == 1) & (i >= 5) & (i < NK + 3))
        def _():
            with jax.named_scope('h_d'):
                handle(diag_order(jnp.where(i == NK + 2, 8, i - 5)), 2)

                @pl.when(i > NK)
                def _():
                    handle(diag_order(jnp.where(i == NK + 2, 9, 7)), 2)

        @pl.when(i == 2)
        def _():
            own_chip()

        @pl.when((i >= 2) & (i < NK + 2))
        def _():
            k = i - 2

            @pl.when(tp == 0)
            def _():
                with jax.named_scope('w_fwd'):
                    drain(xs.at[k, pl.ds(128, 128), :], fwd_recv.at[k])
                with jax.named_scope('acc_a'):
                    accumulate((k,), 128, 256, 0)

            @pl.when(tp == 1)
            def _():
                with jax.named_scope('w_fwd'):
                    drain(xs.at[k, pl.ds(128, BLK), :], fwd_recv.at[k])
                with jax.named_scope('acc_y'):
                    accumulate((k,), 128, 128, 0)

        def wait_d(k):
            with jax.named_scope('w_fwd'):
                drain(xs.at[k, pl.ds(256, BLK), :], fwd_recv.at[NK + LATE + k])

        @pl.when((tp == 1) & (i >= 6) & (i < NK + 2))
        def _():
            k = diag_order(i - 6)
            wait_d(k)
            with jax.named_scope('acc_d'):
                accumulate((k,), 256, 128, 128)

        @pl.when((tp == 1) & (i >= NK + 2) & (i < NK + 4))
        def _():
            k, k2 = i - NK + 3, i - NK + 6
            wait_d(k)
            wait_d(k2)
            with jax.named_scope('acc_d'):
                accumulate((k, k2), 256, 128, 128)

        @pl.when((tp == 0) & (i > NK) & (i < NK + LATE))
        def _():
            pair(i - NK - 1)

    for col, n in NSTEPS:
        for s in range(4):
            put_qkv(2 + s, col, n, acc[s * BLK:(s + 1) * BLK, col:col + n])

    def rest_of_rows():
        @pl.when(tp == 1)
        def _():
            @pl.loop(0, LATE)
            def _(j):
                with jax.named_scope('h_x2'):
                    handle(j + LATE, 1)

                @pl.when(j > 0)
                def _():
                    pair(j - 1)

        wait_fwd2(LATE - 1)
        with jax.named_scope('acc_b'):
            for col, n in NSTEPS:
                val = acc[256:384, col:col + n]
                for k in (LATE - 1, NK - 1):
                    val += jnp.dot(xs[k, 384:512, :], w[k * KC:(k + 1) * KC, col:col + n], preferred_element_type=F32)
                for s in range(2):
                    put_qkv(6 + s, col, n, val[s * BLK:(s + 1) * BLK])

    inv_sqrt = E ** -0.5

    def o_copy(b, half, dev_cp):
        lohi, part = b // 4, pl.ds(half * HALF, HALF)
        return remote(osend.at[b, part], ofull.at[lohi, part, pl.ds(pl.multiple_of(cp * HE, E), HE)],
                      o_send_sem, o_recv_sem.at[jnp.where(lohi == tp, 4, 2 * half + jnp.where(x == dev_cp // 2, 0, 1))], {'cp': dev_cp, 'tp': tp})

    def attend(b):
        length = 128 * (b // 2 + 1)
        ri = lax.broadcasted_iota(jnp.int32, (BLK, 128), 0) + BLK * (b % 2)
        ci = lax.broadcasted_iota(jnp.int32, (BLK, 128), 1)
        mask = ci <= ri
        heads = range(HEADS)
        q = [qkv[b * BLK:(b + 1) * BLK, h * E:(h + 1) * E] for h in heads]
        kk = [qkv[0:length, HE + h * E:HE + (h + 1) * E] for h in heads]
        v = [qkv[0:length, 2 * HE + h * E:2 * HE + (h + 1) * E] for h in heads]
        s = [lax.dot_general(q[h], kk[h], (((1,), (1,)), ((), ())), preferred_element_type=F32) * inv_sqrt for h in heads]
        last = [jnp.where(mask, s[h][:, length - 128:], NEG_BIG) for h in heads]
        s = [last[h] if length == 128 else jnp.concatenate([s[h][:, :length - 128], last[h]], axis=1) for h in heads]
        m = [jnp.max(s[h], axis=-1, keepdims=True) for h in heads]
        p = [jnp.exp(s[h] - m[h]) for h in heads]
        l = [jnp.sum(p[h], axis=-1, keepdims=True) for h in heads]
        o = [jnp.dot(p[h].astype(BF16), v[h], preferred_element_type=F32) for h in heads]
        for h in heads:
            osend[b, :, h * E:(h + 1) * E] = (o[h] / l[h]).astype(BF16)
    def send_o(b, half):
        r = jnp.where(b < 4, b, 7 - b)

        @pl.when(cp == r)
        def _():
            part = pl.ds(half * HALF, HALF)
            ofull[b // 4, part, pl.ds(pl.multiple_of(cp * HE, E), HE)] = osend[b, part]

        @pl.when(cp != r)
        def _():
            o_copy(b, half, r).start()

    def wait_o(half, far):
        drain(osend.at[pl.ds(0, 1 + far), pl.ds(0, HALF)], o_recv_sem.at[2 * half + far])

    def attend_blocks(hi):
        def block_at(step):
            first, odd = step < 2, step % 2
            pair = jnp.where(hi, jnp.where(first, 2 + x, 3 - x), jnp.where(first, 1 - x, x))
            return 2 * pair + jnp.where(hi, odd, 1 - odd)

        @pl.loop(0, 4)
        def _(step):
            block = block_at(step)
            for b in range(8):
                @pl.when(block == b)
                def _():
                    with jax.named_scope(f'attend{b}'):
                        attend(b)

            for at, sends in enumerate((((0, 0),), ((0, 1),), ((1, 0), (1, 1), (2, 0), (2, 1)), ((3, 0), (3, 1)))):
                @pl.when(step == at)
                def _():
                    for which, half in sends:
                        send_o(block_at(which), half)

    away, home = 1 - tp, tp

    def y_copy(n, half):
        part = pl.ds(half * HALF, HALF)
        return remote(ysend.at[n, part], yrecv.at[n, part], y_send_sem, y_recv_sem.at[n], yn)

    top, bottom = slice(0, HALF), slice(HALF, BLK)

    def project_away():
        near = pl.ds(pl.multiple_of(2 * x * HE, E), 2 * HE)
        far = pl.ds(pl.multiple_of(2 * (1 - x) * HE, E), 2 * HE)
        drain(wo, in_sem)
        with jax.named_scope('wait_o_away'):
            wait_o(0, 0)
        with jax.named_scope('proj'):
            ysend[0, top] = jnp.dot(ofull[away, top, near], wo[0, near, :], preferred_element_type=F32)
        with jax.named_scope('wait_o_away'):
            wait_o(0, 1)
        for first in (0, NC // 2):
            cols = pl.ds(first, NC // 2)
            ysend[0, top, cols] += jnp.dot(ofull[away, top, far], wo[0, far, cols], preferred_element_type=F32)
            remote(ysend.at[0, pl.ds(0, HALF), cols], yrecv.at[0, pl.ds(0, HALF), cols], y_send_sem, y_recv_sem.at[0], yn).start()

        @pl.loop(1, NOUT)
        def _(n):
            with jax.named_scope('proj'):
                ysend[n, top] = jnp.dot(ofull[away, top], wo[n], preferred_element_type=F32)
            y_copy(n, 0).start()

    def project_rest():
        with jax.named_scope('wait_o_away'):
            wait_o(1, 0)
            wait_o(1, 1)

        @pl.loop(0, NOUT)
        def _(n):
            with jax.named_scope('proj'):
                ysend[n, bottom] = jnp.dot(ofull[away, bottom], wo[n], preferred_element_type=F32)
            y_copy(n, 1).start()

    @pl.loop(0, 4)
    def _(stage):
        @pl.when(stage == 2 * tp)
        def _():
            rest_of_rows()

        @pl.when((stage == 1 - tp) | (stage == 3))
        def _():
            attend_blocks((stage < 2) == (tp == 0))

            @pl.when((tp == 1) & (stage == 0))
            def _():
                for k in range(LATE, NK):
                    own(k, 1).start()

        @pl.when(stage == 2 - tp)
        def _():
            project_away()

            @pl.when((tp == 1) | (c == 0))
            def _():
                project_rest()

    with jax.named_scope('wait_o_home'):
        drain(osend.at[pl.ds(0, 3)], o_recv_sem.at[4])

    @pl.when((tp == 0) & (c == 1))
    def _():
        project_rest()

    def kept(n):
        return acc.at[pl.ds(pl.multiple_of(n % 6 * BLK, BLK), BLK), pl.ds(pl.multiple_of(n // 6 * NC, NC), NC)]

    @pl.loop(0, NOUT)
    def _(n):
        kept(n)[...] = jnp.dot(ofull[home], wo[n], preferred_element_type=F32)

    @pl.loop(0, NOUT)
    def _(n):
        with jax.named_scope('wait_y'):
            drain(yrecv.at[n], y_recv_sem.at[n])
        y_ref[:, pl.ds(pl.multiple_of(n * NC, NC), NC)] = (kept(n)[...] + yrecv[n]).astype(BF16)

    drain(xs.at[:, pl.ds(0, 6 * BLK), :], x_send)
    for t in range(2):
        for xx in range(2):
            over_x = DIAG_X * BLK if t else (NK - LATE) * BLK + (1 - xx) * HALF
            over_y = LATE * BLK - xx * HALF if t else (NK - DIAG_X) * BLK

            @pl.when((tp == t) & (x == xx))
            def _():
                drain(xs.at[pl.ds(0, 2), pl.ds(0, (over_x + over_y) // 2), :], dg_send)
    drain(osend.at[pl.ds(0, 6)], o_send_sem)
    drain(ysend, y_send_sem)


def solution(mesh):
    def device_fn(x_loc, w_q, w_k, w_v, w_o):
        dma = pltpu.SemaphoreType.DMA
        heads_major = [jnp.transpose(t, (1, 0, 2)) for t in (w_q, w_k, w_v)]
        return pl.pallas_call(
            kernel,
            name='attention_layer',
            out_shape=pltpu.VMEM((BLK, D), BF16),
            in_specs=[pl.BlockSpec(memory_space=pl.ANY)] * 5,
            out_specs=pl.BlockSpec(memory_space=pltpu.VMEM),
            scratch_shapes=[
                pltpu.VMEM((NK, 512, KC), BF16),
                pltpu.VMEM((D, NQKV), BF16),
                pltpu.VMEM((NOUT, 20 * E, NC), BF16),
                pltpu.VMEM((512, NQKV), BF16),
                pltpu.VMEM((384, NQKV), F32),
                pltpu.VMEM((8, BLK, HE), BF16),
                pltpu.VMEM((2, BLK, 20 * E), BF16),
                pltpu.VMEM((NOUT, BLK, NC), F32),
                pltpu.VMEM((NOUT, BLK, NC), F32),
                dma, dma, dma, dma, dma((3, NK)), dma((2 * NK + LATE,)), dma,
                dma, dma((5,)),
                dma, dma((NOUT,)),
            ],
            compiler_params=pltpu.CompilerParams(collective_id=0, has_side_effects=True, vmem_limit_bytes=64 * 1000 * 1000),
        )(x_loc, *heads_major, w_o.reshape(20 * E, D))

    seq_spec = P(('dp', 'cp', 'tp'), None)
    head_spec = P(None, 'tp', None)
    return jax.shard_map(device_fn, mesh=mesh, in_specs=(seq_spec, head_spec, head_spec, head_spec, P('tp', None, None)), out_specs=seq_spec, check_vma=False)
```
